256 devices in a mesh: sec: 4 (over z_hi), row: 8 (over x, core), col: 8 (over y, z_lo).
Axes of the slice: x: 4, y: 4, z: 8 (z_hi: 4, z_lo: 2; z = z_hi * 2 + z_lo), core: 2. Of those that a mesh axis runs over, the one named last changes fastest.
Arguments:
- vel_modes: float32 [3, 2, 4, 1024, 1024], P(None, None, 'sec', 'row', 'col'), may hold values from -0.005859375 to 0.005859375
- scalar: float32 [4, 2048, 2048], P('sec', 'row', 'col'), may hold values from -6 to 6
- obstacle: int32 [4, 16, 16], P('sec', 'row', 'col'), may hold values from 0 to 2
Outputs:
- scalar_next: float32 [4, 2048, 2048], P('sec', 'row', 'col')
The draws below stay inside these ranges and needn't reach their ends.
All inputs are finite; a program needn't handle non-finite values.
Results may differ from the reference program's by a relative error of at most 0.00005.
Values sent between devices are 32-bit elements; how exact they have to be, the bound alone decides.
A program may use at most 64 MiB of HBM per device.

```python
import jax
import jax.numpy as jnp
from jax import lax

NV = 1024
NS = 2048
BLOCK = 128
PLANES = 4
TILES = 16


def set_ends(array, stream_key, low, top_value):
    longest = array.shape.index(max(array.shape))
    spots = []
    for shift in (0, 1):
        where = [jax.random.randint(jax.random.fold_in(stream_key, axis), (), 0, length) for axis, length in enumerate(array.shape)]
        where[longest] = (where[longest] + shift) % array.shape[longest]
        spots.append(tuple(where))
    return array.at[spots[0]].set(low).at[spots[1]].set(top_value)


def shard_levels(rng, shape, cuts, least, largest):
    factor_of = 1.0
    for axis_at, shards_of in cuts:
        steps = jax.random.uniform(jax.random.fold_in(jax.random.fold_in(rng, 6), axis_at), (shards_of,), jnp.float32, least / len(cuts), largest / len(cuts))
        factor_of = factor_of * jnp.repeat(jnp.exp(steps), shape[axis_at] // shards_of).reshape((-1,) + (1,) * (len(shape) - 1 - axis_at))
    return factor_of


def centred(stream_key, shape, width, bound, pieces=(), kind=jnp.bfloat16):
    result = width * jax.random.normal(stream_key, shape, jnp.float32)
    if pieces:
        result = result * shard_levels(stream_key, shape, pieces, -0.22, 0.18)
    return jnp.clip(result, -bound, bound).astype(kind)


def setup_inputs(seed: int = 0) -> dict:
    key_list = jax.random.split(jax.random.key(seed), 4)
    return {
        "vel_modes": centred(key_list[0], (3, 2, PLANES, NV, NV), (NV * NV) ** -0.5, 0.005859375, ((2, 4), (3, 8), (4, 8)), jnp.float32),
        "scalar": centred(key_list[1], (PLANES, NS, NS), 1.0, 6.0, ((0, 4), (1, 8), (2, 8)), jnp.float32),
        "obstacle": set_ends(jax.random.randint(key_list[2], (PLANES, TILES, TILES), 0, 3), jax.random.fold_in(key_list[2], 1), 0, 2).astype(jnp.int32),
    }


def pad_modes(spectral):
    middle = NV // 2
    filler = jnp.zeros((NS - NV, NV), spectral.dtype)
    spectral = jnp.concatenate([spectral[:middle], filler, spectral[middle:]], 0)
    filler = jnp.zeros((NS, NS - NV), spectral.dtype)
    return jnp.concatenate([spectral[:, :middle], filler, spectral[:, middle:]], 1)


def plane_field(mode_pair):
    spectrum = pad_modes(mode_pair[0] + 1j * mode_pair[1])
    return jnp.real(jnp.fft.ifft2(spectrum)) * (NS * NS)


def reference(vel_modes, scalar, obstacle):
    fields = [lax.map(plane_field, (vel_modes[component, 0], vel_modes[component, 1])) for component in range(3)]
    right_cell = jnp.roll(scalar, -1, 2)
    left_cell = jnp.roll(scalar, 1, 2)
    front_cell = jnp.roll(scalar, -1, 1)
    back_cell = jnp.roll(scalar, 1, 1)
    padded = jnp.pad(scalar, ((1, 1), (0, 0), (0, 0)))
    above_cell = padded[2:]
    below_cell = padded[:-2]
    transport = fields[0] * (right_cell - left_cell) + fields[1] * (front_cell - back_cell) + fields[2] * (above_cell - below_cell)
    laplace = right_cell + left_cell + front_cell + back_cell + above_cell + below_cell - 6.0 * scalar
    cell_flags = jnp.repeat(jnp.repeat(obstacle.astype(jnp.float32), BLOCK, 1), BLOCK, 2)
    return scalar - 0.125 * transport + 0.04 * laplace - 0.25 * cell_flags * (scalar - 1.0)
```

```python
import math

import jax
import jax.numpy as jnp
import numpy as np
from jax import lax
from jax.experimental import pallas as pl
from jax.experimental.pallas import tpu as pltpu
from jax.sharding import PartitionSpec as P

NV = 1024
NS = 2048
ROWS = 8
COLS = 8
SECS = 4
F32 = jnp.float32
BF16 = jnp.bfloat16
MESH = pl.DeviceIdType.MESH
HALF_ROOT = math.sqrt(0.5)


def split_pair(table):
    high = table.astype(BF16)
    low = (table - high.astype(np.float64)).astype(BF16)
    return high, low


def tables():
    k = np.arange(NV)
    k = np.where(k < NV // 2, k, k - NV)
    s = np.arange(256)
    turn = 2.0 * math.pi / NS * ((k[:, None] * s[None, :]) % NS)
    x_high, x_low = split_pair(np.concatenate([np.cos(turn), np.sin(turn)], 1))
    m = np.arange(128)
    m = np.where(m < 64, m, m - 128)
    turn = 2.0 * math.pi / 256 * ((s[:, None] * m[None, :]) % 256)
    c, d = np.cos(turn), np.sin(turn)
    y_high, y_low = split_pair(np.block([[c, -d], [d, c]]))
    lanes = np.arange(128)
    turn = 2.0 * math.pi / 8 * ((np.arange(8)[:, None] * lanes[None, :]) % 8)
    phases = np.concatenate([np.cos(turn), np.sin(turn)], 0).astype(np.float32)
    q = np.arange(8)
    turn = 2.0 * math.pi / NS * (s[:, None] * q[None, :])
    twiddles = np.concatenate([np.cos(turn), np.sin(turn)], 1).astype(np.float32)
    return x_high, x_low, y_high, y_low, phases, twiddles


def split(value):
    high = value.astype(BF16)
    return high, (value - high.astype(F32)).astype(BF16)


def kernel(modes, scalar, obstacle, x_high_in, x_low_in, y_high, y_low, phases, twiddles, out,
           arrived, x_high, x_low, lhs, sent, spectra, rhs, waves, twist, fields, velocity,
           padded, edges_out, edges_in, planes, base, slopes,
           table_sem, mode_sem, spectra_sem, velocity_sem, halo_sem, plane_sem, send_sem):
    sec, row, col = lax.axis_index("sec"), lax.axis_index("row"), lax.axis_index("col")
    place = row * COLS + col
    own_part = lax.rem(row, 4)
    own_half = lax.div(row, 4)

    loads = (pltpu.make_async_copy(scalar.at[0], padded.at[pl.ds(8, 256)], table_sem.at[0]),
             pltpu.make_async_copy(x_high_in, x_high, table_sem.at[1]),
             pltpu.make_async_copy(x_low_in, x_low, table_sem.at[2]))
    for load in loads:
        load.start()

    def own_modes(p):
        return pltpu.make_async_copy(
            modes.at[p, :, 0, pl.ds(pl.multiple_of(16 * col, 16), 16), :], arrived.at[p, col], mode_sem.at[p])

    for p in range(3):
        own_modes(p).start()

    barrier = pltpu.get_barrier_semaphore()

    def greet(i, carry):
        peer = lax.rem(place + i, ROWS * COLS)
        pl.semaphore_signal(barrier, inc=1, device_id=(sec, lax.div(peer, COLS), lax.rem(peer, COLS)), device_id_type=MESH)
        return carry

    lax.fori_loop(1, ROWS * COLS, greet, 0)
    for step in (1, 3):
        pl.semaphore_signal(barrier, inc=1, device_id=(lax.rem(sec + step, SECS), row, col), device_id_type=MESH)
    pl.semaphore_wait(barrier, ROWS * COLS + 1)

    def send_modes(i, carry):
        p = lax.div(i, COLS - 1)
        peer = lax.rem(col + 1 + lax.rem(i, COLS - 1), COLS)
        pltpu.make_async_remote_copy(
            modes.at[p, :, 0, pl.ds(pl.multiple_of(16 * peer, 16), 16), :], arrived.at[p, col],
            send_sem.at[0], mode_sem.at[p], device_id=(sec, row, peer), device_id_type=MESH).start()
        return carry

    lax.fori_loop(0, 3 * (COLS - 1), send_modes, 0)

    row_next, row_last = lax.rem(row + 1, ROWS), lax.rem(row + ROWS - 1, ROWS)
    col_next, col_last = lax.rem(col + 1, COLS), lax.rem(col + COLS - 1, COLS)
    loads[0].wait()
    edges_out[0] = padded[pl.ds(8, 256), pl.ds(128, 128)].T[120:128]
    edges_out[1] = padded[pl.ds(8, 256), pl.ds(0, 128)].T[0:8]
    halo_copies = (
        pltpu.make_async_remote_copy(scalar.at[0, pl.ds(248, 8)], padded.at[pl.ds(0, 8)], send_sem.at[3], halo_sem.at[0],
                                     device_id=(sec, row_next, col), device_id_type=MESH),
        pltpu.make_async_remote_copy(scalar.at[0, pl.ds(0, 8)], padded.at[pl.ds(264, 8)], send_sem.at[4], halo_sem.at[1],
                                     device_id=(sec, row_last, col), device_id_type=MESH),
        pltpu.make_async_remote_copy(edges_out.at[0], edges_in.at[0], send_sem.at[5], halo_sem.at[2],
                                     device_id=(sec, row, col_next), device_id_type=MESH),
        pltpu.make_async_remote_copy(edges_out.at[1], edges_in.at[1], send_sem.at[6], halo_sem.at[3],
                                     device_id=(sec, row, col_last), device_id_type=MESH),
    )
    for copy in halo_copies:
        copy.start()

    for q in range(1, 8):
        twist[0, q - 1] = jnp.broadcast_to(twiddles[:, q:q + 1], (256, 128))
        twist[1, q - 1] = jnp.broadcast_to(twiddles[:, 8 + q:9 + q], (256, 128))

    loads[1].wait()
    loads[2].wait()

    def transform_x(p, carry):
        pltpu.make_async_copy(arrived.at[p], arrived.at[p], mode_sem.at[p]).wait()
        for a in range(8):
            real, imag = arrived[p, a, 0], arrived[p, a, 1]
            for block in range(8):
                cosine, sine = phases[block:block + 1, :], phases[8 + block:9 + block, :]
                if block == 0:
                    turned = (real, imag)
                else:
                    turned = (real * cosine - imag * sine, real * sine + imag * cosine)
                for part in range(2):
                    high, low = split(turned[part])
                    lhs[pl.ds((block * 2 + part) * 16, 16), pl.ds(128 * a, 128)] = high
                    lhs[pl.ds(256 + (block * 2 + part) * 16, 16), pl.ds(128 * a, 128)] = low
        main = jnp.dot(lhs[...], x_high[...], preferred_element_type=F32)
        rest = jnp.dot(lhs[pl.ds(0, 256), :], x_low[...], preferred_element_type=F32)
        total = main[:256] + main[256:] + rest
        for block in range(8):
            real, imag = total[32 * block:32 * block + 16], total[32 * block + 16:32 * block + 32]
            new_real = real[:, :256] - imag[:, 256:]
            new_imag = real[:, 256:] + imag[:, :256]
            for half in range(2):
                sent[p, block, half, 0] = new_real[:, 128 * half:128 * half + 128]
                sent[p, block, half, 1] = new_imag[:, 128 * half:128 * half + 128]

        def send_spectra(i, inner):
            block = lax.rem(col + lax.div(i, 2), COLS)
            half = lax.rem(i, 2)
            owner = 4 * half + p
            rows = pl.ds(pl.multiple_of(16 * place, 16), 16)

            @pl.when((block != col) | (owner != row))
            def _():
                pltpu.make_async_remote_copy(
                    sent.at[p, block, half], spectra.at[:, rows, :], send_sem.at[1], spectra_sem,
                    device_id=(sec, owner, block), device_id_type=MESH).start()

            @pl.when((block == col) & (owner == row))
            def _():
                spectra[:, rows, :] = sent[p, block, half]

            return inner

        lax.fori_loop(0, 16, send_spectra, 0)
        return carry

    lax.fori_loop(0, 3, transform_x, 0)

    up = pltpu.make_async_remote_copy(scalar.at[0], planes.at[0], send_sem.at[7], plane_sem.at[0],
                                      device_id=(lax.rem(sec + 1, SECS), row, col), device_id_type=MESH)
    down = pltpu.make_async_remote_copy(scalar.at[0], planes.at[1], send_sem.at[8], plane_sem.at[1],
                                        device_id=(lax.rem(sec + SECS - 1, SECS), row, col), device_id_type=MESH)

    @pl.when(sec < SECS - 1)
    def _():
        up.start()

    @pl.when(sec > 0)
    def _():
        down.start()

    @pl.when(sec == 0)
    def _():
        planes[0] = jnp.zeros((256, 256), F32)

    @pl.when(sec == SECS - 1)
    def _():
        planes[1] = jnp.zeros((256, 256), F32)

    for copy in halo_copies:
        copy.wait()
    left_edge = edges_in[0].T[:, 7:8]
    right_edge = edges_in[1].T[:, 0:1]
    lane = lax.broadcasted_iota(jnp.int32, (128, 256), 1)
    for block in range(2):
        at = 8 + 128 * block
        here = padded[pl.ds(at, 128), :]
        left = jnp.where(lane == 0, left_edge[128 * block:128 * block + 128], pltpu.roll(here, 1, 1))
        right = jnp.where(lane == 255, right_edge[128 * block:128 * block + 128], pltpu.roll(here, 255, 1))
        back = padded[pl.ds(at - 1, 128), :]
        front = padded[pl.ds(at + 1, 128), :]
        flag = jnp.where(lane < 128, obstacle[0, block, 0].astype(F32), obstacle[0, block, 1].astype(F32))
        rows = pl.ds(128 * block, 128)
        slopes[0, rows, :] = right - left
        slopes[1, rows, :] = front - back
        base[rows, :] = here + 0.04 * (left + right + back + front - 6.0 * here) - 0.25 * flag * (here - 1.0)

    @pl.when(own_part < 3)
    def _():
        pltpu.make_async_copy(spectra.at[:, pl.ds(0, 1008), :], spectra.at[:, pl.ds(0, 1008), :], spectra_sem).wait()
        for q in range(8):
            for part in range(2):
                high, low = split(spectra[part, pl.ds(q, 128, stride=8), :])
                rhs[pl.ds(128 * part, 128), pl.ds(128 * q, 128)] = high
                rhs[pl.ds(256 + 128 * part, 128), pl.ds(128 * q, 128)] = low
        waves[...] = (jnp.dot(y_high[...], rhs[pl.ds(0, 256), :], preferred_element_type=F32)
                      + jnp.dot(y_high[...], rhs[pl.ds(256, 256), :], preferred_element_type=F32)
                      + jnp.dot(y_low[...], rhs[pl.ds(0, 256), :], preferred_element_type=F32))

        def combine(i, carry):
            at = pl.multiple_of(16 * i, 16)
            rows = pl.ds(at, 16)
            real, imag = [], []
            for q in range(8):
                re = waves[rows, pl.ds(128 * q, 128)]
                if q == 0:
                    real.append(re)
                    imag.append(None)
                    continue
                im = waves[pl.ds(256 + at, 16), pl.ds(128 * q, 128)]
                cosine, sine = twist[0, q - 1, rows, :], twist[1, q - 1, rows, :]
                real.append(re * cosine - im * sine)
                imag.append(None if q == 4 else re * sine + im * cosine)
            a1, b1 = real[1] + real[7], imag[1] - imag[7]
            a2, b2 = real[2] + real[6], imag[2] - imag[6]
            a3, b3 = real[3] + real[5], imag[3] - imag[5]
            even, odd = real[0] + real[4], real[0] - real[4]
            e0, e2, e1, e3 = even + a2, even - a2, odd - b2, odd + b2
            d0, d2 = a1 + a3, b3 - b1
            amid, bmid = HALF_ROOT * (a1 - a3), HALF_ROOT * (b1 + b3)
            d1, d3 = amid - bmid, -amid - bmid
            for r, (e, d) in enumerate(((e0, d0), (e1, d1), (e2, d2), (e3, d3))):
                fields[r, rows, :] = e + d
                fields[r + 4, rows, :] = e - d
            return carry

        lax.fori_loop(0, 16, combine, 0)

        def send_fields(i, carry):
            peer = lax.rem(row + i, ROWS)
            pltpu.make_async_remote_copy(
                fields.at[peer], velocity.at[own_part, own_half], send_sem.at[2], velocity_sem.at[own_part],
                device_id=(sec, peer, col), device_id_type=MESH).start()
            return carry

        lax.fori_loop(1, ROWS, send_fields, 0)
        velocity[own_part, own_half] = fields[row]

    @pl.when(sec > 0)
    def _():
        up.wait_recv()

    @pl.when(sec < SECS - 1)
    def _():
        down.wait_recv()

    slopes[2] = planes[1] - planes[0]
    base[...] = base[...] + 0.04 * (planes[1] + planes[0])

    for p in range(3):
        one = pltpu.make_async_copy(velocity.at[p, 0], velocity.at[p, 0], velocity_sem.at[p])
        two = pltpu.make_async_copy(velocity.at[p], velocity.at[p], velocity_sem.at[p])
        pl.when(own_part == p)(one.wait)
        pl.when(own_part != p)(two.wait)
    for half in range(2):
        lanes = pl.ds(128 * half, 128)
        out[0, :, lanes] = base[:, lanes] - 0.125 * (
            velocity[0, half] * slopes[0, :, lanes] + velocity[1, half] * slopes[1, :, lanes]
            + velocity[2, half] * slopes[2, :, lanes])

    sent_modes = arrived.at[:, pl.ds(0, 7)]
    pltpu.make_async_copy(sent_modes, sent_modes, send_sem.at[0]).wait()

    @pl.when(own_part < 3)
    def _():
        some = spectra.at[:, pl.ds(0, 47 * 16), :]
        pltpu.make_async_copy(some, some, send_sem.at[1]).wait()
        most = fields.at[pl.ds(0, 7)]
        pltpu.make_async_copy(most, most, send_sem.at[2]).wait()

    @pl.when(own_part == 3)
    def _():
        some = spectra.at[:, pl.ds(0, 48 * 16), :]
        pltpu.make_async_copy(some, some, send_sem.at[1]).wait()

    @pl.when(sec < SECS - 1)
    def _():
        up.wait_send()

    @pl.when(sec > 0)
    def _():
        down.wait_send()


def body(modes, scalar, obstacle):
    x_high, x_low, y_high, y_low, phases, twiddles = (jnp.asarray(t) for t in tables())
    anywhere = pl.BlockSpec(memory_space=pl.ANY)
    vmem = pl.BlockSpec(memory_space=pltpu.VMEM)
    smem = pl.BlockSpec(memory_space=pltpu.SMEM)
    dma = pltpu.SemaphoreType.DMA
    return pl.pallas_call(
        kernel,
        out_shape=jax.ShapeDtypeStruct((1, 256, 256), F32),
        in_specs=[anywhere, anywhere, smem, anywhere, anywhere, vmem, vmem, vmem, vmem],
        out_specs=vmem,
        scratch_shapes=[
            pltpu.VMEM((3, 8, 2, 16, 128), F32),
            pltpu.VMEM((1024, 512), BF16),
            pltpu.VMEM((1024, 512), BF16),
            pltpu.VMEM((512, 1024), BF16),
            pltpu.VMEM((3, 8, 2, 2, 16, 128), F32),
            pltpu.VMEM((2, 1024, 128), F32),
            pltpu.VMEM((512, 1024), BF16),
            pltpu.VMEM((512, 1024), F32),
            pltpu.VMEM((2, 7, 256, 128), F32),
            pltpu.VMEM((8, 256, 128), F32),
            pltpu.VMEM((3, 2, 256, 128), F32),
            pltpu.VMEM((272, 256), F32),
            pltpu.VMEM((2, 8, 256), F32),
            pltpu.VMEM((2, 8, 256), F32),
            pltpu.VMEM((2, 256, 256), F32),
            pltpu.VMEM((256, 256), F32),
            pltpu.VMEM((3, 256, 256), F32),
            dma((3,)), dma((3,)), dma, dma((3,)), dma((4,)), dma((2,)), dma((9,)),
        ],
        compiler_params=pltpu.CompilerParams(
            collective_id=0, has_side_effects=True, vmem_limit_bytes=56 * 1024 * 1024),
    )(modes, scalar, obstacle, x_high, x_low, y_high, y_low, phases, twiddles)


def solution(mesh):
    in_specs = (P(None, None, "sec", "row", "col"), P("sec", "row", "col"), P("sec", "row", "col"))
    out_specs = P("sec", "row", "col")
    return jax.shard_map(body, mesh=mesh, in_specs=in_specs, out_specs=out_specs, check_vma=False)
```

```python
import math

import jax
import jax.numpy as jnp
import numpy as np
from jax import lax
from jax.experimental import pallas as pl
from jax.experimental.pallas import tpu as pltpu
from jax.sharding import PartitionSpec as P

NV = 1024
NS = 2048
ROWS = 8
COLS = 8
SECS = 4
F32 = jnp.float32
BF16 = jnp.bfloat16
MESH = pl.DeviceIdType.MESH
HALF_ROOT = math.sqrt(0.5)


def split_pair(table):
    high = table.astype(BF16)
    low = (table - high.astype(np.float64)).astype(BF16)
    return high, low


def tables():
    k = np.arange(NV)
    k = np.where(k < NV // 2, k, k - NV)
    s = np.arange(256)
    turn = 2.0 * math.pi / NS * ((k[:, None] * s[None, :]) % NS)
    x_high, x_low = split_pair(np.concatenate([np.cos(turn), np.sin(turn)], 1))
    m = np.arange(128)
    m = np.where(m < 64, m, m - 128)
    turn = 2.0 * math.pi / 256 * ((s[:, None] * m[None, :]) % 256)
    c, d = np.cos(turn), np.sin(turn)
    y_high, y_low = split_pair(np.block([[c, -d], [d, c]]))
    lanes = np.arange(128)
    turn = 2.0 * math.pi / 8 * ((np.arange(8)[:, None] * lanes[None, :]) % 8)
    phases = np.concatenate([np.cos(turn), np.sin(turn)], 0).astype(np.float32)
    q = np.arange(8)
    turn = 2.0 * math.pi / NS * (s[:, None] * q[None, :])
    twiddles = np.concatenate([np.cos(turn), np.sin(turn)], 1).astype(np.float32)
    return x_high, x_low, y_high, y_low, phases, twiddles


def split(value):
    high = value.astype(BF16)
    return high, (value - high.astype(F32)).astype(BF16)


def kernel(modes_in, scalar, obstacle, x_high_in, x_low_in, y_high_in, y_low_in, phases_in, twiddles_in, out,
           modes, arrived, x_high, x_low, y_high, y_low, phases, twiddles, lhs, sent, spectra, rhs, waves, twist, fields, velocity,
           padded, edges_out, edges_in, planes, base, slopes,
           table_sem, mode_sem, spectra_sem, velocity_sem, halo_sem, plane_sem, send_sem, ready_sem):
    sec, row, col = lax.axis_index("sec"), lax.axis_index("row"), lax.axis_index("col")

    barrier = pltpu.get_barrier_semaphore()

    def at_row(i):
        return (sec, lax.rem(row + i, ROWS), col)

    def at_col(i):
        return (sec, row, lax.rem(col + i, COLS))

    for i in range(1, 8):
        pl.semaphore_signal(barrier, inc=1, device_id=at_col(i), device_id_type=MESH)
        pl.semaphore_signal(barrier, inc=1, device_id=at_row(i), device_id_type=MESH)
    for step in (1, 3):
        pl.semaphore_signal(barrier, inc=1, device_id=(lax.rem(sec + step, SECS), row, col), device_id_type=MESH)

    pairs = ((modes_in, modes), (scalar.at[0], padded.at[pl.ds(8, 256)]), (twiddles_in, twiddles), (phases_in, phases),
             (x_high_in, x_high), (x_low_in, x_low), (y_high_in, y_high), (y_low_in, y_low))
    loads = [pltpu.make_async_copy(here, there, table_sem.at[i]) for i, (here, there) in enumerate(pairs)]
    for load in loads:
        load.start()

    lead = (col, col, row)
    follow = (row, row, col)
    lead_peer = (at_col, at_col, at_row)
    follow_peer = (at_row, at_row, at_col)

    loads[0].wait()
    for part in range(2):
        modes[2, part, 0] = modes[2, part, 0].T
    pl.semaphore_wait(barrier, 16)

    for i in range(1, 8):
        for p in (0, 2, 1):
            peer = lax.rem(lead[p] + i, 8)
            pltpu.make_async_remote_copy(
                modes.at[p, :, 0, pl.ds(pl.multiple_of(16 * peer, 16), 16), :], arrived.at[p, lead[p]],
                send_sem.at[0], mode_sem.at[p], device_id=lead_peer[p](i), device_id_type=MESH).start()
    for i in range(1, 8):
        pl.semaphore_signal(ready_sem, inc=1, device_id=at_row(i), device_id_type=MESH)

    loads[1].wait()
    edges_out[0] = padded[pl.ds(8, 256), pl.ds(128, 128)].T[120:128]
    edges_out[1] = padded[pl.ds(8, 256), pl.ds(0, 128)].T[0:8]
    halo_copies = (
        pltpu.make_async_remote_copy(scalar.at[0, pl.ds(248, 8)], padded.at[pl.ds(0, 8)], send_sem.at[3], halo_sem.at[0],
                                     device_id=at_row(1), device_id_type=MESH),
        pltpu.make_async_remote_copy(scalar.at[0, pl.ds(0, 8)], padded.at[pl.ds(264, 8)], send_sem.at[4], halo_sem.at[1],
                                     device_id=at_row(7), device_id_type=MESH),
        pltpu.make_async_remote_copy(edges_out.at[0], edges_in.at[0], send_sem.at[5], halo_sem.at[2],
                                     device_id=at_col(1), device_id_type=MESH),
        pltpu.make_async_remote_copy(edges_out.at[1], edges_in.at[1], send_sem.at[6], halo_sem.at[3],
                                     device_id=at_col(7), device_id_type=MESH),
    )
    for copy in halo_copies:
        copy.start()

    loads[2].wait()
    for q in range(1, 8):
        twist[0, q - 1] = jnp.broadcast_to(twiddles[:, q:q + 1], (256, 128))
        twist[1, q - 1] = jnp.broadcast_to(twiddles[:, 8 + q:9 + q], (256, 128))
    for p in range(3):
        arrived[p, lead[p]] = modes[p, :, 0, pl.ds(pl.multiple_of(16 * lead[p], 16), 16), :]
    for load in loads[3:]:
        load.wait()
    pl.semaphore_wait(ready_sem, 7)

    parity = lax.rem(row + col, 2)
    chunk = lax.div(row, 2)
    plain_owner = parity == 0
    turned_owner = lax.rem(col, 4) == 1 + lax.rem(row, 2)
    own_half = jnp.where(plain_owner, lax.rem(chunk, 2), lax.div(col, 4))
    own_part = jnp.where(plain_owner, lax.div(chunk, 2), jnp.where(turned_owner, 2, 3))

    for p in (0, 2, 1):
        some = arrived.at[p, pl.ds(0, 7)]
        pltpu.make_async_copy(some, some, mode_sem.at[p]).wait()
        for a in range(8):
            real, imag = arrived[p, a, 0], arrived[p, a, 1]
            for block in range(8):
                cosine, sine = phases[block:block + 1, :], phases[8 + block:9 + block, :]
                if block == 0:
                    turned = (real, imag)
                else:
                    turned = (real * cosine - imag * sine, real * sine + imag * cosine)
                for part in range(2):
                    high, low = split(turned[part])
                    lhs[pl.ds((block * 2 + part) * 16, 16), pl.ds(128 * a, 128)] = high
                    lhs[pl.ds(256 + (block * 2 + part) * 16, 16), pl.ds(128 * a, 128)] = low
        main = jnp.dot(lhs[...], x_high[...], preferred_element_type=F32)
        rest = jnp.dot(lhs[pl.ds(0, 256), :], x_low[...], preferred_element_type=F32)
        total = main[:256] + main[256:] + rest
        for block in range(8):
            real, imag = total[32 * block:32 * block + 16], total[32 * block + 16:32 * block + 32]
            new_real = real[:, :256] - imag[:, 256:]
            new_imag = real[:, 256:] + imag[:, :256]
            for half in range(2):
                sent[p, block, half, 0] = new_real[:, 128 * half:128 * half + 128]
                sent[p, block, half, 1] = new_imag[:, 128 * half:128 * half + 128]

        rows = pl.ds(pl.multiple_of(16 * (follow[p] * 8 + lead[p]), 16), 16)
        for i in range(8):
            block = lax.rem(lead[p] + i, 8)
            for half in range(2):
                if p < 2:
                    owner = 2 * (2 * p + half) + lax.rem(block, 2)
                    target = (sec, owner, block)
                else:
                    owner = 4 * half + 1 + lax.rem(block, 2)
                    target = (sec, block, owner)

                def away():
                    pltpu.make_async_remote_copy(
                        sent.at[p, block, half], spectra.at[:, rows, :], send_sem.at[1], spectra_sem,
                        device_id=target, device_id_type=MESH).start()

                if i > 0:
                    away()
                else:
                    pl.when(owner != follow[p])(away)

                    @pl.when(owner == follow[p])
                    def _():
                        spectra[:, rows, :] = sent[p, block, half]

    up = pltpu.make_async_remote_copy(scalar.at[0], planes.at[0], send_sem.at[7], plane_sem.at[0],
                                      device_id=(lax.rem(sec + 1, SECS), row, col), device_id_type=MESH)
    down = pltpu.make_async_remote_copy(scalar.at[0], planes.at[1], send_sem.at[8], plane_sem.at[1],
                                        device_id=(lax.rem(sec + SECS - 1, SECS), row, col), device_id_type=MESH)

    @pl.when(sec < SECS - 1)
    def _():
        up.start()

    @pl.when(sec > 0)
    def _():
        down.start()

    @pl.when(sec == 0)
    def _():
        planes[0] = jnp.zeros((256, 256), F32)

    @pl.when(sec == SECS - 1)
    def _():
        planes[1] = jnp.zeros((256, 256), F32)

    for copy in halo_copies:
        copy.wait()
    left_edge = edges_in[0].T[:, 7:8]
    right_edge = edges_in[1].T[:, 0:1]
    lane = lax.broadcasted_iota(jnp.int32, (128, 256), 1)
    for block in range(2):
        at = 8 + 128 * block
        here = padded[pl.ds(at, 128), :]
        left = jnp.where(lane == 0, left_edge[128 * block:128 * block + 128], pltpu.roll(here, 1, 1))
        right = jnp.where(lane == 255, right_edge[128 * block:128 * block + 128], pltpu.roll(here, 255, 1))
        back = padded[pl.ds(at - 1, 128), :]
        front = padded[pl.ds(at + 1, 128), :]
        flag = jnp.where(lane < 128, obstacle[0, block, 0].astype(F32), obstacle[0, block, 1].astype(F32))
        rows = pl.ds(128 * block, 128)
        slopes[0, rows, :] = right - left
        slopes[1, rows, :] = front - back
        base[rows, :] = here + 0.04 * (left + right + back + front - 6.0 * here) - 0.25 * flag * (here - 1.0)

    @pl.when(own_part < 3)
    def _():
        pltpu.make_async_copy(spectra.at[:, pl.ds(0, 1008), :], spectra.at[:, pl.ds(0, 1008), :], spectra_sem).wait()
        for q in range(8):
            for part in range(2):
                high, low = split(spectra[part, pl.ds(q, 128, stride=8), :])
                rhs[pl.ds(128 * part, 128), pl.ds(128 * q, 128)] = high
                rhs[pl.ds(256 + 128 * part, 128), pl.ds(128 * q, 128)] = low
        waves[...] = (jnp.dot(y_high[...], rhs[pl.ds(0, 256), :], preferred_element_type=F32)
                      + jnp.dot(y_high[...], rhs[pl.ds(256, 256), :], preferred_element_type=F32)
                      + jnp.dot(y_low[...], rhs[pl.ds(0, 256), :], preferred_element_type=F32))

        def combine(i, carry):
            at = pl.multiple_of(16 * i, 16)
            rows = pl.ds(at, 16)
            real, imag = [], []
            for q in range(8):
                re = waves[rows, pl.ds(128 * q, 128)]
                if q == 0:
                    real.append(re)
                    imag.append(None)
                    continue
                im = waves[pl.ds(256 + at, 16), pl.ds(128 * q, 128)]
                cosine, sine = twist[0, q - 1, rows, :], twist[1, q - 1, rows, :]
                real.append(re * cosine - im * sine)
                imag.append(None if q == 4 else re * sine + im * cosine)
            a1, b1 = real[1] + real[7], imag[1] - imag[7]
            a2, b2 = real[2] + real[6], imag[2] - imag[6]
            a3, b3 = real[3] + real[5], imag[3] - imag[5]
            even, odd = real[0] + real[4], real[0] - real[4]
            e0, e2, e1, e3 = even + a2, even - a2, odd - b2, odd + b2
            d0, d2 = a1 + a3, b3 - b1
            amid, bmid = HALF_ROOT * (a1 - a3), HALF_ROOT * (b1 + b3)
            d1, d3 = amid - bmid, -amid - bmid
            for r, (e, d) in enumerate(((e0, d0), (e1, d1), (e2, d2), (e3, d3))):
                fields[r, rows, :] = e + d
                fields[r + 4, rows, :] = e - d
            return carry

        lax.fori_loop(0, 16, combine, 0)

    def send_fields(number, peers):
        def go():
            for i in range(1, 8):
                peer = lax.rem(number + i, 8)
                pltpu.make_async_remote_copy(
                    fields.at[peer], velocity.at[own_part, own_half], send_sem.at[2], velocity_sem.at[own_part],
                    device_id=peers(i), device_id_type=MESH).start()
            velocity[own_part, own_half] = fields[number]
        return go

    pl.when(own_part < 2)(send_fields(row, at_row))
    pl.when(own_part == 2)(send_fields(col, at_col))

    @pl.when(sec > 0)
    def _():
        up.wait_recv()

    @pl.when(sec < SECS - 1)
    def _():
        down.wait_recv()

    slopes[2] = planes[1] - planes[0]
    base[...] = base[...] + 0.04 * (planes[1] + planes[0])

    for p in range(3):
        one = pltpu.make_async_copy(velocity.at[p, 0], velocity.at[p, 0], velocity_sem.at[p])
        two = pltpu.make_async_copy(velocity.at[p], velocity.at[p], velocity_sem.at[p])
        pl.when(own_part == p)(one.wait)
        pl.when(own_part != p)(two.wait)
    for half in range(2):
        rows = pl.ds(128 * half, 128)
        turned = velocity[2, half].T
        for block in range(2):
            lanes = pl.ds(128 * block, 128)
            out[0, rows, lanes] = base[rows, lanes] - 0.125 * (
                velocity[0, block, rows, :] * slopes[0, rows, lanes] + velocity[1, block, rows, :] * slopes[1, rows, lanes]
                + turned[:, 128 * block:128 * block + 128] * slopes[2, rows, lanes])

    sent_modes = arrived.at[:, pl.ds(0, 7)]
    pltpu.make_async_copy(sent_modes, sent_modes, send_sem.at[0]).wait()

    @pl.when(own_part < 3)
    def _():
        some = spectra.at[:, pl.ds(0, 47 * 16), :]
        pltpu.make_async_copy(some, some, send_sem.at[1]).wait()
        most = fields.at[pl.ds(0, 7)]
        pltpu.make_async_copy(most, most, send_sem.at[2]).wait()

    @pl.when(own_part == 3)
    def _():
        some = spectra.at[:, pl.ds(0, 48 * 16), :]
        pltpu.make_async_copy(some, some, send_sem.at[1]).wait()

    @pl.when(sec < SECS - 1)
    def _():
        up.wait_send()

    @pl.when(sec > 0)
    def _():
        down.wait_send()


def body(modes, scalar, obstacle):
    x_high, x_low, y_high, y_low, phases, twiddles = (jnp.asarray(t) for t in tables())
    anywhere = pl.BlockSpec(memory_space=pl.ANY)
    vmem = pl.BlockSpec(memory_space=pltpu.VMEM)
    smem = pl.BlockSpec(memory_space=pltpu.SMEM)
    dma = pltpu.SemaphoreType.DMA
    return pl.pallas_call(
        kernel,
        out_shape=jax.ShapeDtypeStruct((1, 256, 256), F32),
        in_specs=[anywhere, anywhere, smem] + [anywhere] * 6,
        out_specs=vmem,
        scratch_shapes=[
            pltpu.VMEM((3, 2, 1, 128, 128), F32),
            pltpu.VMEM((3, 8, 2, 16, 128), F32),
            pltpu.VMEM((1024, 512), BF16),
            pltpu.VMEM((1024, 512), BF16),
            pltpu.VMEM((512, 256), BF16),
            pltpu.VMEM((512, 256), BF16),
            pltpu.VMEM((16, 128), F32),
            pltpu.VMEM((256, 16), F32),
            pltpu.VMEM((512, 1024), BF16),
            pltpu.VMEM((3, 8, 2, 2, 16, 128), F32),
            pltpu.VMEM((2, 1024, 128), F32),
            pltpu.VMEM((512, 1024), BF16),
            pltpu.VMEM((512, 1024), F32),
            pltpu.VMEM((2, 7, 256, 128), F32),
            pltpu.VMEM((8, 256, 128), F32),
            pltpu.VMEM((3, 2, 256, 128), F32),
            pltpu.VMEM((272, 256), F32),
            pltpu.VMEM((2, 8, 256), F32),
            pltpu.VMEM((2, 8, 256), F32),
            pltpu.VMEM((2, 256, 256), F32),
            pltpu.VMEM((256, 256), F32),
            pltpu.VMEM((3, 256, 256), F32),
            dma((8,)), dma((3,)), dma, dma((3,)), dma((4,)), dma((2,)), dma((9,)), pltpu.SemaphoreType.REGULAR,
        ],
        compiler_params=pltpu.CompilerParams(
            collective_id=0, has_side_effects=True, vmem_limit_bytes=56 * 1024 * 1024),
    )(modes, scalar, obstacle, x_high, x_low, y_high, y_low, phases, twiddles)


def solution(mesh):
    in_specs = (P(None, None, "sec", "row", "col"), P("sec", "row", "col"), P("sec", "row", "col"))
    out_specs = P("sec", "row", "col")
    return jax.shard_map(body, mesh=mesh, in_specs=in_specs, out_specs=out_specs, check_vma=False)
```

```python
import math

import jax
import jax.numpy as jnp
import numpy as np
from jax import lax
from jax.experimental import pallas as pl
from jax.experimental.pallas import tpu as pltpu
from jax.sharding import PartitionSpec as P

NV = 1024
NS = 2048
ROWS = 8
COLS = 8
SECS = 4
EARLY = 64
F32 = jnp.float32
BF16 = jnp.bfloat16
MESH = pl.DeviceIdType.MESH
HALF_ROOT = math.sqrt(0.5)


def split_pair(table):
    high = table.astype(BF16)
    low = (table - high.astype(np.float64)).astype(BF16)
    return high, low


def tables():
    k = np.arange(NV)
    k = np.where(k < NV // 2, k, k - NV)
    s = np.arange(256)
    turn = 2.0 * math.pi / NS * ((k[:, None] * s[None, :]) % NS)
    x_high, x_low = split_pair(np.concatenate([np.cos(turn), np.sin(turn)], 1))
    m = np.arange(128)
    m = np.where(m < 64, m, m - 128)
    turn = 2.0 * math.pi / 256 * ((s[:, None] * m[None, :]) % 256)
    c, d = np.cos(turn), np.sin(turn)
    y_high, y_low = split_pair(np.block([[c, -d], [d, c]]))
    lanes = np.arange(128)
    turn = 2.0 * math.pi / 8 * ((np.arange(8)[:, None] * lanes[None, :]) % 8)
    phases = np.concatenate([np.cos(turn), np.sin(turn)], 0).astype(np.float32)
    q = np.arange(8)
    turn = 2.0 * math.pi / NS * (s[:, None] * q[None, :])
    twiddles = np.concatenate([np.cos(turn), np.sin(turn)], 1).astype(np.float32)
    return x_high, x_low, y_high, y_low, phases, twiddles


def split(value):
    high = value.astype(BF16)
    return high, (value - high.astype(F32)).astype(BF16)


def kernel(modes_in, scalar, obstacle, x_high_in, x_low_in, y_high_in, y_low_in, phases_in, twiddles_in, out,
           modes, arrived, x_high, x_low, y_high, y_low, phases, twiddles, lhs, sent, spectra, rhs, waves, twist, fields, velocity,
           padded, edges_out, edges_in, planes, base, slopes,
           table_sem, mode_sem, spectra_sem, velocity_sem, halo_sem, plane_sem, send_sem, ready_sem, go_sem):
    sec, row, col = lax.axis_index("sec"), lax.axis_index("row"), lax.axis_index("col")

    barrier = pltpu.get_barrier_semaphore()

    def at_row(i):
        return (sec, lax.rem(row + i, ROWS), col)

    def at_col(i):
        return (sec, row, lax.rem(col + i, COLS))

    for i in range(1, 8):
        pl.semaphore_signal(barrier, inc=1, device_id=at_col(i), device_id_type=MESH)
        pl.semaphore_signal(barrier, inc=1, device_id=at_row(i), device_id_type=MESH)
    for step in (1, 3):
        pl.semaphore_signal(barrier, inc=1, device_id=(lax.rem(sec + step, SECS), row, col), device_id_type=MESH)

    pairs = ((modes_in, modes), (scalar.at[0], padded.at[pl.ds(8, 256)]), (twiddles_in, twiddles), (phases_in, phases),
             (x_high_in, x_high), (x_low_in, x_low), (y_high_in, y_high), (y_low_in, y_low))
    loads = [pltpu.make_async_copy(here, there, table_sem.at[i]) for i, (here, there) in enumerate(pairs)]
    for load in loads:
        load.start()

    lead = (col, col, row)
    follow = (row, row, col)
    lead_peer = (at_col, at_col, at_row)
    follow_peer = (at_row, at_row, at_col)

    loads[0].wait()
    for part in range(2):
        modes[2, part, 0] = modes[2, part, 0].T
    pl.semaphore_wait(barrier, 16)

    for p in (0, 2, 1):
        for i in range(1, 8):
            peer = lax.rem(lead[p] + i, 8)
            pltpu.make_async_remote_copy(
                modes.at[p, :, 0, pl.ds(pl.multiple_of(16 * peer, 16), 16), :], arrived.at[p, lead[p]],
                send_sem.at[0], mode_sem.at[p], device_id=lead_peer[p](i), device_id_type=MESH).start()
    for i in range(1, 8):
        pl.semaphore_signal(ready_sem, inc=1, device_id=at_row(i), device_id_type=MESH)

    loads[1].wait()
    edges_out[0] = padded[pl.ds(8, 256), pl.ds(128, 128)].T[120:128]
    edges_out[1] = padded[pl.ds(8, 256), pl.ds(0, 128)].T[0:8]
    halo_copies = (
        pltpu.make_async_remote_copy(scalar.at[0, pl.ds(248, 8)], padded.at[pl.ds(0, 8)], send_sem.at[3], halo_sem.at[0],
                                     device_id=at_row(1), device_id_type=MESH),
        pltpu.make_async_remote_copy(scalar.at[0, pl.ds(0, 8)], padded.at[pl.ds(264, 8)], send_sem.at[4], halo_sem.at[1],
                                     device_id=at_row(7), device_id_type=MESH),
        pltpu.make_async_remote_copy(edges_out.at[0], edges_in.at[0], send_sem.at[5], halo_sem.at[2],
                                     device_id=at_col(1), device_id_type=MESH),
        pltpu.make_async_remote_copy(edges_out.at[1], edges_in.at[1], send_sem.at[6], halo_sem.at[3],
                                     device_id=at_col(7), device_id_type=MESH),
    )
    for copy in halo_copies:
        copy.start()

    loads[2].wait()
    for q in range(1, 8):
        twist[0, q - 1] = jnp.broadcast_to(twiddles[:, q:q + 1], (256, 128))
        twist[1, q - 1] = jnp.broadcast_to(twiddles[:, 8 + q:9 + q], (256, 128))
    for p in range(3):
        arrived[p, lead[p]] = modes[p, :, 0, pl.ds(pl.multiple_of(16 * lead[p], 16), 16), :]
    for load in loads[3:]:
        load.wait()
    pl.semaphore_wait(ready_sem, 7)

    parity = lax.rem(row + col, 2)
    chunk = lax.div(row, 2)
    plain_owner = parity == 0
    turned_owner = lax.rem(col, 4) == 1 + lax.rem(row, 2)
    own_half = jnp.where(plain_owner, lax.rem(chunk, 2), lax.div(col, 4))
    own_part = jnp.where(plain_owner, lax.div(chunk, 2), jnp.where(turned_owner, 2, 3))

    def plane_copies(piece):
        rows = pl.ds(0, EARLY) if piece == 0 else pl.ds(EARLY, 256 - EARLY)
        return [pltpu.make_async_remote_copy(
            scalar.at[0, rows], planes.at[i, rows], send_sem.at[7 + 2 * piece + i], plane_sem.at[2 * piece + i],
            device_id=(lax.rem(sec + step, SECS), row, col), device_id_type=MESH) for i, step in enumerate((1, 3))]

    has_above, has_below = sec < SECS - 1, sec > 0

    def send_planes(piece):
        up, down = plane_copies(piece)
        pl.when(has_above)(up.start)
        pl.when(has_below)(down.start)

    @pl.when(sec == 0)
    def _():
        planes[0] = jnp.zeros((256, 256), F32)

    @pl.when(sec == SECS - 1)
    def _():
        planes[1] = jnp.zeros((256, 256), F32)

    for p in (0, 2, 1):
        some = arrived.at[p, pl.ds(0, 7)]
        pltpu.make_async_copy(some, some, mode_sem.at[p]).wait()
        if p == 0:
            send_planes(0)
        for a in range(8):
            real, imag = arrived[p, a, 0], arrived[p, a, 1]
            for block in range(8):
                cosine, sine = phases[block:block + 1, :], phases[8 + block:9 + block, :]
                if block == 0:
                    turned = (real, imag)
                else:
                    turned = (real * cosine - imag * sine, real * sine + imag * cosine)
                for part in range(2):
                    high, low = split(turned[part])
                    lhs[pl.ds((block * 2 + part) * 16, 16), pl.ds(128 * a, 128)] = high
                    lhs[pl.ds(256 + (block * 2 + part) * 16, 16), pl.ds(128 * a, 128)] = low
        main = jnp.dot(lhs[...], x_high[...], preferred_element_type=F32)
        rest = jnp.dot(lhs[pl.ds(0, 256), :], x_low[...], preferred_element_type=F32)
        total = main[:256] + main[256:] + rest
        for block in range(8):
            real, imag = total[32 * block:32 * block + 16], total[32 * block + 16:32 * block + 32]
            new_real = real[:, :256] - imag[:, 256:]
            new_imag = real[:, 256:] + imag[:, :256]
            for half in range(2):
                sent[p, block, half, 0] = new_real[:, 128 * half:128 * half + 128]
                sent[p, block, half, 1] = new_imag[:, 128 * half:128 * half + 128]

        rows = pl.ds(pl.multiple_of(16 * (follow[p] * 8 + lead[p]), 16), 16)
        for i in range(8):
            block = lax.rem(lead[p] + i, 8)
            for half in range(2):
                if p < 2:
                    owner = 2 * (2 * p + half) + lax.rem(block, 2)
                    target = (sec, owner, block)
                else:
                    owner = 4 * half + 1 + lax.rem(block, 2)
                    target = (sec, block, owner)

                def away():
                    pltpu.make_async_remote_copy(
                        sent.at[p, block, half], spectra.at[:, rows, :], send_sem.at[1], spectra_sem,
                        device_id=target, device_id_type=MESH).start()

                if i > 0:
                    away()
                else:
                    pl.when(owner != follow[p])(away)

                    @pl.when(owner == follow[p])
                    def _():
                        spectra[:, rows, :] = sent[p, block, half]

    for copy in halo_copies:
        copy.wait()
    left_edge = edges_in[0].T[:, 7:8]
    right_edge = edges_in[1].T[:, 0:1]
    lane = lax.broadcasted_iota(jnp.int32, (128, 256), 1)
    for block in range(2):
        at = 8 + 128 * block
        here = padded[pl.ds(at, 128), :]
        left = jnp.where(lane == 0, left_edge[128 * block:128 * block + 128], pltpu.roll(here, 1, 1))
        right = jnp.where(lane == 255, right_edge[128 * block:128 * block + 128], pltpu.roll(here, 255, 1))
        back = padded[pl.ds(at - 1, 128), :]
        front = padded[pl.ds(at + 1, 128), :]
        flag = jnp.where(lane < 128, obstacle[0, block, 0].astype(F32), obstacle[0, block, 1].astype(F32))
        rows = pl.ds(128 * block, 128)
        slopes[0, rows, :] = right - left
        slopes[1, rows, :] = front - back
        base[rows, :] = here + 0.04 * (left + right + back + front - 6.0 * here) - 0.25 * flag * (here - 1.0)

    @pl.when(own_part < 3)
    def _():
        pltpu.make_async_copy(spectra.at[:, pl.ds(0, 1008), :], spectra.at[:, pl.ds(0, 1008), :], spectra_sem).wait()
        send_planes(1)

        @pl.when(plain_owner)
        def _():
            pl.semaphore_signal(go_sem, inc=1, device_id=(sec, row + 1 - 2 * lax.rem(row, 2), col), device_id_type=MESH)

        for q in range(8):
            for part in range(2):
                high, low = split(spectra[part, pl.ds(q, 128, stride=8), :])
                rhs[pl.ds(128 * part, 128), pl.ds(128 * q, 128)] = high
                rhs[pl.ds(256 + 128 * part, 128), pl.ds(128 * q, 128)] = low
        waves[...] = (jnp.dot(y_high[...], rhs[pl.ds(0, 256), :], preferred_element_type=F32)
                      + jnp.dot(y_high[...], rhs[pl.ds(256, 256), :], preferred_element_type=F32)
                      + jnp.dot(y_low[...], rhs[pl.ds(0, 256), :], preferred_element_type=F32))

        def combine(i, carry):
            at = pl.multiple_of(16 * i, 16)
            rows = pl.ds(at, 16)
            real, imag = [], []
            for q in range(8):
                re = waves[rows, pl.ds(128 * q, 128)]
                if q == 0:
                    real.append(re)
                    imag.append(None)
                    continue
                im = waves[pl.ds(256 + at, 16), pl.ds(128 * q, 128)]
                cosine, sine = twist[0, q - 1, rows, :], twist[1, q - 1, rows, :]
                real.append(re * cosine - im * sine)
                imag.append(None if q == 4 else re * sine + im * cosine)
            a1, b1 = real[1] + real[7], imag[1] - imag[7]
            a2, b2 = real[2] + real[6], imag[2] - imag[6]
            a3, b3 = real[3] + real[5], imag[3] - imag[5]
            even, odd = real[0] + real[4], real[0] - real[4]
            e0, e2, e1, e3 = even + a2, even - a2, odd - b2, odd + b2
            d0, d2 = a1 + a3, b3 - b1
            amid, bmid = HALF_ROOT * (a1 - a3), HALF_ROOT * (b1 + b3)
            d1, d3 = amid - bmid, -amid - bmid
            for r, (e, d) in enumerate(((e0, d0), (e1, d1), (e2, d2), (e3, d3))):
                fields[r, rows, :] = e + d
                fields[r + 4, rows, :] = e - d
            return carry

        lax.fori_loop(0, 16, combine, 0)

    @pl.when(parity == 1)
    def _():
        pl.semaphore_wait(go_sem, 1)

    @pl.when(own_part == 3)
    def _():
        send_planes(1)

    def send_fields(number, peers):
        def go():
            for i in range(1, 8):
                peer = lax.rem(number + i, 8)
                pltpu.make_async_remote_copy(
                    fields.at[peer], velocity.at[own_part, own_half], send_sem.at[2], velocity_sem.at[own_part],
                    device_id=peers(i), device_id_type=MESH).start()
            velocity[own_part, own_half] = fields[number]
        return go

    pl.when(own_part < 2)(send_fields(row, at_row))
    pl.when(own_part == 2)(send_fields(col, at_col))

    for piece in range(2):
        up, down = plane_copies(piece)
        pl.when(has_below)(up.wait_recv)
        pl.when(has_above)(down.wait_recv)
    slopes[2] = planes[1] - planes[0]
    base[...] = base[...] + 0.04 * (planes[1] + planes[0])

    for p in range(3):
        one = pltpu.make_async_copy(velocity.at[p, 0], velocity.at[p, 0], velocity_sem.at[p])
        two = pltpu.make_async_copy(velocity.at[p], velocity.at[p], velocity_sem.at[p])
        pl.when(own_part == p)(one.wait)
        pl.when(own_part != p)(two.wait)
    for half in range(2):
        rows = pl.ds(128 * half, 128)
        turned = velocity[2, half].T
        for block in range(2):
            lanes = pl.ds(128 * block, 128)
            out[0, rows, lanes] = base[rows, lanes] - 0.125 * (
                velocity[0, block, rows, :] * slopes[0, rows, lanes] + velocity[1, block, rows, :] * slopes[1, rows, lanes]
                + turned[:, 128 * block:128 * block + 128] * slopes[2, rows, lanes])

    sent_modes = arrived.at[:, pl.ds(0, 7)]
    pltpu.make_async_copy(sent_modes, sent_modes, send_sem.at[0]).wait()

    @pl.when(own_part < 3)
    def _():
        some = spectra.at[:, pl.ds(0, 47 * 16), :]
        pltpu.make_async_copy(some, some, send_sem.at[1]).wait()
        most = fields.at[pl.ds(0, 7)]
        pltpu.make_async_copy(most, most, send_sem.at[2]).wait()

    @pl.when(own_part == 3)
    def _():
        some = spectra.at[:, pl.ds(0, 48 * 16), :]
        pltpu.make_async_copy(some, some, send_sem.at[1]).wait()

    for piece in range(2):
        up, down = plane_copies(piece)
        pl.when(has_above)(up.wait_send)
        pl.when(has_below)(down.wait_send)


def body(modes, scalar, obstacle):
    x_high, x_low, y_high, y_low, phases, twiddles = (jnp.asarray(t) for t in tables())
    anywhere = pl.BlockSpec(memory_space=pl.ANY)
    vmem = pl.BlockSpec(memory_space=pltpu.VMEM)
    smem = pl.BlockSpec(memory_space=pltpu.SMEM)
    dma = pltpu.SemaphoreType.DMA
    return pl.pallas_call(
        kernel,
        out_shape=jax.ShapeDtypeStruct((1, 256, 256), F32),
        in_specs=[anywhere, anywhere, smem] + [anywhere] * 6,
        out_specs=vmem,
        scratch_shapes=[
            pltpu.VMEM((3, 2, 1, 128, 128), F32),
            pltpu.VMEM((3, 8, 2, 16, 128), F32),
            pltpu.VMEM((1024, 512), BF16),
            pltpu.VMEM((1024, 512), BF16),
            pltpu.VMEM((512, 256), BF16),
            pltpu.VMEM((512, 256), BF16),
            pltpu.VMEM((16, 128), F32),
            pltpu.VMEM((256, 16), F32),
            pltpu.VMEM((512, 1024), BF16),
            pltpu.VMEM((3, 8, 2, 2, 16, 128), F32),
            pltpu.VMEM((2, 1024, 128), F32),
            pltpu.VMEM((512, 1024), BF16),
            pltpu.VMEM((512, 1024), F32),
            pltpu.VMEM((2, 7, 256, 128), F32),
            pltpu.VMEM((8, 256, 128), F32),
            pltpu.VMEM((3, 2, 256, 128), F32),
            pltpu.VMEM((272, 256), F32),
            pltpu.VMEM((2, 8, 256), F32),
            pltpu.VMEM((2, 8, 256), F32),
            pltpu.VMEM((2, 256, 256), F32),
            pltpu.VMEM((256, 256), F32),
            pltpu.VMEM((3, 256, 256), F32),
            dma((8,)), dma((3,)), dma, dma((3,)), dma((4,)), dma((4,)), dma((11,)), pltpu.SemaphoreType.REGULAR, pltpu.SemaphoreType.REGULAR,
        ],
        compiler_params=pltpu.CompilerParams(
            collective_id=0, has_side_effects=True, vmem_limit_bytes=56 * 1024 * 1024),
    )(modes, scalar, obstacle, x_high, x_low, y_high, y_low, phases, twiddles)


def solution(mesh):
    in_specs = (P(None, None, "sec", "row", "col"), P("sec", "row", "col"), P("sec", "row", "col"))
    out_specs = P("sec", "row", "col")
    return jax.shard_map(body, mesh=mesh, in_specs=in_specs, out_specs=out_specs, check_vma=False)
```

```python
import math

import jax
import jax.numpy as jnp
import numpy as np
from jax import lax
from jax.experimental import pallas as pl
from jax.experimental.pallas import tpu as pltpu
from jax.sharding import PartitionSpec as P

NV = 1024
NS = 2048
ROWS = 8
COLS = 8
SECS = 4
EARLY = 64
F32 = jnp.float32
BF16 = jnp.bfloat16
MESH = pl.DeviceIdType.MESH
HALF_ROOT = math.sqrt(0.5)


def split_pair(table):
    high = table.astype(BF16)
    low = (table - high.astype(np.float64)).astype(BF16)
    return high, low


def tables():
    k = np.arange(NV)
    k = np.where(k < NV // 2, k, k - NV)
    s = np.arange(256)
    turn = 2.0 * math.pi / NS * ((k[:, None] * s[None, :]) % NS)
    x_high, x_low = split_pair(np.concatenate([np.cos(turn), np.sin(turn)], 0))
    m = np.arange(64)
    turn = 2.0 * math.pi / 256 * ((s[:, None] * m[None, :]) % 256)
    c, d = np.cos(turn), np.sin(turn)
    y_high, y_low = split_pair(np.block([[c, d], [d, -c]]))
    y_high = np.concatenate([y_high, y_high], 1)
    lanes = np.arange(128)
    turn = 2.0 * math.pi / 8 * ((np.arange(8)[:, None] * lanes[None, :]) % 8)
    phases = np.concatenate([np.cos(turn), np.sin(turn)], 0).astype(np.float32)
    q = np.arange(8)
    turn = 2.0 * math.pi / NS * (s[:, None] * q[None, :])
    twiddles = np.concatenate([np.cos(turn), np.sin(turn)], 1).astype(np.float32)
    return x_high, x_low, y_high, y_low, phases, twiddles


def split(value):
    high = value.astype(BF16)
    return high, (value - high.astype(F32)).astype(BF16)


def flip(index, bits):
    total = 0
    for unit in (1, 2, 4):
        bit = lax.rem(lax.div(index, unit), 2)
        total = total + unit * ((1 - bit) if bits & unit else bit)
    return total


def kernel(modes_in, scalar, obstacle, x_high_in, x_low_in, y_high_in, y_low_in, phases_in, twiddles_in, out,
           modes, row_zero, extra, arrived, x_high, x_low, y_high, y_low, phases, twiddles, lhs, lone, lone_sent, lone_row, sent, spectra, rhs, waves, twist, fields, velocity,
           padded, edges_out, edges_in, planes, base, slopes,
           table_sem, mode_sem, extra_sem, lone_sem, spectra_sem, velocity_sem, halo_sem, plane_sem, send_sem, ready_sem, go_sem):
    sec, row, col = lax.axis_index("sec"), lax.axis_index("row"), lax.axis_index("col")

    barrier = pltpu.get_barrier_semaphore()

    def at_row(i):
        return (sec, lax.rem(row + i, ROWS), col)

    def at_col(i):
        return (sec, row, lax.rem(col + i, COLS))

    greeted = [at_col(i) for i in range(1, 8)] + [(sec, 7 - row, lax.rem(col + i, COLS)) for i in range(8)]
    greeted += [(sec, flip(row, i), c) for i in range(1, 7) for c in (col, 7 - col)]
    for device in greeted:
        pl.semaphore_signal(barrier, inc=1, device_id=device, device_id_type=MESH)
    for step in (1, 3):
        pl.semaphore_signal(barrier, inc=1, device_id=(lax.rem(sec + step, SECS), row, col), device_id_type=MESH)

    pairs = ((modes_in, modes), (scalar.at[0], padded.at[pl.ds(8, 256)]), (twiddles_in, twiddles), (phases_in, phases),
             (x_high_in, x_high), (x_low_in, x_low), (y_high_in, y_high), (y_low_in, y_low))
    loads = [pltpu.make_async_copy(here, there, table_sem.at[i]) for i, (here, there) in enumerate(pairs)]
    for load in loads:
        load.start()

    lead = (col, col, row)
    follow = (row, row, col)
    upper = [lax.div(f, 4) for f in follow]
    group = [f + u * (7 - 2 * f) for f, u in zip(follow, upper)]

    def device_at(p, f, l):
        return (sec, f, l) if p < 2 else (sec, l, f)

    loads[0].wait()
    for part in range(2):
        modes[2, part, 0] = modes[2, part, 0].T
    ahead = lax.broadcasted_iota(jnp.int32, (128, 128), 0) + lax.broadcasted_iota(jnp.int32, (128, 128), 1)
    mirror = jnp.where(ahead == 128, 1.0, 0.0).astype(F32)

    def turn_round(p):
        def go():
            for part in range(2):
                block = modes[p, part, 0]
                row_zero[p, part:part + 1] = block[0:1]
                modes[p, part, 0] = jnp.dot(mirror, block, precision=lax.Precision.HIGHEST, preferred_element_type=F32)
        return go

    for p in (0, 2, 1):
        pl.when(follow[p] >= 4)(turn_round(p))
    pl.semaphore_wait(barrier, 29)
    for i in (1, 2, 3):
        pl.semaphore_signal(ready_sem, inc=1, device_id=(sec, flip(row, i), col), device_id_type=MESH)

    for p in (0, 2, 1):
        slot = 8 * upper[p] + lead[p]
        for i in range(8):
            other = lax.rem(lead[p] + i, 8)
            for f in ((follow[p], 7 - follow[p]) if i else (7 - follow[p],)):
                pltpu.make_async_remote_copy(
                    modes.at[p, :, 0, pl.ds(pl.multiple_of(8 * (2 * other + lax.div(f, 4)), 8), 8), :], arrived.at[p, slot],
                    send_sem.at[0], mode_sem.at[p], device_id=device_at(p, f, other), device_id_type=MESH).start()

    loads[1].wait()
    edges_out[0] = padded[pl.ds(8, 256), pl.ds(128, 128)].T[120:128]
    edges_out[1] = padded[pl.ds(8, 256), pl.ds(0, 128)].T[0:8]
    halo_copies = (
        pltpu.make_async_remote_copy(scalar.at[0, pl.ds(248, 8)], padded.at[pl.ds(0, 8)], send_sem.at[3], halo_sem.at[0],
                                     device_id=at_row(1), device_id_type=MESH),
        pltpu.make_async_remote_copy(scalar.at[0, pl.ds(0, 8)], padded.at[pl.ds(264, 8)], send_sem.at[4], halo_sem.at[1],
                                     device_id=at_row(7), device_id_type=MESH),
        pltpu.make_async_remote_copy(edges_out.at[0], edges_in.at[0], send_sem.at[5], halo_sem.at[2],
                                     device_id=at_col(1), device_id_type=MESH),
        pltpu.make_async_remote_copy(edges_out.at[1], edges_in.at[1], send_sem.at[6], halo_sem.at[3],
                                     device_id=at_col(7), device_id_type=MESH),
    )
    for copy in halo_copies:
        copy.start()

    loads[2].wait()
    for q in range(1, 8):
        twist[0, q - 1] = jnp.broadcast_to(twiddles[:, q:q + 1], (256, 128))
        twist[1, q - 1] = jnp.broadcast_to(twiddles[:, 8 + q:9 + q], (256, 128))
    for p in range(3):
        own = 2 * lead[p] + upper[p]
        arrived[p, 8 * upper[p] + lead[p]] = modes[p, :, 0, pl.ds(pl.multiple_of(8 * own, 8), 8), :]
    for load in loads[3:]:
        load.wait()
    pl.semaphore_wait(ready_sem, 3)

    def send_zero(p):
        return pltpu.make_async_remote_copy(
            row_zero.at[p], extra.at[p, lead[p]], send_sem.at[11 + p], extra_sem.at[p],
            device_id=device_at(p, lax.rem(8 - follow[p], 4), 0), device_id_type=MESH)

    for p in (0, 2, 1):
        pl.when(follow[p] >= 4)(send_zero(p).start)
    first = (row == 0) & (col == 0)
    sublane = lax.broadcasted_iota(jnp.int32, (8, 128), 0)
    special = sublane < jnp.where(first, 1, 0)

    def owner_of(p, block, half):
        if p < 2:
            return (sec, 2 * (2 * p + half) + lax.rem(block, 2), block)
        return (sec, block, 4 * half + 1 + lax.rem(block, 2))

    parity = lax.rem(row + col, 2)
    chunk = lax.div(row, 2)
    plain_owner = parity == 0
    turned_owner = lax.rem(col, 4) == 1 + lax.rem(row, 2)
    own_half = jnp.where(plain_owner, lax.rem(chunk, 2), lax.div(col, 4))
    own_part = jnp.where(plain_owner, lax.div(chunk, 2), jnp.where(turned_owner, 2, 3))

    def plane_copies(piece):
        rows = pl.ds(0, EARLY) if piece == 0 else pl.ds(EARLY, 256 - EARLY)
        return [pltpu.make_async_remote_copy(
            scalar.at[0, rows], planes.at[i, rows], send_sem.at[7 + 2 * piece + i], plane_sem.at[2 * piece + i],
            device_id=(lax.rem(sec + step, SECS), row, col), device_id_type=MESH) for i, step in enumerate((1, 3))]

    has_above, has_below = sec < SECS - 1, sec > 0

    def send_planes(piece):
        up, down = plane_copies(piece)
        pl.when(has_above)(up.start)
        pl.when(has_below)(down.start)

    @pl.when(sec == 0)
    def _():
        planes[0] = jnp.zeros((256, 256), F32)

    @pl.when(sec == SECS - 1)
    def _():
        planes[1] = jnp.zeros((256, 256), F32)

    for p in (0, 2, 1):
        some = arrived.at[p, pl.ds(0, 15)]
        pltpu.make_async_copy(some, some, mode_sem.at[p]).wait()
        if p == 0:
            send_planes(0)

        @pl.when((lead[p] == 0) & (follow[p] < 4))
        def _():
            pltpu.make_async_copy(extra.at[p], extra.at[p], extra_sem.at[p]).wait()
            for a in range(8):
                for part in range(2):
                    arrived[p, 8 + a, part, 0:1] = jnp.where(follow[p] > 0, extra[p, a, part:part + 1], 0.0)

        for a in range(8):
            plus, minus = arrived[p, a], arrived[p, 8 + a]
            sum_real, sum_imag = plus[0] + minus[0], plus[1] + minus[1]
            gap_real = jnp.where(special, extra[p, a, 1:2], plus[0] - minus[0])
            gap_imag = jnp.where(special, -extra[p, a, 0:1], plus[1] - minus[1])
            for block in range(8):
                cosine, sine = phases[block:block + 1, :], phases[8 + block:9 + block, :]
                if block == 0:
                    a_real, a_imag, b_real, b_imag = sum_real, sum_imag, gap_real, gap_imag
                else:
                    a_real, a_imag = sum_real * cosine - sum_imag * sine, sum_real * sine + sum_imag * cosine
                    b_real, b_imag = gap_real * cosine - gap_imag * sine, gap_real * sine + gap_imag * cosine
                for part, tile in enumerate(((a_real, -b_imag), (-a_imag, -b_real))):
                    high, low = split(jnp.concatenate(tile, 0))
                    lhs[pl.ds(16 * block, 16), pl.ds(1024 * part + 128 * a, 128)] = high
                    lhs[pl.ds(128 + 16 * block, 16), pl.ds(1024 * part + 128 * a, 128)] = low
        main = jnp.dot(lhs[...], x_high[...], preferred_element_type=F32)
        rest = jnp.dot(lhs[pl.ds(0, 128), :], x_low[...], preferred_element_type=F32)
        total = main[:128] + main[128:] + rest
        for block in range(8):
            for half in range(2):
                tile = total[16 * block:16 * block + 16, 128 * half:128 * half + 128]
                sent[p, block, half, 0] = tile[:8]
                sent[p, block, half, 1] = tile[8:]

        rows = pl.ds(pl.multiple_of(8 * (16 * group[p] + 2 * lead[p] + upper[p]), 8), 8)
        for i in range(8):
            block = lax.rem(lead[p] + i, 8)
            for half in range(2):
                target = owner_of(p, block, half)
                mine = target[1 if p < 2 else 2] == follow[p]

                def away():
                    pltpu.make_async_remote_copy(
                        sent.at[p, block, half], spectra.at[:, rows, :], send_sem.at[1], spectra_sem,
                        device_id=target, device_id_type=MESH).start()

                if i > 0:
                    away()
                else:
                    pl.when(jnp.logical_not(mine))(away)

                    @pl.when(mine)
                    def _():
                        spectra[:, rows, :] = sent[p, block, half]

    @pl.when(first)
    def _():
        lone[...] = jnp.zeros_like(lone)
        for p in range(3):
            for a in range(8):
                real, imag = extra[p, a, 0:1], extra[p, a, 1:2]
                cosine, sine = phases[0:8, :], phases[8:16, :]
                lone[8 * p:8 * p + 8, pl.ds(128 * a, 128)] = real * sine + imag * cosine
                lone[8 * p:8 * p + 8, pl.ds(1024 + 128 * a, 128)] = real * cosine - imag * sine
        high, low = split(lone[...])
        total = (jnp.dot(high, x_high[...], preferred_element_type=F32) + jnp.dot(low, x_high[...], preferred_element_type=F32)
                 + jnp.dot(high, x_low[...], preferred_element_type=F32))
        for p in range(3):
            for block in range(8):
                for half in range(2):
                    tile = jnp.broadcast_to(total[8 * p + block:8 * p + block + 1, 128 * half:128 * half + 128], (8, 128))
                    if p == block == half == 0:
                        lone_row[...] = tile
                        continue
                    index = (p * 8 + block) * 2 + half
                    lone_sent[index] = tile
                    pltpu.make_async_remote_copy(
                        lone_sent.at[index], lone_row, send_sem.at[14], lone_sem,
                        device_id=(sec, 2 * (2 * p + half) + block % 2, block) if p < 2 else (sec, block, 4 * half + 1 + block % 2),
                        device_id_type=MESH).start()

    for copy in halo_copies:
        copy.wait()
    left_edge = edges_in[0].T[:, 7:8]
    right_edge = edges_in[1].T[:, 0:1]
    lane = lax.broadcasted_iota(jnp.int32, (128, 256), 1)
    for block in range(2):
        at = 8 + 128 * block
        here = padded[pl.ds(at, 128), :]
        left = jnp.where(lane == 0, left_edge[128 * block:128 * block + 128], pltpu.roll(here, 1, 1))
        right = jnp.where(lane == 255, right_edge[128 * block:128 * block + 128], pltpu.roll(here, 255, 1))
        back = padded[pl.ds(at - 1, 128), :]
        front = padded[pl.ds(at + 1, 128), :]
        flag = jnp.where(lane < 128, obstacle[0, block, 0].astype(F32), obstacle[0, block, 1].astype(F32))
        rows = pl.ds(128 * block, 128)
        slopes[0, rows, :] = right - left
        slopes[1, rows, :] = front - back
        base[rows, :] = here + 0.04 * (left + right + back + front - 6.0 * here) - 0.25 * flag * (here - 1.0)

    @pl.when(own_part < 3)
    def _():
        pltpu.make_async_copy(spectra.at[:, pl.ds(0, 504), :], spectra.at[:, pl.ds(0, 504), :], spectra_sem).wait()
        send_planes(1)

        @pl.when(plain_owner)
        def _():
            pl.semaphore_signal(go_sem, inc=1, device_id=(sec, row + 1 - 2 * lax.rem(row, 2), col), device_id_type=MESH)

        for q in range(8):
            for part in range(2):
                high, low = split(spectra[part, pl.ds(q, 64, stride=8), :])
                rhs[pl.ds(64 * part, 64), pl.ds(128 * q, 128)] = high
                rhs[pl.ds(128 + 64 * part, 64), pl.ds(128 * q, 128)] = low
        waves[...] = (jnp.dot(y_high[...], rhs[...], preferred_element_type=F32)
                      + jnp.dot(y_low[...], rhs[pl.ds(0, 128), :], preferred_element_type=F32))

        @pl.when(jnp.logical_not(first))
        def _():
            pltpu.make_async_copy(lone_row, lone_row, lone_sem).wait()

        quarter = lax.rem(lax.broadcasted_iota(jnp.int32, (16, 128), 0), 4)
        lone_term = (jnp.where(quarter == 0, 1.0, jnp.where(quarter == 2, -1.0, 0.0)) * spectra[1, 0:1, :]
                     + jnp.where(quarter == 1, 1.0, jnp.where(quarter == 3, -1.0, 0.0)) * lone_row[0:1, :])

        def combine(i, carry):
            at = pl.multiple_of(16 * i, 16)
            rows = pl.ds(at, 16)
            real, imag = [], []
            for q in range(8):
                re = waves[rows, pl.ds(128 * q, 128)]
                if q == 0:
                    real.append(re + lone_term)
                    imag.append(None)
                    continue
                im = waves[pl.ds(256 + at, 16), pl.ds(128 * q, 128)]
                cosine, sine = twist[0, q - 1, rows, :], twist[1, q - 1, rows, :]
                real.append(re * cosine - im * sine)
                imag.append(None if q == 4 else re * sine + im * cosine)
            a1, b1 = real[1] + real[7], imag[1] - imag[7]
            a2, b2 = real[2] + real[6], imag[2] - imag[6]
            a3, b3 = real[3] + real[5], imag[3] - imag[5]
            even, odd = real[0] + real[4], real[0] - real[4]
            e0, e2, e1, e3 = even + a2, even - a2, odd - b2, odd + b2
            d0, d2 = a1 + a3, b3 - b1
            amid, bmid = HALF_ROOT * (a1 - a3), HALF_ROOT * (b1 + b3)
            d1, d3 = amid - bmid, -amid - bmid
            for r, (e, d) in enumerate(((e0, d0), (e1, d1), (e2, d2), (e3, d3))):
                fields[r, rows, :] = e + d
                fields[r + 4, rows, :] = e - d
            return carry

        lax.fori_loop(0, 16, combine, 0)

    @pl.when(parity == 1)
    def _():
        pl.semaphore_wait(go_sem, 1)

    @pl.when(own_part == 3)
    def _():
        send_planes(1)

    def send_fields(number, peers):
        def go():
            for i in range(1, 8):
                peer = lax.rem(number + i, 8)
                pltpu.make_async_remote_copy(
                    fields.at[peer], velocity.at[own_part, own_half], send_sem.at[2], velocity_sem.at[own_part],
                    device_id=peers(i), device_id_type=MESH).start()
            velocity[own_part, own_half] = fields[number]
        return go

    pl.when(own_part < 2)(send_fields(row, at_row))
    pl.when(own_part == 2)(send_fields(col, at_col))

    for piece in range(2):
        up, down = plane_copies(piece)
        pl.when(has_below)(up.wait_recv)
        pl.when(has_above)(down.wait_recv)
    slopes[2] = planes[1] - planes[0]
    base[...] = base[...] + 0.04 * (planes[1] + planes[0])

    for p in range(3):
        one = pltpu.make_async_copy(velocity.at[p, 0], velocity.at[p, 0], velocity_sem.at[p])
        two = pltpu.make_async_copy(velocity.at[p], velocity.at[p], velocity_sem.at[p])
        pl.when(own_part == p)(one.wait)
        pl.when(own_part != p)(two.wait)
    for half in range(2):
        rows = pl.ds(128 * half, 128)
        turned = velocity[2, half].T
        for block in range(2):
            lanes = pl.ds(128 * block, 128)
            out[0, rows, lanes] = base[rows, lanes] - 0.125 * (
                velocity[0, block, rows, :] * slopes[0, rows, lanes] + velocity[1, block, rows, :] * slopes[1, rows, lanes]
                + turned[:, 128 * block:128 * block + 128] * slopes[2, rows, lanes])

    sent_modes = arrived.at[:, pl.ds(0, 15)]
    pltpu.make_async_copy(sent_modes, sent_modes, send_sem.at[0]).wait()

    @pl.when(own_part < 3)
    def _():
        some = spectra.at[:, pl.ds(0, 47 * 8), :]
        pltpu.make_async_copy(some, some, send_sem.at[1]).wait()
        most = fields.at[pl.ds(0, 7)]
        pltpu.make_async_copy(most, most, send_sem.at[2]).wait()

    @pl.when(own_part == 3)
    def _():
        some = spectra.at[:, pl.ds(0, 48 * 8), :]
        pltpu.make_async_copy(some, some, send_sem.at[1]).wait()

    for p in range(3):
        pl.when(follow[p] >= 4)(send_zero(p).wait_send)

    @pl.when(first)
    def _():
        some = lone_sent.at[pl.ds(1, 47)]
        pltpu.make_async_copy(some, some, send_sem.at[14]).wait()

    for piece in range(2):
        up, down = plane_copies(piece)
        pl.when(has_above)(up.wait_send)
        pl.when(has_below)(down.wait_send)


def body(modes, scalar, obstacle):
    x_high, x_low, y_high, y_low, phases, twiddles = (jnp.asarray(t) for t in tables())
    anywhere = pl.BlockSpec(memory_space=pl.ANY)
    vmem = pl.BlockSpec(memory_space=pltpu.VMEM)
    smem = pl.BlockSpec(memory_space=pltpu.SMEM)
    dma = pltpu.SemaphoreType.DMA
    return pl.pallas_call(
        kernel,
        out_shape=jax.ShapeDtypeStruct((1, 256, 256), F32),
        in_specs=[anywhere, anywhere, smem] + [anywhere] * 6,
        out_specs=vmem,
        scratch_shapes=[
            pltpu.VMEM((3, 2, 1, 128, 128), F32),
            pltpu.VMEM((3, 8, 128), F32),
            pltpu.VMEM((3, 8, 8, 128), F32),
            pltpu.VMEM((3, 16, 2, 8, 128), F32),
            pltpu.VMEM((2048, 256), BF16),
            pltpu.VMEM((2048, 256), BF16),
            pltpu.VMEM((512, 256), BF16),
            pltpu.VMEM((512, 128), BF16),
            pltpu.VMEM((16, 128), F32),
            pltpu.VMEM((256, 16), F32),
            pltpu.VMEM((256, 2048), BF16),
            pltpu.VMEM((32, 2048), F32),
            pltpu.VMEM((48, 8, 128), F32),
            pltpu.VMEM((8, 128), F32),
            pltpu.VMEM((3, 8, 2, 2, 8, 128), F32),
            pltpu.VMEM((2, 512, 128), F32),
            pltpu.VMEM((256, 1024), BF16),
            pltpu.VMEM((512, 1024), F32),
            pltpu.VMEM((2, 7, 256, 128), F32),
            pltpu.VMEM((8, 256, 128), F32),
            pltpu.VMEM((3, 2, 256, 128), F32),
            pltpu.VMEM((272, 256), F32),
            pltpu.VMEM((2, 8, 256), F32),
            pltpu.VMEM((2, 8, 256), F32),
            pltpu.VMEM((2, 256, 256), F32),
            pltpu.VMEM((256, 256), F32),
            pltpu.VMEM((3, 256, 256), F32),
            dma((8,)), dma((3,)), dma((3,)), dma, dma, dma((3,)), dma((4,)), dma((4,)), dma((15,)), pltpu.SemaphoreType.REGULAR, pltpu.SemaphoreType.REGULAR,
        ],
        compiler_params=pltpu.CompilerParams(
            collective_id=0, has_side_effects=True, vmem_limit_bytes=56 * 1024 * 1024),
    )(modes, scalar, obstacle, x_high, x_low, y_high, y_low, phases, twiddles)


def solution(mesh):
    in_specs = (P(None, None, "sec", "row", "col"), P("sec", "row", "col"), P("sec", "row", "col"))
    out_specs = P("sec", "row", "col")
    return jax.shard_map(body, mesh=mesh, in_specs=in_specs, out_specs=out_specs, check_vma=False)
```

```python
import math

import jax
import jax.numpy as jnp
import numpy as np
from jax import lax
from jax.experimental import pallas as pl
from jax.experimental.pallas import tpu as pltpu
from jax.sharding import PartitionSpec as P

NV = 1024
NS = 2048
ROWS = 8
COLS = 8
SECS = 4
PIECES = (0,64,0,192)
ORDER = (0,1,2)
F32 = jnp.float32
BF16 = jnp.bfloat16
MESH = pl.DeviceIdType.MESH
HALF_ROOT = math.sqrt(0.5)


def split_pair(table):
    high = table.astype(BF16)
    low = (table - high.astype(np.float64)).astype(BF16)
    return high, low


def tables():
    k = np.arange(NV)
    k = np.where(k < NV // 2, k, k - NV)
    s = np.arange(256)
    turn = 2.0 * math.pi / NS * ((k[:, None] * s[None, :]) % NS)
    x_high, x_low = split_pair(np.concatenate([np.cos(turn), np.sin(turn)], 0))
    m = np.arange(64)
    turn = 2.0 * math.pi / 256 * ((s[:, None] * m[None, :]) % 256)
    c, d = np.cos(turn), np.sin(turn)
    y_high, y_low = split_pair(np.block([[c, d], [d, -c]]))
    y_high = np.concatenate([y_high, y_high], 1)
    lanes = np.arange(128)
    turn = 2.0 * math.pi / 8 * ((np.arange(8)[:, None] * lanes[None, :]) % 8)
    phases = np.concatenate([np.cos(turn), np.sin(turn)], 0).astype(np.float32)
    q = np.arange(8)
    turn = 2.0 * math.pi / NS * (s[:, None] * q[None, :])
    twiddles = np.concatenate([np.cos(turn), np.sin(turn)], 1).astype(np.float32)
    return x_high, x_low, y_high, y_low, phases, twiddles


def split(value):
    high = value.astype(BF16)
    return high, (value - high.astype(F32)).astype(BF16)


def flip(index, bits):
    total = 0
    for unit in (1, 2, 4):
        bit = lax.rem(lax.div(index, unit), 2)
        total = total + unit * ((1 - bit) if bits & unit else bit)
    return total


def kernel(modes_in, scalar, obstacle, x_high_in, x_low_in, y_high_in, y_low_in, phases_in, twiddles_in, out,
           modes, row_zero, extra, arrived, x_high, x_low, y_high, y_low, phases, twiddles, lhs, lone, lone_sent, lone_row, sent, spectra, rhs, waves, twist, fields, velocity,
           padded, edges_out, edges_in, planes, base, slopes,
           table_sem, mode_sem, extra_sem, lone_sem, spectra_sem, velocity_sem, halo_sem, plane_sem, send_sem, ready_sem):
    sec, row, col = lax.axis_index("sec"), lax.axis_index("row"), lax.axis_index("col")

    pairs = ((modes_in, modes), (scalar.at[0], padded.at[pl.ds(8, 256)]), (twiddles_in, twiddles), (phases_in, phases),
             (x_high_in, x_high), (x_low_in, x_low), (y_high_in, y_high), (y_low_in, y_low))
    loads = [pltpu.make_async_copy(here, there, table_sem.at[i]) for i, (here, there) in enumerate(pairs)]
    for load in loads:
        load.start()

    barrier = pltpu.get_barrier_semaphore()

    def at_row(i):
        return (sec, lax.rem(row + i, ROWS), col)

    def at_col(i):
        return (sec, row, lax.rem(col + i, COLS))

    greeted = [at_col(i) for i in range(1, 8)] + [(sec, 7 - row, lax.rem(col + i, COLS)) for i in range(8)]
    greeted += [(sec, flip(row, i), c) for i in range(1, 7) for c in (col, 7 - col)]
    for device in greeted:
        pl.semaphore_signal(barrier, inc=1, device_id=device, device_id_type=MESH)
    for step in (1, 3):
        pl.semaphore_signal(barrier, inc=1, device_id=(lax.rem(sec + step, SECS), row, col), device_id_type=MESH)

    lead = (col, col, row)
    follow = (row, row, col)
    upper = [lax.div(f, 4) for f in follow]
    group = [f + u * (7 - 2 * f) for f, u in zip(follow, upper)]

    def device_at(p, f, l):
        return (sec, f, l) if p < 2 else (sec, l, f)

    loads[0].wait()
    for part in range(2):
        modes[2, part, 0] = modes[2, part, 0].T
    ahead = lax.broadcasted_iota(jnp.int32, (128, 128), 0) + lax.broadcasted_iota(jnp.int32, (128, 128), 1)
    mirror = jnp.where(ahead == 128, 1.0, 0.0).astype(F32)

    def turn_round(p):
        def go():
            for part in range(2):
                block = modes[p, part, 0]
                row_zero[p, part:part + 1] = block[0:1]
                modes[p, part, 0] = jnp.dot(mirror, block, precision=lax.Precision.HIGHEST, preferred_element_type=F32)
        return go

    for p in ORDER:
        pl.when(follow[p] >= 4)(turn_round(p))
    pl.semaphore_wait(barrier, 29)
    for i in (1, 2, 3):
        pl.semaphore_signal(ready_sem, inc=1, device_id=(sec, flip(row, i), col), device_id_type=MESH)

    for p in ORDER:
        slot = 8 * upper[p] + lead[p]
        for i in range(8):
            other = lax.rem(lead[p] + i, 8)
            for f in ((follow[p], 7 - follow[p]) if i else (7 - follow[p],)):
                pltpu.make_async_remote_copy(
                    modes.at[p, :, 0, pl.ds(pl.multiple_of(8 * (2 * other + lax.div(f, 4)), 8), 8), :], arrived.at[p, slot],
                    send_sem.at[0], mode_sem.at[p], device_id=device_at(p, f, other), device_id_type=MESH).start()

    def plane_copies(piece):
        rows = pl.ds(sum(PIECES[:piece]), PIECES[piece])
        return [pltpu.make_async_remote_copy(
            scalar.at[0, rows], planes.at[i, rows], send_sem.at[15 + 2 * piece + i], plane_sem.at[2 * piece + i],
            device_id=(lax.rem(sec + step, SECS), row, col), device_id_type=MESH) for i, step in enumerate((1, 3))]

    has_above, has_below = sec < SECS - 1, sec > 0

    def send_planes(piece):
        if PIECES[piece]:
            up, down = plane_copies(piece)
            pl.when(has_above)(up.start)
            pl.when(has_below)(down.start)

    send_planes(0)

    loads[1].wait()
    edges_out[0] = padded[pl.ds(8, 256), pl.ds(128, 128)].T[120:128]
    edges_out[1] = padded[pl.ds(8, 256), pl.ds(0, 128)].T[0:8]
    halo_copies = (
        pltpu.make_async_remote_copy(scalar.at[0, pl.ds(248, 8)], padded.at[pl.ds(0, 8)], send_sem.at[3], halo_sem.at[0],
                                     device_id=at_row(1), device_id_type=MESH),
        pltpu.make_async_remote_copy(scalar.at[0, pl.ds(0, 8)], padded.at[pl.ds(264, 8)], send_sem.at[4], halo_sem.at[1],
                                     device_id=at_row(7), device_id_type=MESH),
        pltpu.make_async_remote_copy(edges_out.at[0], edges_in.at[0], send_sem.at[5], halo_sem.at[2],
                                     device_id=at_col(1), device_id_type=MESH),
        pltpu.make_async_remote_copy(edges_out.at[1], edges_in.at[1], send_sem.at[6], halo_sem.at[3],
                                     device_id=at_col(7), device_id_type=MESH),
    )
    for copy in halo_copies:
        copy.start()

    loads[2].wait()
    for q in range(1, 8):
        twist[0, q - 1] = jnp.broadcast_to(twiddles[:, q:q + 1], (256, 128))
        twist[1, q - 1] = jnp.broadcast_to(twiddles[:, 8 + q:9 + q], (256, 128))
    for p in range(3):
        own = 2 * lead[p] + upper[p]
        arrived[p, 8 * upper[p] + lead[p]] = modes[p, :, 0, pl.ds(pl.multiple_of(8 * own, 8), 8), :]
    for load in loads[3:]:
        load.wait()
    pl.semaphore_wait(ready_sem, 3)

    @pl.when(sec == 0)
    def _():
        planes[0] = jnp.zeros((256, 256), F32)

    @pl.when(sec == SECS - 1)
    def _():
        planes[1] = jnp.zeros((256, 256), F32)

    def send_zero(p):
        return pltpu.make_async_remote_copy(
            row_zero.at[p], extra.at[p, lead[p]], send_sem.at[11 + p], extra_sem.at[p],
            device_id=device_at(p, lax.rem(8 - follow[p], 4), 0), device_id_type=MESH)

    for p in ORDER:
        pl.when(follow[p] >= 4)(send_zero(p).start)
    first = (row == 0) & (col == 0)
    sublane = lax.broadcasted_iota(jnp.int32, (8, 128), 0)
    special = sublane < jnp.where(first, 1, 0)

    def owners_of(p, block, half):
        if p < 2:
            return [(sec, 2 * (2 * p + half) + lax.rem(lax.div(block, 2), 2), block)]
        return [(sec, block, 4 * half + 2 * (1 - lax.rem(block, 2)) + side) for side in range(2)]

    plain_owner = lax.rem(row + lax.div(col, 2), 2) == 0
    chunk = lax.div(row, 2)
    own_half = jnp.where(plain_owner, lax.rem(chunk, 2), lax.div(col, 4))
    own_part = jnp.where(plain_owner, lax.div(chunk, 2), 2)

    for p in ORDER:
        some = arrived.at[p, pl.ds(0, 15)]
        pltpu.make_async_copy(some, some, mode_sem.at[p]).wait()

        @pl.when((lead[p] == 0) & (follow[p] < 4))
        def _():
            pltpu.make_async_copy(extra.at[p], extra.at[p], extra_sem.at[p]).wait()
            for a in range(8):
                for part in range(2):
                    arrived[p, 8 + a, part, 0:1] = jnp.where(follow[p] > 0, extra[p, a, part:part + 1], 0.0)

        for a in range(8):
            plus, minus = arrived[p, a], arrived[p, 8 + a]
            sum_real, sum_imag = plus[0] + minus[0], plus[1] + minus[1]
            gap_real = jnp.where(special, extra[p, a, 1:2], plus[0] - minus[0])
            gap_imag = jnp.where(special, -extra[p, a, 0:1], plus[1] - minus[1])
            for block in range(8):
                cosine, sine = phases[block:block + 1, :], phases[8 + block:9 + block, :]
                if block == 0:
                    a_real, a_imag, b_real, b_imag = sum_real, sum_imag, gap_real, gap_imag
                else:
                    a_real, a_imag = sum_real * cosine - sum_imag * sine, sum_real * sine + sum_imag * cosine
                    b_real, b_imag = gap_real * cosine - gap_imag * sine, gap_real * sine + gap_imag * cosine
                for part, tile in enumerate(((a_real, -b_imag), (-a_imag, -b_real))):
                    high, low = split(jnp.concatenate(tile, 0))
                    lhs[pl.ds(16 * block, 16), pl.ds(1024 * part + 128 * a, 128)] = high
                    lhs[pl.ds(128 + 16 * block, 16), pl.ds(1024 * part + 128 * a, 128)] = low
        main = jnp.dot(lhs[...], x_high[...], preferred_element_type=F32)
        rest = jnp.dot(lhs[pl.ds(0, 128), :], x_low[...], preferred_element_type=F32)
        total = main[:128] + main[128:] + rest
        for block in range(8):
            for half in range(2):
                tile = total[16 * block:16 * block + 16, 128 * half:128 * half + 128]
                sent[p, block, half, 0] = tile[:8]
                sent[p, block, half, 1] = tile[8:]

        rows = pl.ds(pl.multiple_of(8 * (16 * group[p] + 2 * lead[p] + upper[p]), 8), 8)
        for i in range(8):
            block = lax.rem(lead[p] + i, 8)
            for half in range(2):
                for target in owners_of(p, block, half):
                    mine = target[1 if p < 2 else 2] == follow[p]

                    def away():
                        pltpu.make_async_remote_copy(
                            sent.at[p, block, half], spectra.at[:, rows, :], send_sem.at[1], spectra_sem,
                            device_id=target, device_id_type=MESH).start()

                    if i > 0:
                        away()
                    else:
                        pl.when(jnp.logical_not(mine))(away)

                        @pl.when(mine)
                        def _():
                            spectra[:, rows, :] = sent[p, block, half]

        if p == ORDER[0]:
            send_planes(1)
    send_planes(2)

    @pl.when(first)
    def _():
        lone[...] = jnp.zeros_like(lone)
        for p in range(3):
            for a in range(8):
                real, imag = extra[p, a, 0:1], extra[p, a, 1:2]
                cosine, sine = phases[0:8, :], phases[8:16, :]
                lone[8 * p:8 * p + 8, pl.ds(128 * a, 128)] = real * sine + imag * cosine
                lone[8 * p:8 * p + 8, pl.ds(1024 + 128 * a, 128)] = real * cosine - imag * sine
        high, low = split(lone[...])
        total = (jnp.dot(high, x_high[...], preferred_element_type=F32) + jnp.dot(low, x_high[...], preferred_element_type=F32)
                 + jnp.dot(high, x_low[...], preferred_element_type=F32))
        def lone_tile(parts, block):
            strip = [total[8 * p + block:8 * p + block + 1, 128 * half:128 * half + 128] for p in parts for half in range(2)]
            blank = jnp.zeros((1, 128), F32)
            strip = strip + [blank] * 4 if len(parts) == 2 else [blank] * 4 + strip + [blank] * 2
            return jnp.concatenate(strip, 0)

        by_col = [lone_tile((0, 1), c) for c in range(8)]
        for r in range(8):
            by_row = lone_tile((2,), r)
            for c in range(8):
                if r == c == 0:
                    lone_row[...] = by_col[c] + by_row
                    continue
                lone_sent[8 * r + c] = by_col[c] + by_row
                pltpu.make_async_remote_copy(
                    lone_sent.at[8 * r + c], lone_row, send_sem.at[14], lone_sem,
                    device_id=(sec, r, c), device_id_type=MESH).start()

    for copy in halo_copies:
        copy.wait()
    left_edge = edges_in[0].T[:, 7:8]
    right_edge = edges_in[1].T[:, 0:1]
    lane = lax.broadcasted_iota(jnp.int32, (128, 256), 1)
    for block in range(2):
        at = 8 + 128 * block
        here = padded[pl.ds(at, 128), :]
        left = jnp.where(lane == 0, left_edge[128 * block:128 * block + 128], pltpu.roll(here, 1, 1))
        right = jnp.where(lane == 255, right_edge[128 * block:128 * block + 128], pltpu.roll(here, 255, 1))
        back = padded[pl.ds(at - 1, 128), :]
        front = padded[pl.ds(at + 1, 128), :]
        flag = jnp.where(lane < 128, obstacle[0, block, 0].astype(F32), obstacle[0, block, 1].astype(F32))
        rows = pl.ds(128 * block, 128)
        slopes[0, rows, :] = right - left
        slopes[1, rows, :] = front - back
        base[rows, :] = here + 0.04 * (left + right + back + front - 6.0 * here) - 0.25 * flag * (here - 1.0)

    pltpu.make_async_copy(spectra.at[:, pl.ds(0, 504), :], spectra.at[:, pl.ds(0, 504), :], spectra_sem).wait()
    send_planes(3)
    for q in range(8):
        for part in range(2):
            high, low = split(spectra[part, pl.ds(q, 64, stride=8), :])
            rhs[pl.ds(64 * part, 64), pl.ds(128 * q, 128)] = high
            rhs[pl.ds(128 + 64 * part, 64), pl.ds(128 * q, 128)] = low
    waves[...] = (jnp.dot(y_high[...], rhs[...], preferred_element_type=F32)
                  + jnp.dot(y_low[...], rhs[pl.ds(0, 128), :], preferred_element_type=F32))

    quarter = lax.rem(lax.broadcasted_iota(jnp.int32, (16, 128), 0), 4)
    lone_real = jnp.where(quarter == 0, 1.0, jnp.where(quarter == 2, -1.0, 0.0)) * spectra[1, 0:1, :]

    def combine(i, carry):
        at = pl.multiple_of(16 * i, 16)
        rows = pl.ds(at, 16)
        real, imag = [], []
        for q in range(8):
            re = waves[rows, pl.ds(128 * q, 128)]
            if q == 0:
                real.append(re + lone_real)
                imag.append(None)
                continue
            im = waves[pl.ds(256 + at, 16), pl.ds(128 * q, 128)]
            cosine, sine = twist[0, q - 1, rows, :], twist[1, q - 1, rows, :]
            real.append(re * cosine - im * sine)
            imag.append(None if q == 4 else re * sine + im * cosine)
        a1, b1 = real[1] + real[7], imag[1] - imag[7]
        a2, b2 = real[2] + real[6], imag[2] - imag[6]
        a3, b3 = real[3] + real[5], imag[3] - imag[5]
        even, odd = real[0] + real[4], real[0] - real[4]
        e0, e2, e1, e3 = even + a2, even - a2, odd - b2, odd + b2
        d0, d2 = a1 + a3, b3 - b1
        amid, bmid = HALF_ROOT * (a1 - a3), HALF_ROOT * (b1 + b3)
        d1, d3 = amid - bmid, -amid - bmid
        for r, (e, d) in enumerate(((e0, d0), (e1, d1), (e2, d2), (e3, d3))):
            fields[r, rows, :] = e + d
            fields[r + 4, rows, :] = e - d
        return carry

    lax.fori_loop(0, 16, combine, 0)

    def send_fields(number, peers, steps):
        def go():
            for i in steps:
                peer = lax.rem(number + i, 8)
                pltpu.make_async_remote_copy(
                    fields.at[peer], velocity.at[own_part, own_half], send_sem.at[2], velocity_sem.at[own_part],
                    device_id=peers(i), device_id_type=MESH).start()
            velocity[own_part, own_half] = fields[number]
        return go

    pl.when(plain_owner)(send_fields(row, at_row, range(1, 8)))
    pl.when(jnp.logical_not(plain_owner))(send_fields(col, at_col, (2, 4, 6)))

    pieces = [piece for piece in range(4) if PIECES[piece]]
    for piece in pieces:
        up, down = plane_copies(piece)
        pl.when(has_below)(up.wait_recv)
        pl.when(has_above)(down.wait_recv)
    slopes[2] = planes[1] - planes[0]
    base[...] = base[...] + 0.04 * (planes[1] + planes[0])

    for p in range(3):
        one = pltpu.make_async_copy(velocity.at[p, 0], velocity.at[p, 0], velocity_sem.at[p])
        two = pltpu.make_async_copy(velocity.at[p], velocity.at[p], velocity_sem.at[p])
        pl.when(own_part == p)(one.wait)
        pl.when(own_part != p)(two.wait)
    @pl.when(jnp.logical_not(first))
    def _():
        pltpu.make_async_copy(lone_row, lone_row, lone_sem).wait()

    quarter = lax.rem(lax.broadcasted_iota(jnp.int32, (256, 128), 0), 4)
    swing = jnp.where(quarter == 1, 1.0, jnp.where(quarter == 3, -1.0, 0.0))

    def field(p, half):
        return velocity[p, half] + swing * lone_row[2 * p + half:2 * p + half + 1, :]

    turned = [field(2, half).T for half in range(2)]
    for block in range(2):
        lanes = pl.ds(128 * block, 128)
        partial = field(0, block) * slopes[0, :, lanes] + field(1, block) * slopes[1, :, lanes]
        for half in range(2):
            rows = pl.ds(128 * half, 128)
            out[0, rows, lanes] = base[rows, lanes] - 0.125 * (
                partial[128 * half:128 * half + 128] + turned[half][:, 128 * block:128 * block + 128] * slopes[2, rows, lanes])

    sent_modes = arrived.at[:, pl.ds(0, 15)]
    pltpu.make_async_copy(sent_modes, sent_modes, send_sem.at[0]).wait()

    some = spectra.at[:, pl.ds(0, 63 * 8), :]
    pltpu.make_async_copy(some, some, send_sem.at[1]).wait()

    def fields_left(count):
        most = fields.at[pl.ds(0, count)]
        return pltpu.make_async_copy(most, most, send_sem.at[2]).wait

    pl.when(plain_owner)(fields_left(7))
    pl.when(jnp.logical_not(plain_owner))(fields_left(3))

    for p in range(3):
        pl.when(follow[p] >= 4)(send_zero(p).wait_send)

    @pl.when(first)
    def _():
        some = lone_sent.at[pl.ds(1, 63)]
        pltpu.make_async_copy(some, some, send_sem.at[14]).wait()

    for piece in pieces:
        up, down = plane_copies(piece)
        pl.when(has_above)(up.wait_send)
        pl.when(has_below)(down.wait_send)


def body(modes, scalar, obstacle):
    x_high, x_low, y_high, y_low, phases, twiddles = (jnp.asarray(t) for t in tables())
    anywhere = pl.BlockSpec(memory_space=pl.ANY)
    vmem = pl.BlockSpec(memory_space=pltpu.VMEM)
    smem = pl.BlockSpec(memory_space=pltpu.SMEM)
    dma = pltpu.SemaphoreType.DMA
    return pl.pallas_call(
        kernel,
        out_shape=pltpu.VMEM((1, 256, 256), F32),
        in_specs=[anywhere, anywhere, smem] + [anywhere] * 6,
        out_specs=vmem,
        scratch_shapes=[
            pltpu.VMEM((3, 2, 1, 128, 128), F32),
            pltpu.VMEM((3, 8, 128), F32),
            pltpu.VMEM((3, 8, 8, 128), F32),
            pltpu.VMEM((3, 16, 2, 8, 128), F32),
            pltpu.VMEM((2048, 256), BF16),
            pltpu.VMEM((2048, 256), BF16),
            pltpu.VMEM((512, 256), BF16),
            pltpu.VMEM((512, 128), BF16),
            pltpu.VMEM((16, 128), F32),
            pltpu.VMEM((256, 16), F32),
            pltpu.VMEM((256, 2048), BF16),
            pltpu.VMEM((32, 2048), F32),
            pltpu.VMEM((64, 8, 128), F32),
            pltpu.VMEM((8, 128), F32),
            pltpu.VMEM((3, 8, 2, 2, 8, 128), F32),
            pltpu.VMEM((2, 512, 128), F32),
            pltpu.VMEM((256, 1024), BF16),
            pltpu.VMEM((512, 1024), F32),
            pltpu.VMEM((2, 7, 256, 128), F32),
            pltpu.VMEM((8, 256, 128), F32),
            pltpu.VMEM((3, 2, 256, 128), F32),
            pltpu.VMEM((272, 256), F32),
            pltpu.VMEM((2, 8, 256), F32),
            pltpu.VMEM((2, 8, 256), F32),
            pltpu.VMEM((2, 256, 256), F32),
            pltpu.VMEM((256, 256), F32),
            pltpu.VMEM((3, 256, 256), F32),
            dma((8,)), dma((3,)), dma((3,)), dma, dma, dma((3,)), dma((4,)), dma((8,)), dma((23,)), pltpu.SemaphoreType.REGULAR,
        ],
        compiler_params=pltpu.CompilerParams(
            collective_id=0, has_side_effects=True, vmem_limit_bytes=56 * 1024 * 1024),
    )(modes, scalar, obstacle, x_high, x_low, y_high, y_low, phases, twiddles)


def solution(mesh):
    in_specs = (P(None, None, "sec", "row", "col"), P("sec", "row", "col"), P("sec", "row", "col"))
    out_specs = P("sec", "row", "col")
    return jax.shard_map(body, mesh=mesh, in_specs=in_specs, out_specs=out_specs, check_vma=False)
```

```python
import math

import jax
import jax.numpy as jnp
import numpy as np
from jax import lax
from jax.experimental import pallas as pl
from jax.experimental.pallas import tpu as pltpu
from jax.sharding import PartitionSpec as P

NV = 1024
NS = 2048
ROWS = 8
COLS = 8
SECS = 4
FAR_FIRST = (4, 5, 3, 2, 6, 1, 7)
PIECES = (48,0,32,176)
ORDER = (0,1,2)
F32 = jnp.float32
BF16 = jnp.bfloat16
MESH = pl.DeviceIdType.MESH
HALF_ROOT = math.sqrt(0.5)


def split_pair(table):
    high = table.astype(BF16)
    low = (table - high.astype(np.float64)).astype(BF16)
    return high, low


def tables():
    k = np.arange(NV)
    k = np.where(k < NV // 2, k, k - NV)
    s = np.arange(256)
    turn = 2.0 * math.pi / NS * ((k[:, None] * s[None, :]) % NS)
    x_high, x_low = split_pair(np.concatenate([np.cos(turn), np.sin(turn)], 0))
    m = np.arange(64)
    turn = 2.0 * math.pi / 256 * ((s[:, None] * m[None, :]) % 256)
    c, d = np.cos(turn), np.sin(turn)
    y_high, y_low = split_pair(np.block([[c, d], [d, -c]]))
    y_high = np.concatenate([y_high, y_high], 1)
    lanes = np.arange(128)
    turn = 2.0 * math.pi / 8 * ((np.arange(8)[:, None] * lanes[None, :]) % 8)
    phases = np.concatenate([np.cos(turn), np.sin(turn)], 0).astype(np.float32)
    q = np.arange(8)
    turn = 2.0 * math.pi / NS * (s[:, None] * q[None, :])
    twiddles = np.concatenate([np.cos(turn), np.sin(turn)], 1).astype(np.float32)
    return x_high, x_low, y_high, y_low, phases, twiddles


def split(value):
    high = value.astype(BF16)
    return high, (value - high.astype(F32)).astype(BF16)


def flip(index, bits):
    total = 0
    for unit in (1, 2, 4):
        bit = lax.rem(lax.div(index, unit), 2)
        total = total + unit * ((1 - bit) if bits & unit else bit)
    return total


def kernel(modes_in, scalar, obstacle, x_high_in, x_low_in, y_high_in, y_low_in, phases_in, twiddles_in, out,
           modes, row_zero, extra, arrived, x_high, x_low, y_high, y_low, phases, twiddles, lhs, lone, lone_sent, lone_row, sent, spectra, rhs, waves, twist, fields, velocity,
           padded, edges_out, edges_in, planes, base, slopes,
           table_sem, mode_sem, extra_sem, lone_sem, spectra_sem, velocity_sem, halo_sem, plane_sem, send_sem, ready_sem):
    sec, row, col = lax.axis_index("sec"), lax.axis_index("row"), lax.axis_index("col")

    barrier = pltpu.get_barrier_semaphore()

    def at_row(i):
        return (sec, lax.rem(row + i, ROWS), col)

    def at_col(i):
        return (sec, row, lax.rem(col + i, COLS))

    greeted = [(sec, 7 - row, lax.rem(col + i, COLS)) for i in FAR_FIRST + (0,)]
    greeted += [(sec, flip(row, i), c) for c in (7 - col, col) for i in range(6, 0, -1)]
    greeted += [at_col(i) for i in FAR_FIRST]
    for device in greeted:
        pl.semaphore_signal(barrier, inc=1, device_id=device, device_id_type=MESH)
    @pl.when((col == 0) & (row < 4))
    def _():
        for i in range(8):
            pl.semaphore_signal(barrier, inc=1, device_id=(sec, jnp.where(row > 0, 8 - row, 4), i), device_id_type=MESH)

    @pl.when((row == 0) & (col < 4))
    def _():
        for i in range(8):
            pl.semaphore_signal(barrier, inc=1, device_id=(sec, i, jnp.where(col > 0, 8 - col, 4)), device_id_type=MESH)

    has_above, has_below = sec < SECS - 1, sec > 0

    @pl.when(has_above)
    def _():
        pl.semaphore_signal(barrier, inc=1, device_id=(lax.rem(sec + 1, SECS), row, col), device_id_type=MESH)

    @pl.when(has_below)
    def _():
        pl.semaphore_signal(barrier, inc=1, device_id=(lax.rem(sec + SECS - 1, SECS), row, col), device_id_type=MESH)

    pairs = ((modes_in, modes), (scalar.at[0], padded.at[pl.ds(8, 256)]), (twiddles_in, twiddles), (phases_in, phases),
             (x_high_in, x_high), (x_low_in, x_low), (y_high_in, y_high), (y_low_in, y_low))
    loads = [pltpu.make_async_copy(here, there, table_sem.at[i]) for i, (here, there) in enumerate(pairs)]
    for load in loads:
        load.start()

    lead = (col, col, row)
    follow = (row, row, col)
    upper = [lax.div(f, 4) for f in follow]
    group = [f + u * (7 - 2 * f) for f, u in zip(follow, upper)]

    def device_at(p, f, l):
        return (sec, f, l) if p < 2 else (sec, l, f)

    loads[0].wait()
    for part in range(2):
        modes[2, part, 0] = modes[2, part, 0].T
    ahead = lax.broadcasted_iota(jnp.int32, (128, 128), 0) + lax.broadcasted_iota(jnp.int32, (128, 128), 1)
    mirror = jnp.where(ahead == 128, 1.0, 0.0).astype(F32)

    def turn_round(p):
        def go():
            for part in range(2):
                block = modes[p, part, 0]
                row_zero[p, part:part + 1] = block[0:1]
                modes[p, part, 0] = jnp.dot(mirror, block, precision=lax.Precision.HIGHEST, preferred_element_type=F32)
        return go

    for p in ORDER:
        pl.when(follow[p] >= 4)(turn_round(p))
    pl.semaphore_wait(barrier, 28 + lax.rem(lax.div(sec + 1, 2), 2) + lax.div(row, 4) + lax.div(col, 4))
    for i in (1, 2, 3):
        pl.semaphore_signal(ready_sem, inc=1, device_id=(sec, flip(row, i), col), device_id_type=MESH)

    def send_zero(p):
        return pltpu.make_async_remote_copy(
            row_zero.at[p], extra.at[p, lead[p]], send_sem.at[11 + p], extra_sem.at[p],
            device_id=device_at(p, lax.rem(8 - follow[p], 4), 0), device_id_type=MESH)

    for p in ORDER:
        pl.when(follow[p] >= 4)(send_zero(p).start)

    for p in ORDER:
        slot = 8 * upper[p] + lead[p]
        for i in FAR_FIRST + (0,):
            other = lax.rem(lead[p] + i, 8)
            for f in ((follow[p], 7 - follow[p]) if i else (7 - follow[p],)):
                pltpu.make_async_remote_copy(
                    modes.at[p, :, 0, pl.ds(pl.multiple_of(8 * (2 * other + lax.div(f, 4)), 8), 8), :], arrived.at[p, slot],
                    send_sem.at[0], mode_sem.at[p], device_id=device_at(p, f, other), device_id_type=MESH).start()

    def plane_copies(piece):
        rows = pl.ds(sum(PIECES[:piece]), PIECES[piece])
        return [pltpu.make_async_remote_copy(
            scalar.at[0, rows], planes.at[i, rows], send_sem.at[15 + 2 * piece + i], plane_sem.at[2 * piece + i],
            device_id=(lax.rem(sec + step, SECS), row, col), device_id_type=MESH) for i, step in enumerate((1, 3))]

    def send_planes(piece):
        if PIECES[piece]:
            up, down = plane_copies(piece)
            pl.when(has_above)(up.start)
            pl.when(has_below)(down.start)

    loads[1].wait()
    edges_out[0] = padded[pl.ds(8, 256), pl.ds(128, 128)].T[120:128]
    edges_out[1] = padded[pl.ds(8, 256), pl.ds(0, 128)].T[0:8]
    halo_copies = (
        pltpu.make_async_remote_copy(scalar.at[0, pl.ds(248, 8)], padded.at[pl.ds(0, 8)], send_sem.at[3], halo_sem.at[0],
                                     device_id=at_row(1), device_id_type=MESH),
        pltpu.make_async_remote_copy(scalar.at[0, pl.ds(0, 8)], padded.at[pl.ds(264, 8)], send_sem.at[4], halo_sem.at[1],
                                     device_id=at_row(7), device_id_type=MESH),
        pltpu.make_async_remote_copy(edges_out.at[0], edges_in.at[0], send_sem.at[5], halo_sem.at[2],
                                     device_id=at_col(1), device_id_type=MESH),
        pltpu.make_async_remote_copy(edges_out.at[1], edges_in.at[1], send_sem.at[6], halo_sem.at[3],
                                     device_id=at_col(7), device_id_type=MESH),
    )
    for copy in halo_copies:
        copy.start()

    loads[2].wait()
    for q in range(1, 8):
        twist[0, q - 1] = jnp.broadcast_to(twiddles[:, q:q + 1], (256, 128))
        twist[1, q - 1] = jnp.broadcast_to(twiddles[:, 8 + q:9 + q], (256, 128))
    for p in range(3):
        own = 2 * lead[p] + upper[p]
        arrived[p, 8 * upper[p] + lead[p]] = modes[p, :, 0, pl.ds(pl.multiple_of(8 * own, 8), 8), :]
    for load in loads[3:]:
        load.wait()
    pl.semaphore_wait(ready_sem, 3)

    @pl.when(sec == 0)
    def _():
        planes[0] = jnp.zeros((256, 256), F32)

    @pl.when(sec == SECS - 1)
    def _():
        planes[1] = jnp.zeros((256, 256), F32)

    first = (row == 0) & (col == 0)
    sublane = lax.broadcasted_iota(jnp.int32, (8, 128), 0)
    special = sublane < jnp.where(first, 1, 0)

    def owners_of(p, block, half):
        if p < 2:
            return [(sec, 2 * (2 * p + half) + lax.rem(lax.div(block, 2), 2), block)]
        return [(sec, block, 4 * half + 2 * (1 - lax.rem(block, 2)) + side) for side in range(2)]

    plain_owner = lax.rem(row + lax.div(col, 2), 2) == 0
    chunk = lax.div(row, 2)
    own_half = jnp.where(plain_owner, lax.rem(chunk, 2), lax.div(col, 4))
    own_part = jnp.where(plain_owner, lax.div(chunk, 2), 2)

    sent_modes = arrived.at[:, pl.ds(0, 15)]
    pltpu.make_async_copy(sent_modes, sent_modes, send_sem.at[0]).wait()
    send_planes(0)

    for p in ORDER:
        some = arrived.at[p, pl.ds(0, 15)]
        pltpu.make_async_copy(some, some, mode_sem.at[p]).wait()

        @pl.when((lead[p] == 0) & (follow[p] < 4))
        def _():
            pltpu.make_async_copy(extra.at[p], extra.at[p], extra_sem.at[p]).wait()
            for a in range(8):
                for part in range(2):
                    arrived[p, 8 + a, part, 0:1] = jnp.where(follow[p] > 0, extra[p, a, part:part + 1], 0.0)

        for a in range(8):
            plus, minus = arrived[p, a], arrived[p, 8 + a]
            sum_real, sum_imag = plus[0] + minus[0], plus[1] + minus[1]
            gap_real = jnp.where(special, extra[p, a, 1:2], plus[0] - minus[0])
            gap_imag = jnp.where(special, -extra[p, a, 0:1], plus[1] - minus[1])
            for block in range(8):
                cosine, sine = phases[block:block + 1, :], phases[8 + block:9 + block, :]
                if block == 0:
                    a_real, a_imag, b_real, b_imag = sum_real, sum_imag, gap_real, gap_imag
                else:
                    a_real, a_imag = sum_real * cosine - sum_imag * sine, sum_real * sine + sum_imag * cosine
                    b_real, b_imag = gap_real * cosine - gap_imag * sine, gap_real * sine + gap_imag * cosine
                for part, tile in enumerate(((a_real, -b_imag), (-a_imag, -b_real))):
                    high, low = split(jnp.concatenate(tile, 0))
                    lhs[pl.ds(16 * block, 16), pl.ds(1024 * part + 128 * a, 128)] = high
                    lhs[pl.ds(128 + 16 * block, 16), pl.ds(1024 * part + 128 * a, 128)] = low
        main = jnp.dot(lhs[...], x_high[...], preferred_element_type=F32)
        rest = jnp.dot(lhs[pl.ds(0, 128), :], x_low[...], preferred_element_type=F32)
        total = main[:128] + main[128:] + rest
        for block in range(8):
            for half in range(2):
                tile = total[16 * block:16 * block + 16, 128 * half:128 * half + 128]
                sent[p, block, half, 0] = tile[:8]
                sent[p, block, half, 1] = tile[8:]

        rows = pl.ds(pl.multiple_of(8 * (16 * group[p] + 2 * lead[p] + upper[p]), 8), 8)
        for i in FAR_FIRST + (0,):
            block = lax.rem(lead[p] + i, 8)
            for half in range(2):
                for target in owners_of(p, block, half):
                    mine = target[1 if p < 2 else 2] == follow[p]

                    def away():
                        pltpu.make_async_remote_copy(
                            sent.at[p, block, half], spectra.at[:, rows, :], send_sem.at[1], spectra_sem,
                            device_id=target, device_id_type=MESH).start()

                    if i > 0:
                        away()
                    else:
                        pl.when(jnp.logical_not(mine))(away)

                        @pl.when(mine)
                        def _():
                            spectra[:, rows, :] = sent[p, block, half]

        if p == ORDER[0]:
            send_planes(1)
        elif p == ORDER[1]:
            send_planes(2)

    @pl.when(first)
    def _():
        lone[...] = jnp.zeros_like(lone)
        for p in range(3):
            for a in range(8):
                real, imag = extra[p, a, 0:1], extra[p, a, 1:2]
                cosine, sine = phases[0:8, :], phases[8:16, :]
                lone[8 * p:8 * p + 8, pl.ds(128 * a, 128)] = real * sine + imag * cosine
                lone[8 * p:8 * p + 8, pl.ds(1024 + 128 * a, 128)] = real * cosine - imag * sine
        high, low = split(lone[...])
        total = (jnp.dot(high, x_high[...], preferred_element_type=F32) + jnp.dot(low, x_high[...], preferred_element_type=F32)
                 + jnp.dot(high, x_low[...], preferred_element_type=F32))
        def lone_tile(parts, block):
            strip = [total[8 * p + block:8 * p + block + 1, 128 * half:128 * half + 128] for p in parts for half in range(2)]
            blank = jnp.zeros((1, 128), F32)
            strip = strip + [blank] * 4 if len(parts) == 2 else [blank] * 4 + strip + [blank] * 2
            return jnp.concatenate(strip, 0)

        by_col = [lone_tile((0, 1), c) for c in range(8)]
        for r in range(8):
            by_row = lone_tile((2,), r)
            for c in range(8):
                if r == c == 0:
                    lone_row[...] = by_col[c] + by_row
                    continue
                lone_sent[8 * r + c] = by_col[c] + by_row
                pltpu.make_async_remote_copy(
                    lone_sent.at[8 * r + c], lone_row, send_sem.at[14], lone_sem,
                    device_id=(sec, r, c), device_id_type=MESH).start()

    for copy in halo_copies:
        copy.wait()
    left_edge = edges_in[0].T[:, 7:8]
    right_edge = edges_in[1].T[:, 0:1]
    lane = lax.broadcasted_iota(jnp.int32, (128, 256), 1)
    for block in range(2):
        at = 8 + 128 * block
        here = padded[pl.ds(at, 128), :]
        left = jnp.where(lane == 0, left_edge[128 * block:128 * block + 128], pltpu.roll(here, 1, 1))
        right = jnp.where(lane == 255, right_edge[128 * block:128 * block + 128], pltpu.roll(here, 255, 1))
        back = padded[pl.ds(at - 1, 128), :]
        front = padded[pl.ds(at + 1, 128), :]
        flag = jnp.where(lane < 128, obstacle[0, block, 0].astype(F32), obstacle[0, block, 1].astype(F32))
        rows = pl.ds(128 * block, 128)
        slopes[0, rows, :] = right - left
        slopes[1, rows, :] = front - back
        base[rows, :] = here + 0.04 * (left + right + back + front - 6.0 * here) - 0.25 * flag * (here - 1.0)

    pltpu.make_async_copy(spectra.at[:, pl.ds(0, 504), :], spectra.at[:, pl.ds(0, 504), :], spectra_sem).wait()
    send_planes(3)
    for q in range(8):
        for part in range(2):
            high, low = split(spectra[part, pl.ds(q, 64, stride=8), :])
            rhs[pl.ds(64 * part, 64), pl.ds(128 * q, 128)] = high
            rhs[pl.ds(128 + 64 * part, 64), pl.ds(128 * q, 128)] = low
    waves[...] = (jnp.dot(y_high[...], rhs[...], preferred_element_type=F32)
                  + jnp.dot(y_low[...], rhs[pl.ds(0, 128), :], preferred_element_type=F32))

    quarter = lax.rem(lax.broadcasted_iota(jnp.int32, (16, 128), 0), 4)
    lone_real = jnp.where(quarter == 0, 1.0, jnp.where(quarter == 2, -1.0, 0.0)) * spectra[1, 0:1, :]

    def combine(i, carry):
        at = pl.multiple_of(16 * i, 16)
        rows = pl.ds(at, 16)
        real, imag = [], []
        for q in range(8):
            re = waves[rows, pl.ds(128 * q, 128)]
            if q == 0:
                real.append(re + lone_real)
                imag.append(None)
                continue
            im = waves[pl.ds(256 + at, 16), pl.ds(128 * q, 128)]
            cosine, sine = twist[0, q - 1, rows, :], twist[1, q - 1, rows, :]
            real.append(re * cosine - im * sine)
            imag.append(None if q == 4 else re * sine + im * cosine)
        a1, b1 = real[1] + real[7], imag[1] - imag[7]
        a2, b2 = real[2] + real[6], imag[2] - imag[6]
        a3, b3 = real[3] + real[5], imag[3] - imag[5]
        even, odd = real[0] + real[4], real[0] - real[4]
        e0, e2, e1, e3 = even + a2, even - a2, odd - b2, odd + b2
        d0, d2 = a1 + a3, b3 - b1
        amid, bmid = HALF_ROOT * (a1 - a3), HALF_ROOT * (b1 + b3)
        d1, d3 = amid - bmid, -amid - bmid
        for r, (e, d) in enumerate(((e0, d0), (e1, d1), (e2, d2), (e3, d3))):
            fields[r, rows, :] = e + d
            fields[r + 4, rows, :] = e - d
        return carry

    lax.fori_loop(0, 16, combine, 0)

    def send_fields(number, peers, steps):
        def go():
            for i in steps:
                peer = lax.rem(number + i, 8)
                pltpu.make_async_remote_copy(
                    fields.at[peer], velocity.at[own_part, own_half], send_sem.at[2], velocity_sem.at[own_part],
                    device_id=peers(i), device_id_type=MESH).start()
            velocity[own_part, own_half] = fields[number]
        return go

    pl.when(plain_owner)(send_fields(row, at_row, FAR_FIRST))
    pl.when(jnp.logical_not(plain_owner))(send_fields(col, at_col, (4, 2, 6)))

    pieces = [piece for piece in range(4) if PIECES[piece]]
    for piece in pieces:
        up, down = plane_copies(piece)
        pl.when(has_below)(up.wait_recv)
        pl.when(has_above)(down.wait_recv)
    slopes[2] = planes[1] - planes[0]
    base[...] = base[...] + 0.04 * (planes[1] + planes[0])

    for p in range(3):
        one = pltpu.make_async_copy(velocity.at[p, 0], velocity.at[p, 0], velocity_sem.at[p])
        two = pltpu.make_async_copy(velocity.at[p], velocity.at[p], velocity_sem.at[p])
        pl.when(own_part == p)(one.wait)
        pl.when(own_part != p)(two.wait)
    @pl.when(jnp.logical_not(first))
    def _():
        pltpu.make_async_copy(lone_row, lone_row, lone_sem).wait()

    quarter = lax.rem(lax.broadcasted_iota(jnp.int32, (256, 128), 0), 4)
    swing = jnp.where(quarter == 1, 1.0, jnp.where(quarter == 3, -1.0, 0.0))

    def field(p, half):
        return velocity[p, half] + swing * lone_row[2 * p + half:2 * p + half + 1, :]

    turned = [field(2, half).T for half in range(2)]
    for block in range(2):
        lanes = pl.ds(128 * block, 128)
        partial = field(0, block) * slopes[0, :, lanes] + field(1, block) * slopes[1, :, lanes]
        for half in range(2):
            rows = pl.ds(128 * half, 128)
            out[0, rows, lanes] = base[rows, lanes] - 0.125 * (
                partial[128 * half:128 * half + 128] + turned[half][:, 128 * block:128 * block + 128] * slopes[2, rows, lanes])


    some = spectra.at[:, pl.ds(0, 63 * 8), :]
    pltpu.make_async_copy(some, some, send_sem.at[1]).wait()

    def fields_left(count):
        most = fields.at[pl.ds(0, count)]
        return pltpu.make_async_copy(most, most, send_sem.at[2]).wait

    pl.when(plain_owner)(fields_left(7))
    pl.when(jnp.logical_not(plain_owner))(fields_left(3))

    for p in range(3):
        pl.when(follow[p] >= 4)(send_zero(p).wait_send)

    @pl.when(first)
    def _():
        some = lone_sent.at[pl.ds(1, 63)]
        pltpu.make_async_copy(some, some, send_sem.at[14]).wait()

    for piece in pieces:
        up, down = plane_copies(piece)
        pl.when(has_above)(up.wait_send)
        pl.when(has_below)(down.wait_send)


def body(modes, scalar, obstacle):
    x_high, x_low, y_high, y_low, phases, twiddles = (jnp.asarray(t) for t in tables())
    anywhere = pl.BlockSpec(memory_space=pl.ANY)
    vmem = pl.BlockSpec(memory_space=pltpu.VMEM)
    smem = pl.BlockSpec(memory_space=pltpu.SMEM)
    dma = pltpu.SemaphoreType.DMA
    return pl.pallas_call(
        kernel,
        out_shape=pltpu.VMEM((1, 256, 256), F32),
        in_specs=[anywhere, anywhere, smem] + [anywhere] * 6,
        out_specs=vmem,
        scratch_shapes=[
            pltpu.VMEM((3, 2, 1, 128, 128), F32),
            pltpu.VMEM((3, 8, 128), F32),
            pltpu.VMEM((3, 8, 8, 128), F32),
            pltpu.VMEM((3, 16, 2, 8, 128), F32),
            pltpu.VMEM((2048, 256), BF16),
            pltpu.VMEM((2048, 256), BF16),
            pltpu.VMEM((512, 256), BF16),
            pltpu.VMEM((512, 128), BF16),
            pltpu.VMEM((16, 128), F32),
            pltpu.VMEM((256, 16), F32),
            pltpu.VMEM((256, 2048), BF16),
            pltpu.VMEM((32, 2048), F32),
            pltpu.VMEM((64, 8, 128), F32),
            pltpu.VMEM((8, 128), F32),
            pltpu.VMEM((3, 8, 2, 2, 8, 128), F32),
            pltpu.VMEM((2, 512, 128), F32),
            pltpu.VMEM((256, 1024), BF16),
            pltpu.VMEM((512, 1024), F32),
            pltpu.VMEM((2, 7, 256, 128), F32),
            pltpu.VMEM((8, 256, 128), F32),
            pltpu.VMEM((3, 2, 256, 128), F32),
            pltpu.VMEM((272, 256), F32),
            pltpu.VMEM((2, 8, 256), F32),
            pltpu.VMEM((2, 8, 256), F32),
            pltpu.VMEM((2, 256, 256), F32),
            pltpu.VMEM((256, 256), F32),
            pltpu.VMEM((3, 256, 256), F32),
            dma((8,)), dma((3,)), dma((3,)), dma, dma, dma((3,)), dma((4,)), dma((8,)), dma((23,)), pltpu.SemaphoreType.REGULAR,
        ],
        compiler_params=pltpu.CompilerParams(
            collective_id=0, has_side_effects=True, vmem_limit_bytes=56 * 1024 * 1024),
    )(modes, scalar, obstacle, x_high, x_low, y_high, y_low, phases, twiddles)


def solution(mesh):
    in_specs = (P(None, None, "sec", "row", "col"), P("sec", "row", "col"), P("sec", "row", "col"))
    out_specs = P("sec", "row", "col")
    return jax.shard_map(body, mesh=mesh, in_specs=in_specs, out_specs=out_specs, check_vma=False)
```

```python
import math

import jax
import jax.numpy as jnp
import numpy as np
from jax import lax
from jax.experimental import pallas as pl
from jax.experimental.pallas import tpu as pltpu
from jax.sharding import PartitionSpec as P

NV = 1024
NS = 2048
ROWS = 8
COLS = 8
SECS = 4
FAR_FIRST = (4, 5, 3, 2, 6, 1, 7)
PIECES = (32,32,64,128)
ORDER = (0,1,2)
F32 = jnp.float32
BF16 = jnp.bfloat16
MESH = pl.DeviceIdType.MESH
HALF_ROOT = math.sqrt(0.5)


def split_pair(table):
    high = table.astype(BF16)
    low = (table - high.astype(np.float64)).astype(BF16)
    return high, low


def tables():
    k = np.arange(NV)
    k = np.where(k < NV // 2, k, k - NV)
    s = np.arange(256)
    turn = 2.0 * math.pi / NS * ((k[:, None] * s[None, :]) % NS)
    x_high, x_low = split_pair(np.concatenate([np.cos(turn), np.sin(turn)], 0))
    m = np.arange(64)
    turn = 2.0 * math.pi / 256 * ((s[:, None] * m[None, :]) % 256)
    c, d = np.cos(turn), np.sin(turn)
    y_high, y_low = split_pair(np.block([[c, d], [d, -c]]))
    y_high = np.concatenate([y_high, y_high], 1)
    lanes = np.arange(128)
    turn = 2.0 * math.pi / 8 * ((np.arange(8)[:, None] * lanes[None, :]) % 8)
    phases = np.concatenate([np.cos(turn), np.sin(turn)], 0).astype(np.float32)
    q = np.arange(8)
    turn = 2.0 * math.pi / NS * (s[:, None] * q[None, :])
    twiddles = np.concatenate([np.cos(turn), np.sin(turn)], 1).astype(np.float32)
    return x_high, x_low, y_high, y_low, phases, twiddles


def split(value):
    high = value.astype(BF16)
    return high, (value - high.astype(F32)).astype(BF16)


def flip(index, bits):
    total = 0
    for unit in (1, 2, 4):
        bit = lax.rem(lax.div(index, unit), 2)
        total = total + unit * ((1 - bit) if bits & unit else bit)
    return total


def kernel(modes_in, scalar, obstacle, x_high_in, x_low_in, y_high_in, y_low_in, phases_in, twiddles_in, out,
           modes, row_zero, extra, arrived, twice, x_high, x_low, y_high, y_low, phases, twiddles, lhs, lone, lone_sent, lone_row, sent, sent_twice, spectra, rhs, waves, twist, fields, velocity,
           padded, edges_out, edges_in, planes, base, slopes,
           table_sem, mode_sem, extra_sem, lone_sem, spectra_sem, velocity_sem, halo_sem, plane_sem, send_sem, ready_sem, above_sem):
    sec, row, col = lax.axis_index("sec"), lax.axis_index("row"), lax.axis_index("col")

    barrier = pltpu.get_barrier_semaphore()

    def at_row(i):
        return (sec, lax.rem(row + i, ROWS), col)

    def at_col(i):
        return (sec, row, lax.rem(col + i, COLS))

    greeted = [(sec, 7 - row, lax.rem(col + i, COLS)) for i in FAR_FIRST + (0,)]
    greeted += [(sec, flip(row, i), c) for c in (7 - col, col) for i in range(6, 0, -1)]
    greeted += [at_col(i) for i in FAR_FIRST]
    for device in greeted:
        pl.semaphore_signal(barrier, inc=1, device_id=device, device_id_type=MESH)
    @pl.when((col == 0) & (row < 4))
    def _():
        for i in range(8):
            pl.semaphore_signal(barrier, inc=1, device_id=(sec, jnp.where(row > 0, 8 - row, 4), i), device_id_type=MESH)

    @pl.when(row == 0)
    def _():
        source = jnp.where(col < 4, jnp.where(col > 0, 8 - col, 4), jnp.where(col < 7, col + 1, 4))
        for i in range(8):
            pl.semaphore_signal(barrier, inc=1, device_id=(sec, i, source), device_id_type=MESH)

    has_above, has_below = sec < SECS - 1, sec > 0

    @pl.when(has_above)
    def _():
        pl.semaphore_signal(barrier, inc=1, device_id=(lax.rem(sec + 1, SECS), row, col), device_id_type=MESH)

    pairs = ((modes_in, modes), (scalar.at[0], padded.at[pl.ds(8, 256)]), (twiddles_in, twiddles), (phases_in, phases),
             (x_high_in, x_high), (x_low_in, x_low), (y_high_in, y_high), (y_low_in, y_low))
    loads = [pltpu.make_async_copy(here, there, table_sem.at[i]) for i, (here, there) in enumerate(pairs)]
    for load in loads:
        load.start()

    lead = (col, col, row)
    follow = (row, row, col)
    upper = [lax.div(f, 4) for f in follow]
    group = [f + u * (7 - 2 * f) for f, u in zip(follow, upper)]

    def device_at(p, f, l):
        return (sec, f, l) if p < 2 else (sec, l, f)

    loads[0].wait()
    for part in range(2):
        modes[2, part, 0] = modes[2, part, 0].T
    ahead = lax.broadcasted_iota(jnp.int32, (128, 128), 0) + lax.broadcasted_iota(jnp.int32, (128, 128), 1)
    mirror = jnp.where(ahead == 128, 1.0, 0.0).astype(F32)

    def turn_round(p):
        def go():
            for part in range(2):
                block = modes[p, part, 0]
                row_zero[p, part:part + 1] = block[0:1]
                modes[p, part, 0] = jnp.dot(mirror, block, precision=lax.Precision.HIGHEST, preferred_element_type=F32)
        return go

    for p in ORDER:
        pl.when(follow[p] >= 4)(turn_round(p))
    pl.semaphore_wait(barrier, 27 + lax.div(sec + 3, 4) + lax.div(row, 4) + 2 * lax.div(col, 4))

    @pl.when(has_below)
    def _():
        pl.semaphore_signal(above_sem, inc=1, device_id=(lax.rem(sec + SECS - 1, SECS), row, col), device_id_type=MESH)

    for i in (1, 2, 3):
        pl.semaphore_signal(ready_sem, inc=1, device_id=(sec, flip(row, i), col), device_id_type=MESH)

    def send_zero(p, copy=0):
        target = lax.rem(8 - follow[p], 4)
        return pltpu.make_async_remote_copy(
            row_zero.at[p], extra.at[p, lead[p]], send_sem.at[11 + p if copy == 0 else 23], extra_sem.at[p],
            device_id=device_at(p, target if copy == 0 else 7 - target, 0), device_id_type=MESH)

    zero_copies = ((0, 0), (1, 0), (2, 0), (2, 1))
    for p, copy in zero_copies:
        pl.when(follow[p] >= 4)(send_zero(p, copy).start)

    for p in ORDER:
        slot = 8 * upper[p] + lead[p]
        for i in FAR_FIRST + (0,):
            other = lax.rem(lead[p] + i, 8)
            for f in ((follow[p], 7 - follow[p]) if i else (7 - follow[p],)):
                pltpu.make_async_remote_copy(
                    modes.at[p, :, 0, pl.ds(pl.multiple_of(8 * (2 * other + lax.div(f, 4)), 8), 8), :] if p < 2
                    else modes.at[p, :, 0, pl.ds(pl.multiple_of(16 * other, 16), 16), :],
                    arrived.at[p, slot] if p < 2 else twice.at[slot],
                    send_sem.at[0], mode_sem.at[p], device_id=device_at(p, f, other), device_id_type=MESH).start()

    def plane_copies(piece):
        rows = pl.ds(sum(PIECES[:piece]), PIECES[piece])
        return [pltpu.make_async_remote_copy(
            scalar.at[0, rows], planes.at[i, rows], send_sem.at[15 + 2 * piece + i], plane_sem.at[2 * piece + i],
            device_id=(lax.rem(sec + step, SECS), row, col), device_id_type=MESH) for i, step in enumerate((1, 3))]

    def send_planes(piece):
        if PIECES[piece]:
            up, down = plane_copies(piece)
            pl.when(has_above)(up.start)
            pl.when(has_below)(down.start)

    loads[1].wait()
    edges_out[0] = padded[pl.ds(8, 256), pl.ds(128, 128)].T[120:128]
    edges_out[1] = padded[pl.ds(8, 256), pl.ds(0, 128)].T[0:8]
    halo_copies = (
        pltpu.make_async_remote_copy(scalar.at[0, pl.ds(248, 8)], padded.at[pl.ds(0, 8)], send_sem.at[3], halo_sem.at[0],
                                     device_id=at_row(1), device_id_type=MESH),
        pltpu.make_async_remote_copy(scalar.at[0, pl.ds(0, 8)], padded.at[pl.ds(264, 8)], send_sem.at[4], halo_sem.at[1],
                                     device_id=at_row(7), device_id_type=MESH),
        pltpu.make_async_remote_copy(edges_out.at[0], edges_in.at[0], send_sem.at[5], halo_sem.at[2],
                                     device_id=at_col(1), device_id_type=MESH),
        pltpu.make_async_remote_copy(edges_out.at[1], edges_in.at[1], send_sem.at[6], halo_sem.at[3],
                                     device_id=at_col(7), device_id_type=MESH),
    )
    for copy in halo_copies:
        copy.start()

    loads[2].wait()
    for q in range(1, 8):
        twist[0, q - 1] = jnp.broadcast_to(twiddles[:, q:q + 1], (256, 128))
        twist[1, q - 1] = jnp.broadcast_to(twiddles[:, 8 + q:9 + q], (256, 128))
    twice[8 * upper[2] + lead[2]] = modes[2, :, 0, pl.ds(pl.multiple_of(16 * lead[2], 16), 16), :]
    for p in range(2):
        own = 2 * lead[p] + upper[p]
        arrived[p, 8 * upper[p] + lead[p]] = modes[p, :, 0, pl.ds(pl.multiple_of(8 * own, 8), 8), :]
    for load in loads[3:]:
        load.wait()
    pl.semaphore_wait(ready_sem, 3)

    @pl.when(sec == 0)
    def _():
        planes[0] = jnp.zeros((256, 256), F32)

    @pl.when(sec == SECS - 1)
    def _():
        planes[1] = jnp.zeros((256, 256), F32)

    first = (row == 0) & (col == 0)

    def owners_of(p, block, half):
        if p < 2:
            return [(sec, 2 * (2 * p + half) + lax.rem(lax.div(block, 2), 2), block)]
        return [(sec, block, 4 * half + 2 * (1 - lax.rem(block, 2)) + side) for side in (lax.rem(col, 2),)]

    plain_owner = lax.rem(row + lax.div(col, 2), 2) == 0
    chunk = lax.div(row, 2)
    own_half = jnp.where(plain_owner, lax.rem(chunk, 2), lax.div(col, 4))
    own_part = jnp.where(plain_owner, lax.div(chunk, 2), 2)

    @pl.when(has_above)
    def _():
        pl.semaphore_wait(above_sem, 1)

    for p in ORDER:
        size = 8 if p < 2 else 16
        gathered = arrived.at[p] if p < 2 else twice
        some = gathered.at[pl.ds(0, 15)]
        pltpu.make_async_copy(some, some, mode_sem.at[p]).wait()
        if p == ORDER[0]:
            send_planes(0)

        @pl.when((lead[p] == 0) & (follow[p] < (4 if p < 2 else 8)))
        def _():
            pltpu.make_async_copy(extra.at[p], extra.at[p], extra_sem.at[p]).wait()
            for a in range(8):
                for part in range(2):
                    gathered[8 + a, part, 0:1] = jnp.where(group[p] > 0, extra[p, a, part:part + 1], 0.0)

        alone = jnp.where((lead[p] == 0) & (group[p] == 0) & (follow[p] < (4 if p < 2 else 8)), 1, 0)
        special = lax.broadcasted_iota(jnp.int32, (size, 128), 0) < alone
        for a in range(8):
            plus, minus = gathered[a], gathered[8 + a]
            sum_real, sum_imag = plus[0] + minus[0], plus[1] + minus[1]
            gap_real = jnp.where(special, extra[p, a, 1:2], plus[0] - minus[0])
            gap_imag = jnp.where(special, -extra[p, a, 0:1], plus[1] - minus[1])
            for block in range(8):
                cosine, sine = phases[block:block + 1, :], phases[8 + block:9 + block, :]
                if block == 0:
                    a_real, a_imag, b_real, b_imag = sum_real, sum_imag, gap_real, gap_imag
                else:
                    a_real, a_imag = sum_real * cosine - sum_imag * sine, sum_real * sine + sum_imag * cosine
                    b_real, b_imag = gap_real * cosine - gap_imag * sine, gap_real * sine + gap_imag * cosine
                for part, tile in enumerate(((a_real, -b_imag), (-a_imag, -b_real))):
                    high, low = split(jnp.concatenate(tile, 0))
                    lhs[pl.ds(2 * size * block, 2 * size), pl.ds(1024 * part + 128 * a, 128)] = high
                    lhs[pl.ds(2 * size * (8 + block), 2 * size), pl.ds(1024 * part + 128 * a, 128)] = low
        main = jnp.dot(lhs[pl.ds(0, 32 * size), :], x_high[...], preferred_element_type=F32)
        rest = jnp.dot(lhs[pl.ds(0, 16 * size), :], x_low[...], preferred_element_type=F32)
        total = main[:16 * size] + main[16 * size:] + rest
        results = sent.at[p] if p < 2 else sent_twice
        for block in range(8):
            for half in range(2):
                tile = total[2 * size * block:2 * size * (block + 1), 128 * half:128 * half + 128]
                results[block, half, 0] = tile[:size]
                results[block, half, 1] = tile[size:]

        place = 128 * group[p] + (8 * (2 * lead[p] + upper[p]) if p < 2 else 16 * lead[p])
        rows = pl.ds(pl.multiple_of(place, size), size)
        for i in FAR_FIRST + (0,):
            block = lax.rem(lead[p] + i, 8)
            for half in range(2):
                for target in owners_of(p, block, half):
                    mine = target[1 if p < 2 else 2] == follow[p]

                    def away():
                        pltpu.make_async_remote_copy(
                            results.at[block, half], spectra.at[:, rows, :], send_sem.at[1], spectra_sem,
                            device_id=target, device_id_type=MESH).start()

                    if i > 0:
                        away()
                    else:
                        pl.when(jnp.logical_not(mine))(away)

                        @pl.when(mine)
                        def _():
                            spectra[:, rows, :] = results[block, half]

        if p == ORDER[0]:
            send_planes(1)
    send_planes(2)

    @pl.when(first)
    def _():
        lone[...] = jnp.zeros_like(lone)
        for p in range(3):
            for a in range(8):
                real, imag = extra[p, a, 0:1], extra[p, a, 1:2]
                cosine, sine = phases[0:8, :], phases[8:16, :]
                lone[8 * p:8 * p + 8, pl.ds(128 * a, 128)] = real * sine + imag * cosine
                lone[8 * p:8 * p + 8, pl.ds(1024 + 128 * a, 128)] = real * cosine - imag * sine
        high, low = split(lone[...])
        total = (jnp.dot(high, x_high[...], preferred_element_type=F32) + jnp.dot(low, x_high[...], preferred_element_type=F32)
                 + jnp.dot(high, x_low[...], preferred_element_type=F32))
        def lone_tile(parts, block):
            strip = [total[8 * p + block:8 * p + block + 1, 128 * half:128 * half + 128] for p in parts for half in range(2)]
            blank = jnp.zeros((1, 128), F32)
            strip = strip + [blank] * 4 if len(parts) == 2 else [blank] * 4 + strip + [blank] * 2
            return jnp.concatenate(strip, 0)

        by_col = [lone_tile((0, 1), c) for c in range(8)]
        for r in range(8):
            by_row = lone_tile((2,), r)
            for c in range(8):
                if r == c == 0:
                    lone_row[...] = by_col[c] + by_row
                    continue
                lone_sent[8 * r + c] = by_col[c] + by_row
                pltpu.make_async_remote_copy(
                    lone_sent.at[8 * r + c], lone_row, send_sem.at[14], lone_sem,
                    device_id=(sec, r, c), device_id_type=MESH).start()

    for copy in halo_copies:
        copy.wait()
    left_edge = edges_in[0].T[:, 7:8]
    right_edge = edges_in[1].T[:, 0:1]
    lane = lax.broadcasted_iota(jnp.int32, (128, 256), 1)
    for block in range(2):
        at = 8 + 128 * block
        here = padded[pl.ds(at, 128), :]
        left = jnp.where(lane == 0, left_edge[128 * block:128 * block + 128], pltpu.roll(here, 1, 1))
        right = jnp.where(lane == 255, right_edge[128 * block:128 * block + 128], pltpu.roll(here, 255, 1))
        back = padded[pl.ds(at - 1, 128), :]
        front = padded[pl.ds(at + 1, 128), :]
        flag = jnp.where(lane < 128, obstacle[0, block, 0].astype(F32), obstacle[0, block, 1].astype(F32))
        rows = pl.ds(128 * block, 128)
        slopes[0, rows, :] = right - left
        slopes[1, rows, :] = front - back
        base[rows, :] = here + 0.04 * (left + right + back + front - 6.0 * here) - 0.25 * flag * (here - 1.0)

    def spectra_through(semaphore):
        for count, here in ((504, plain_owner), (496, jnp.logical_not(plain_owner))):
            some = spectra.at[:, pl.ds(0, count), :]
            pl.when(here)(pltpu.make_async_copy(some, some, semaphore).wait)

    spectra_through(spectra_sem)
    send_planes(3)
    for q in range(8):
        for part in range(2):
            high, low = split(spectra[part, pl.ds(q, 64, stride=8), :])
            rhs[pl.ds(64 * part, 64), pl.ds(128 * q, 128)] = high
            rhs[pl.ds(128 + 64 * part, 64), pl.ds(128 * q, 128)] = low
    waves[...] = (jnp.dot(y_high[...], rhs[...], preferred_element_type=F32)
                  + jnp.dot(y_low[...], rhs[pl.ds(0, 128), :], preferred_element_type=F32))

    quarter = lax.rem(lax.broadcasted_iota(jnp.int32, (16, 128), 0), 4)
    lone_real = jnp.where(quarter == 0, 1.0, jnp.where(quarter == 2, -1.0, 0.0)) * spectra[1, 0:1, :]

    def combine(i, carry):
        at = pl.multiple_of(16 * i, 16)
        rows = pl.ds(at, 16)
        real, imag = [], []
        for q in range(8):
            re = waves[rows, pl.ds(128 * q, 128)]
            if q == 0:
                real.append(re + lone_real)
                imag.append(None)
                continue
            im = waves[pl.ds(256 + at, 16), pl.ds(128 * q, 128)]
            cosine, sine = twist[0, q - 1, rows, :], twist[1, q - 1, rows, :]
            real.append(re * cosine - im * sine)
            imag.append(None if q == 4 else re * sine + im * cosine)
        a1, b1 = real[1] + real[7], imag[1] - imag[7]
        a2, b2 = real[2] + real[6], imag[2] - imag[6]
        a3, b3 = real[3] + real[5], imag[3] - imag[5]
        even, odd = real[0] + real[4], real[0] - real[4]
        e0, e2, e1, e3 = even + a2, even - a2, odd - b2, odd + b2
        d0, d2 = a1 + a3, b3 - b1
        amid, bmid = HALF_ROOT * (a1 - a3), HALF_ROOT * (b1 + b3)
        d1, d3 = amid - bmid, -amid - bmid
        for r, (e, d) in enumerate(((e0, d0), (e1, d1), (e2, d2), (e3, d3))):
            fields[r, rows, :] = e + d
            fields[r + 4, rows, :] = e - d
        return carry

    lax.fori_loop(0, 16, combine, 0)

    def send_fields(number, peers, steps):
        def go():
            for i in steps:
                peer = lax.rem(number + i, 8)
                pltpu.make_async_remote_copy(
                    fields.at[peer], velocity.at[own_part, own_half], send_sem.at[2], velocity_sem.at[own_part],
                    device_id=peers(i), device_id_type=MESH).start()
            velocity[own_part, own_half] = fields[number]
        return go

    pl.when(plain_owner)(send_fields(row, at_row, FAR_FIRST))
    pl.when(jnp.logical_not(plain_owner))(send_fields(col, at_col, (4, 2, 6)))

    pieces = [piece for piece in range(4) if PIECES[piece]]
    for piece in pieces:
        up, down = plane_copies(piece)
        pl.when(has_below)(up.wait_recv)
        pl.when(has_above)(down.wait_recv)
    slopes[2] = planes[1] - planes[0]
    base[...] = base[...] + 0.04 * (planes[1] + planes[0])

    for p in range(3):
        one = pltpu.make_async_copy(velocity.at[p, 0], velocity.at[p, 0], velocity_sem.at[p])
        two = pltpu.make_async_copy(velocity.at[p], velocity.at[p], velocity_sem.at[p])
        pl.when(own_part == p)(one.wait)
        pl.when(own_part != p)(two.wait)
    @pl.when(jnp.logical_not(first))
    def _():
        pltpu.make_async_copy(lone_row, lone_row, lone_sem).wait()

    quarter = lax.rem(lax.broadcasted_iota(jnp.int32, (256, 128), 0), 4)
    swing = jnp.where(quarter == 1, 1.0, jnp.where(quarter == 3, -1.0, 0.0))

    def field(p, half):
        return velocity[p, half] + swing * lone_row[2 * p + half:2 * p + half + 1, :]

    turned = [field(2, half).T for half in range(2)]
    for block in range(2):
        lanes = pl.ds(128 * block, 128)
        partial = field(0, block) * slopes[0, :, lanes] + field(1, block) * slopes[1, :, lanes]
        for half in range(2):
            rows = pl.ds(128 * half, 128)
            out[0, rows, lanes] = base[rows, lanes] - 0.125 * (
                partial[128 * half:128 * half + 128] + turned[half][:, 128 * block:128 * block + 128] * slopes[2, rows, lanes])

    sent_modes = spectra.at[:, pl.ds(0, 480), :]
    pltpu.make_async_copy(sent_modes, sent_modes, send_sem.at[0]).wait()

    spectra_through(send_sem.at[1])

    def fields_left(count):
        most = fields.at[pl.ds(0, count)]
        return pltpu.make_async_copy(most, most, send_sem.at[2]).wait

    pl.when(plain_owner)(fields_left(7))
    pl.when(jnp.logical_not(plain_owner))(fields_left(3))

    for p, copy in zero_copies:
        pl.when(follow[p] >= 4)(send_zero(p, copy).wait_send)

    @pl.when(first)
    def _():
        some = lone_sent.at[pl.ds(1, 63)]
        pltpu.make_async_copy(some, some, send_sem.at[14]).wait()

    for piece in pieces:
        up, down = plane_copies(piece)
        pl.when(has_above)(up.wait_send)
        pl.when(has_below)(down.wait_send)


def body(modes, scalar, obstacle):
    x_high, x_low, y_high, y_low, phases, twiddles = (jnp.asarray(t) for t in tables())
    anywhere = pl.BlockSpec(memory_space=pl.ANY)
    vmem = pl.BlockSpec(memory_space=pltpu.VMEM)
    smem = pl.BlockSpec(memory_space=pltpu.SMEM)
    dma = pltpu.SemaphoreType.DMA
    return pl.pallas_call(
        kernel,
        out_shape=pltpu.VMEM((1, 256, 256), F32),
        in_specs=[anywhere, anywhere, smem] + [anywhere] * 6,
        out_specs=vmem,
        scratch_shapes=[
            pltpu.VMEM((3, 2, 1, 128, 128), F32),
            pltpu.VMEM((3, 8, 128), F32),
            pltpu.VMEM((3, 8, 8, 128), F32),
            pltpu.VMEM((2, 16, 2, 8, 128), F32),
            pltpu.VMEM((16, 2, 16, 128), F32),
            pltpu.VMEM((2048, 256), BF16),
            pltpu.VMEM((2048, 256), BF16),
            pltpu.VMEM((512, 256), BF16),
            pltpu.VMEM((512, 128), BF16),
            pltpu.VMEM((16, 128), F32),
            pltpu.VMEM((256, 16), F32),
            pltpu.VMEM((512, 2048), BF16),
            pltpu.VMEM((32, 2048), F32),
            pltpu.VMEM((64, 8, 128), F32),
            pltpu.VMEM((8, 128), F32),
            pltpu.VMEM((2, 8, 2, 2, 8, 128), F32),
            pltpu.VMEM((8, 2, 2, 16, 128), F32),
            pltpu.VMEM((2, 512, 128), F32),
            pltpu.VMEM((256, 1024), BF16),
            pltpu.VMEM((512, 1024), F32),
            pltpu.VMEM((2, 7, 256, 128), F32),
            pltpu.VMEM((8, 256, 128), F32),
            pltpu.VMEM((3, 2, 256, 128), F32),
            pltpu.VMEM((272, 256), F32),
            pltpu.VMEM((2, 8, 256), F32),
            pltpu.VMEM((2, 8, 256), F32),
            pltpu.VMEM((2, 256, 256), F32),
            pltpu.VMEM((256, 256), F32),
            pltpu.VMEM((3, 256, 256), F32),
            dma((8,)), dma((3,)), dma((3,)), dma, dma, dma((3,)), dma((4,)), dma((8,)), dma((24,)), pltpu.SemaphoreType.REGULAR, pltpu.SemaphoreType.REGULAR,
        ],
        compiler_params=pltpu.CompilerParams(
            collective_id=0, has_side_effects=True, vmem_limit_bytes=56 * 1024 * 1024),
    )(modes, scalar, obstacle, x_high, x_low, y_high, y_low, phases, twiddles)


def solution(mesh):
    in_specs = (P(None, None, "sec", "row", "col"), P("sec", "row", "col"), P("sec", "row", "col"))
    out_specs = P("sec", "row", "col")
    return jax.shard_map(body, mesh=mesh, in_specs=in_specs, out_specs=out_specs, check_vma=False)
```

```python
import math

import jax
import jax.numpy as jnp
import numpy as np
from jax import lax
from jax.experimental import pallas as pl
from jax.experimental.pallas import tpu as pltpu
from jax.sharding import PartitionSpec as P

NV = 1024
NS = 2048
ROWS = 8
COLS = 8
SECS = 4
FAR_FIRST = (4, 5, 3, 2, 6, 1, 7)
PIECES = (32,0,96,128)
ORDER = (0,1,2)
F32 = jnp.float32
BF16 = jnp.bfloat16
MESH = pl.DeviceIdType.MESH
HALF_ROOT = math.sqrt(0.5)


def split_pair(table):
    high = table.astype(BF16)
    low = (table - high.astype(np.float64)).astype(BF16)
    return high, low


def tables():
    k = np.arange(NV)
    k = np.where(k < NV // 2, k, k - NV)
    s = np.arange(256)
    turn = 2.0 * math.pi / NS * ((k[:, None] * s[None, :]) % NS)
    x_high, x_low = split_pair(np.concatenate([np.cos(turn), np.sin(turn)], 0))
    m = np.arange(64)
    turn = 2.0 * math.pi / 256 * ((s[:, None] * m[None, :]) % 256)
    c, d = np.cos(turn), np.sin(turn)
    y_high, y_low = split_pair(np.concatenate([np.block([[c[h], d[h]], [d[h], -c[h]]]) for h in (slice(0, 128), slice(128, 256))], 0))
    y_high = np.concatenate([y_high, y_high], 1)
    lanes = np.arange(128)
    turn = 2.0 * math.pi / 8 * ((np.arange(8)[:, None] * lanes[None, :]) % 8)
    phases = np.concatenate([np.cos(turn), np.sin(turn)], 0).astype(np.float32)
    q = np.arange(8)
    turn = 2.0 * math.pi / NS * (s[:, None] * q[None, :])
    twiddles = np.concatenate([np.cos(turn), np.sin(turn)], 1).astype(np.float32)
    return x_high, x_low, y_high, y_low, phases, twiddles


def split(value):
    high = value.astype(BF16)
    return high, (value - high.astype(F32)).astype(BF16)


def flip(index, bits):
    total = 0
    for unit in (1, 2, 4):
        bit = lax.rem(lax.div(index, unit), 2)
        total = total + unit * ((1 - bit) if bits & unit else bit)
    return total


def kernel(modes_in, scalar, obstacle, x_high_in, x_low_in, y_high_in, y_low_in, phases_in, twiddles_in, out,
           modes, row_zero, extra, arrived, twice, x_high, x_low, y_high, y_low, phases, twiddles, lhs, lone, lone_sent, lone_row, sent, sent_twice, spectra, rhs, waves, twist, fields, velocity,
           padded, edges_out, edges_in, planes, base, slopes,
           table_sem, mode_sem, extra_sem, lone_sem, spectra_sem, velocity_sem, halo_sem, plane_sem, send_sem, ready_sem, above_sem):
    sec, row, col = lax.axis_index("sec"), lax.axis_index("row"), lax.axis_index("col")

    barrier = pltpu.get_barrier_semaphore()

    def at_row(i):
        return (sec, lax.rem(row + i, ROWS), col)

    def at_col(i):
        return (sec, row, lax.rem(col + i, COLS))

    greeted = [(sec, 7 - row, lax.rem(col + i, COLS)) for i in FAR_FIRST + (0,)]
    greeted += [(sec, flip(row, i), c) for c in (7 - col, col) for i in range(6, 0, -1)]
    greeted += [at_col(i) for i in FAR_FIRST]
    for device in greeted:
        pl.semaphore_signal(barrier, inc=1, device_id=device, device_id_type=MESH)
    @pl.when((col == 0) & (row < 4))
    def _():
        for i in range(8):
            pl.semaphore_signal(barrier, inc=1, device_id=(sec, jnp.where(row > 0, 8 - row, 4), i), device_id_type=MESH)

    @pl.when(row == 0)
    def _():
        source = jnp.where(col < 4, jnp.where(col > 0, 8 - col, 4), jnp.where(col < 7, col + 1, 4))
        for i in range(8):
            pl.semaphore_signal(barrier, inc=1, device_id=(sec, i, source), device_id_type=MESH)

    has_above, has_below = sec < SECS - 1, sec > 0

    @pl.when(has_above)
    def _():
        pl.semaphore_signal(barrier, inc=1, device_id=(lax.rem(sec + 1, SECS), row, col), device_id_type=MESH)

    pairs = ((modes_in, modes), (scalar.at[0], padded.at[pl.ds(8, 256)]), (twiddles_in, twiddles), (phases_in, phases),
             (x_high_in, x_high), (x_low_in, x_low), (y_high_in, y_high), (y_low_in, y_low))
    loads = [pltpu.make_async_copy(here, there, table_sem.at[i]) for i, (here, there) in enumerate(pairs)]
    for load in loads:
        load.start()

    lead = (col, col, row)
    follow = (row, row, col)
    upper = [lax.div(f, 4) for f in follow]
    group = [f + u * (7 - 2 * f) for f, u in zip(follow, upper)]

    def device_at(p, f, l):
        return (sec, f, l) if p < 2 else (sec, l, f)

    loads[0].wait()
    for part in range(2):
        modes[2, part, 0] = modes[2, part, 0].T
    ahead = lax.broadcasted_iota(jnp.int32, (128, 128), 0) + lax.broadcasted_iota(jnp.int32, (128, 128), 1)
    mirror = jnp.where(ahead == 128, 1.0, 0.0).astype(F32)

    def turn_round(p):
        def go():
            for part in range(2):
                block = modes[p, part, 0]
                row_zero[p, part:part + 1] = block[0:1]
                modes[p, part, 0] = jnp.dot(mirror, block, precision=lax.Precision.HIGHEST, preferred_element_type=F32)
        return go

    for p in ORDER:
        pl.when(follow[p] >= 4)(turn_round(p))
    pl.semaphore_wait(barrier, 27 + lax.div(sec + 3, 4) + lax.div(row, 4) + 2 * lax.div(col, 4))

    @pl.when(has_below)
    def _():
        pl.semaphore_signal(above_sem, inc=1, device_id=(lax.rem(sec + SECS - 1, SECS), row, col), device_id_type=MESH)

    for i in (1, 2, 3):
        pl.semaphore_signal(ready_sem, inc=1, device_id=(sec, flip(row, i), col), device_id_type=MESH)

    def send_zero(p, copy=0):
        target = lax.rem(8 - follow[p], 4)
        return pltpu.make_async_remote_copy(
            row_zero.at[p], extra.at[p, lead[p]], send_sem.at[11 + p if copy == 0 else 23], extra_sem.at[p],
            device_id=device_at(p, target if copy == 0 else 7 - target, 0), device_id_type=MESH)

    zero_copies = ((0, 0), (1, 0), (2, 0), (2, 1))
    for p, copy in zero_copies:
        pl.when(follow[p] >= 4)(send_zero(p, copy).start)

    for p in ORDER:
        slot = 8 * upper[p] + lead[p]
        for i in FAR_FIRST + (0,):
            other = lax.rem(lead[p] + i, 8)
            for f in ((follow[p], 7 - follow[p]) if i else (7 - follow[p],)):
                pltpu.make_async_remote_copy(
                    modes.at[p, :, 0, pl.ds(pl.multiple_of(8 * (2 * other + lax.div(f, 4)), 8), 8), :] if p < 2
                    else modes.at[p, :, 0, pl.ds(pl.multiple_of(16 * other, 16), 16), :],
                    arrived.at[p, slot] if p < 2 else twice.at[slot],
                    send_sem.at[0], mode_sem.at[p], device_id=device_at(p, f, other), device_id_type=MESH).start()

    def plane_copies(piece):
        rows = pl.ds(sum(PIECES[:piece]), PIECES[piece])
        return [pltpu.make_async_remote_copy(
            scalar.at[0, rows], planes.at[i, rows], send_sem.at[15 + 2 * piece + i], plane_sem.at[2 * piece + i],
            device_id=(lax.rem(sec + step, SECS), row, col), device_id_type=MESH) for i, step in enumerate((1, 3))]

    def send_planes(piece):
        if PIECES[piece]:
            up, down = plane_copies(piece)
            pl.when(has_above)(up.start)
            pl.when(has_below)(down.start)

    loads[1].wait()
    edges_out[0] = padded[pl.ds(8, 256), pl.ds(128, 128)].T[120:128]
    edges_out[1] = padded[pl.ds(8, 256), pl.ds(0, 128)].T[0:8]
    halo_copies = (
        pltpu.make_async_remote_copy(scalar.at[0, pl.ds(248, 8)], padded.at[pl.ds(0, 8)], send_sem.at[3], halo_sem.at[0],
                                     device_id=at_row(1), device_id_type=MESH),
        pltpu.make_async_remote_copy(scalar.at[0, pl.ds(0, 8)], padded.at[pl.ds(264, 8)], send_sem.at[4], halo_sem.at[1],
                                     device_id=at_row(7), device_id_type=MESH),
        pltpu.make_async_remote_copy(edges_out.at[0], edges_in.at[0], send_sem.at[5], halo_sem.at[2],
                                     device_id=at_col(1), device_id_type=MESH),
        pltpu.make_async_remote_copy(edges_out.at[1], edges_in.at[1], send_sem.at[6], halo_sem.at[3],
                                     device_id=at_col(7), device_id_type=MESH),
    )
    for copy in halo_copies:
        copy.start()

    loads[2].wait()
    for q in range(1, 8):
        twist[0, q - 1] = jnp.broadcast_to(twiddles[:, q:q + 1], (256, 128))
        twist[1, q - 1] = jnp.broadcast_to(twiddles[:, 8 + q:9 + q], (256, 128))
    twice[8 * upper[2] + lead[2]] = modes[2, :, 0, pl.ds(pl.multiple_of(16 * lead[2], 16), 16), :]
    for p in range(2):
        own = 2 * lead[p] + upper[p]
        arrived[p, 8 * upper[p] + lead[p]] = modes[p, :, 0, pl.ds(pl.multiple_of(8 * own, 8), 8), :]
    for load in loads[3:]:
        load.wait()
    pl.semaphore_wait(ready_sem, 3)

    @pl.when(sec == 0)
    def _():
        planes[0] = jnp.zeros((256, 256), F32)

    @pl.when(sec == SECS - 1)
    def _():
        planes[1] = jnp.zeros((256, 256), F32)

    first = (row == 0) & (col == 0)

    def owners_of(p, block, half):
        if p < 2:
            return [(sec, 2 * (2 * p + half) + lax.rem(lax.div(block, 2), 2), block)]
        return [(sec, block, 4 * half + 2 * (1 - lax.rem(block, 2)) + side) for side in (lax.rem(col, 2),)]

    plain_owner = lax.rem(row + lax.div(col, 2), 2) == 0
    chunk = lax.div(row, 2)
    own_half = jnp.where(plain_owner, lax.rem(chunk, 2), lax.div(col, 4))
    own_part = jnp.where(plain_owner, lax.div(chunk, 2), 2)

    @pl.when(has_above)
    def _():
        pl.semaphore_wait(above_sem, 1)

    for p in ORDER:
        size = 8 if p < 2 else 16
        gathered = arrived.at[p] if p < 2 else twice
        some = gathered.at[pl.ds(0, 15)]
        pltpu.make_async_copy(some, some, mode_sem.at[p]).wait()
        if p == ORDER[0]:
            send_planes(0)

        @pl.when((lead[p] == 0) & (follow[p] < (4 if p < 2 else 8)))
        def _():
            pltpu.make_async_copy(extra.at[p], extra.at[p], extra_sem.at[p]).wait()
            for a in range(8):
                for part in range(2):
                    gathered[8 + a, part, 0:1] = jnp.where(group[p] > 0, extra[p, a, part:part + 1], 0.0)

        alone = jnp.where((lead[p] == 0) & (group[p] == 0) & (follow[p] < (4 if p < 2 else 8)), 1, 0)
        special = lax.broadcasted_iota(jnp.int32, (size, 128), 0) < alone
        for a in range(8):
            plus, minus = gathered[a], gathered[8 + a]
            sum_real, sum_imag = plus[0] + minus[0], plus[1] + minus[1]
            gap_real = jnp.where(special, extra[p, a, 1:2], plus[0] - minus[0])
            gap_imag = jnp.where(special, -extra[p, a, 0:1], plus[1] - minus[1])
            for block in range(8):
                cosine, sine = phases[block:block + 1, :], phases[8 + block:9 + block, :]
                if block == 0:
                    a_real, a_imag, b_real, b_imag = sum_real, sum_imag, gap_real, gap_imag
                else:
                    a_real, a_imag = sum_real * cosine - sum_imag * sine, sum_real * sine + sum_imag * cosine
                    b_real, b_imag = gap_real * cosine - gap_imag * sine, gap_real * sine + gap_imag * cosine
                for part, tile in enumerate(((a_real, -b_imag), (-a_imag, -b_real))):
                    high, low = split(jnp.concatenate(tile, 0))
                    lhs[pl.ds(2 * size * block, 2 * size), pl.ds(1024 * part + 128 * a, 128)] = high
                    lhs[pl.ds(2 * size * (8 + block), 2 * size), pl.ds(1024 * part + 128 * a, 128)] = low
        main = jnp.dot(lhs[pl.ds(0, 32 * size), :], x_high[...], preferred_element_type=F32)
        rest = jnp.dot(lhs[pl.ds(0, 16 * size), :], x_low[...], preferred_element_type=F32)
        total = main[:16 * size] + main[16 * size:] + rest
        results = sent.at[p] if p < 2 else sent_twice
        for block in range(8):
            for half in range(2):
                tile = total[2 * size * block:2 * size * (block + 1), 128 * half:128 * half + 128]
                results[block, half, 0] = tile[:size]
                results[block, half, 1] = tile[size:]

        place = 128 * group[p] + (8 * (2 * lead[p] + upper[p]) if p < 2 else 16 * lead[p])
        rows = pl.ds(pl.multiple_of(place, size), size)
        for i in FAR_FIRST + (0,):
            block = lax.rem(lead[p] + i, 8)
            for half in range(2):
                for target in owners_of(p, block, half):
                    mine = target[1 if p < 2 else 2] == follow[p]

                    def away():
                        pltpu.make_async_remote_copy(
                            results.at[block, half], spectra.at[:, rows, :], send_sem.at[1], spectra_sem,
                            device_id=target, device_id_type=MESH).start()

                    if i > 0:
                        away()
                    else:
                        pl.when(jnp.logical_not(mine))(away)

                        @pl.when(mine)
                        def _():
                            spectra[:, rows, :] = results[block, half]

        if p == ORDER[0]:
            send_planes(1)
    send_planes(2)

    @pl.when(first)
    def _():
        lone[...] = jnp.zeros_like(lone)
        for p in range(3):
            for a in range(8):
                real, imag = extra[p, a, 0:1], extra[p, a, 1:2]
                cosine, sine = phases[0:8, :], phases[8:16, :]
                lone[8 * p:8 * p + 8, pl.ds(128 * a, 128)] = real * sine + imag * cosine
                lone[8 * p:8 * p + 8, pl.ds(1024 + 128 * a, 128)] = real * cosine - imag * sine
        high, low = split(lone[...])
        total = (jnp.dot(high, x_high[...], preferred_element_type=F32) + jnp.dot(low, x_high[...], preferred_element_type=F32)
                 + jnp.dot(high, x_low[...], preferred_element_type=F32))
        def lone_tile(parts, block):
            strip = [total[8 * p + block:8 * p + block + 1, 128 * half:128 * half + 128] for p in parts for half in range(2)]
            blank = jnp.zeros((1, 128), F32)
            strip = strip + [blank] * 4 if len(parts) == 2 else [blank] * 4 + strip + [blank] * 2
            return jnp.concatenate(strip, 0)

        by_col = [lone_tile((0, 1), c) for c in range(8)]
        for r in range(8):
            by_row = lone_tile((2,), r)
            for c in range(8):
                if r == c == 0:
                    lone_row[...] = by_col[c] + by_row
                    continue
                lone_sent[8 * r + c] = by_col[c] + by_row
                pltpu.make_async_remote_copy(
                    lone_sent.at[8 * r + c], lone_row, send_sem.at[14], lone_sem,
                    device_id=(sec, r, c), device_id_type=MESH).start()

    for copy in halo_copies:
        copy.wait()
    left_edge = edges_in[0].T[:, 7:8]
    right_edge = edges_in[1].T[:, 0:1]
    lane = lax.broadcasted_iota(jnp.int32, (128, 256), 1)
    for block in range(2):
        at = 8 + 128 * block
        here = padded[pl.ds(at, 128), :]
        left = jnp.where(lane == 0, left_edge[128 * block:128 * block + 128], pltpu.roll(here, 1, 1))
        right = jnp.where(lane == 255, right_edge[128 * block:128 * block + 128], pltpu.roll(here, 255, 1))
        back = padded[pl.ds(at - 1, 128), :]
        front = padded[pl.ds(at + 1, 128), :]
        flag = jnp.where(lane < 128, obstacle[0, block, 0].astype(F32), obstacle[0, block, 1].astype(F32))
        rows = pl.ds(128 * block, 128)
        slopes[0, rows, :] = right - left
        slopes[1, rows, :] = front - back
        base[rows, :] = here + 0.04 * (left + right + back + front - 6.0 * here) - 0.25 * flag * (here - 1.0)

    def spectra_through(semaphore):
        for count, here in ((504, plain_owner), (496, jnp.logical_not(plain_owner))):
            some = spectra.at[:, pl.ds(0, count), :]
            pl.when(here)(pltpu.make_async_copy(some, some, semaphore).wait)

    spectra_through(spectra_sem)
    send_planes(3)
    for q in range(8):
        for part in range(2):
            high, low = split(spectra[part, pl.ds(q, 64, stride=8), :])
            rhs[pl.ds(64 * part, 64), pl.ds(128 * q, 128)] = high
            rhs[pl.ds(128 + 64 * part, 64), pl.ds(128 * q, 128)] = low
    quarter = lax.rem(lax.broadcasted_iota(jnp.int32, (16, 128), 0), 4)
    lone_real = jnp.where(quarter == 0, 1.0, jnp.where(quarter == 2, -1.0, 0.0)) * spectra[1, 0:1, :]

    def combine(i, number):
        at = 16 * i
        rows = pl.ds(128 * number + at, 16)
        real, imag = [], []
        for q in range(8):
            re = waves[pl.ds(256 * number + at, 16), pl.ds(128 * q, 128)]
            if q == 0:
                real.append(re + lone_real)
                imag.append(None)
                continue
            im = waves[pl.ds(256 * number + 128 + at, 16), pl.ds(128 * q, 128)]
            cosine, sine = twist[0, q - 1, rows, :], twist[1, q - 1, rows, :]
            real.append(re * cosine - im * sine)
            imag.append(None if q == 4 else re * sine + im * cosine)
        a1, b1 = real[1] + real[7], imag[1] - imag[7]
        a2, b2 = real[2] + real[6], imag[2] - imag[6]
        a3, b3 = real[3] + real[5], imag[3] - imag[5]
        even, odd = real[0] + real[4], real[0] - real[4]
        e0, e2, e1, e3 = even + a2, even - a2, odd - b2, odd + b2
        d0, d2 = a1 + a3, b3 - b1
        amid, bmid = HALF_ROOT * (a1 - a3), HALF_ROOT * (b1 + b3)
        d1, d3 = amid - bmid, -amid - bmid
        for r, (e, d) in enumerate(((e0, d0), (e1, d1), (e2, d2), (e3, d3))):
            fields[r, rows, :] = e + d
            fields[r + 4, rows, :] = e - d
        return number

    def send_fields(number, peers, steps, rows):
        def go():
            for i in steps:
                peer = lax.rem(number + i, 8)
                pltpu.make_async_remote_copy(
                    fields.at[peer, rows], velocity.at[own_part, own_half, rows], send_sem.at[2], velocity_sem.at[own_part],
                    device_id=peers(i), device_id_type=MESH).start()
            velocity[own_part, own_half, rows] = fields[number, rows]
        return go

    for number in range(2):
        rows = pl.ds(256 * number, 256)
        waves[rows, :] = (jnp.dot(y_high[rows, :], rhs[...], preferred_element_type=F32)
                          + jnp.dot(y_low[rows, :], rhs[pl.ds(0, 128), :], preferred_element_type=F32))
        for i in range(8):
            combine(i, number)
        rows = pl.ds(128 * number, 128)
        pl.when(plain_owner)(send_fields(row, at_row, FAR_FIRST, rows))
        pl.when(jnp.logical_not(plain_owner))(send_fields(col, at_col, (4, 2, 6), rows))

    pieces = [piece for piece in range(4) if PIECES[piece]]
    for piece in pieces:
        up, down = plane_copies(piece)
        pl.when(has_below)(up.wait_recv)
        pl.when(has_above)(down.wait_recv)
    slopes[2] = planes[1] - planes[0]
    base[...] = base[...] + 0.04 * (planes[1] + planes[0])

    for p in range(3):
        one = pltpu.make_async_copy(velocity.at[p, 0], velocity.at[p, 0], velocity_sem.at[p])
        two = pltpu.make_async_copy(velocity.at[p], velocity.at[p], velocity_sem.at[p])
        pl.when(own_part == p)(one.wait)
        pl.when(own_part != p)(two.wait)
    @pl.when(jnp.logical_not(first))
    def _():
        pltpu.make_async_copy(lone_row, lone_row, lone_sem).wait()

    quarter = lax.rem(lax.broadcasted_iota(jnp.int32, (256, 128), 0), 4)
    swing = jnp.where(quarter == 1, 1.0, jnp.where(quarter == 3, -1.0, 0.0))

    def field(p, half):
        return velocity[p, half] + swing * lone_row[2 * p + half:2 * p + half + 1, :]

    turned = [field(2, half).T for half in range(2)]
    for block in range(2):
        lanes = pl.ds(128 * block, 128)
        partial = field(0, block) * slopes[0, :, lanes] + field(1, block) * slopes[1, :, lanes]
        for half in range(2):
            rows = pl.ds(128 * half, 128)
            out[0, rows, lanes] = base[rows, lanes] - 0.125 * (
                partial[128 * half:128 * half + 128] + turned[half][:, 128 * block:128 * block + 128] * slopes[2, rows, lanes])

    sent_modes = spectra.at[:, pl.ds(0, 480), :]
    pltpu.make_async_copy(sent_modes, sent_modes, send_sem.at[0]).wait()

    spectra_through(send_sem.at[1])

    def fields_left(count):
        most = fields.at[pl.ds(0, count)]
        return pltpu.make_async_copy(most, most, send_sem.at[2]).wait

    pl.when(plain_owner)(fields_left(7))
    pl.when(jnp.logical_not(plain_owner))(fields_left(3))

    for p, copy in zero_copies:
        pl.when(follow[p] >= 4)(send_zero(p, copy).wait_send)

    @pl.when(first)
    def _():
        some = lone_sent.at[pl.ds(1, 63)]
        pltpu.make_async_copy(some, some, send_sem.at[14]).wait()

    for piece in pieces:
        up, down = plane_copies(piece)
        pl.when(has_above)(up.wait_send)
        pl.when(has_below)(down.wait_send)


def body(modes, scalar, obstacle):
    x_high, x_low, y_high, y_low, phases, twiddles = (jnp.asarray(t) for t in tables())
    anywhere = pl.BlockSpec(memory_space=pl.ANY)
    vmem = pl.BlockSpec(memory_space=pltpu.VMEM)
    smem = pl.BlockSpec(memory_space=pltpu.SMEM)
    dma = pltpu.SemaphoreType.DMA
    return pl.pallas_call(
        kernel,
        out_shape=pltpu.VMEM((1, 256, 256), F32),
        in_specs=[anywhere, anywhere, smem] + [anywhere] * 6,
        out_specs=vmem,
        scratch_shapes=[
            pltpu.VMEM((3, 2, 1, 128, 128), F32),
            pltpu.VMEM((3, 8, 128), F32),
            pltpu.VMEM((3, 8, 8, 128), F32),
            pltpu.VMEM((2, 16, 2, 8, 128), F32),
            pltpu.VMEM((16, 2, 16, 128), F32),
            pltpu.VMEM((2048, 256), BF16),
            pltpu.VMEM((2048, 256), BF16),
            pltpu.VMEM((512, 256), BF16),
            pltpu.VMEM((512, 128), BF16),
            pltpu.VMEM((16, 128), F32),
            pltpu.VMEM((256, 16), F32),
            pltpu.VMEM((512, 2048), BF16),
            pltpu.VMEM((32, 2048), F32),
            pltpu.VMEM((64, 8, 128), F32),
            pltpu.VMEM((8, 128), F32),
            pltpu.VMEM((2, 8, 2, 2, 8, 128), F32),
            pltpu.VMEM((8, 2, 2, 16, 128), F32),
            pltpu.VMEM((2, 512, 128), F32),
            pltpu.VMEM((256, 1024), BF16),
            pltpu.VMEM((512, 1024), F32),
            pltpu.VMEM((2, 7, 256, 128), F32),
            pltpu.VMEM((8, 256, 128), F32),
            pltpu.VMEM((3, 2, 256, 128), F32),
            pltpu.VMEM((272, 256), F32),
            pltpu.VMEM((2, 8, 256), F32),
            pltpu.VMEM((2, 8, 256), F32),
            pltpu.VMEM((2, 256, 256), F32),
            pltpu.VMEM((256, 256), F32),
            pltpu.VMEM((3, 256, 256), F32),
            dma((8,)), dma((3,)), dma((3,)), dma, dma, dma((3,)), dma((4,)), dma((8,)), dma((24,)), pltpu.SemaphoreType.REGULAR, pltpu.SemaphoreType.REGULAR,
        ],
        compiler_params=pltpu.CompilerParams(
            collective_id=0, has_side_effects=True, vmem_limit_bytes=56 * 1024 * 1024),
    )(modes, scalar, obstacle, x_high, x_low, y_high, y_low, phases, twiddles)


def solution(mesh):
    in_specs = (P(None, None, "sec", "row", "col"), P("sec", "row", "col"), P("sec", "row", "col"))
    out_specs = P("sec", "row", "col")
    return jax.shard_map(body, mesh=mesh, in_specs=in_specs, out_specs=out_specs, check_vma=False)
```

```python
import math

import jax
import jax.numpy as jnp
import numpy as np
from jax import lax
from jax.experimental import pallas as pl
from jax.experimental.pallas import tpu as pltpu
from jax.sharding import PartitionSpec as P

NV = 1024
NS = 2048
ROWS = 8
COLS = 8
SECS = 4
FAR_FIRST = (4, 5, 3, 2, 6, 1, 7)
PIECES = (32,0,112,112)
ORDER = (0,1,2)
F32 = jnp.float32
BF16 = jnp.bfloat16
MESH = pl.DeviceIdType.MESH
HALF_ROOT = math.sqrt(0.5)


def split_pair(table):
    high = table.astype(BF16)
    low = (table - high.astype(np.float64)).astype(BF16)
    return high, low


def tables():
    k = np.arange(NV)
    k = np.where(k < NV // 2, k, k - NV)
    s = np.arange(256)
    turn = 2.0 * math.pi / NS * ((k[:, None] * s[None, :]) % NS)
    x_high, x_low = split_pair(np.concatenate([np.cos(turn), np.sin(turn)], 0))
    m = np.arange(64)
    turn = 2.0 * math.pi / 256 * ((s[:, None] * m[None, :]) % 256)
    c, d = np.cos(turn), np.sin(turn)
    y_high, y_low = split_pair(np.concatenate([np.block([[c[h], d[h]], [d[h], -c[h]]]) for h in (slice(0, 128), slice(128, 256))], 0))
    y_high = np.concatenate([y_high, y_high], 1)
    lanes = np.arange(128)
    turn = 2.0 * math.pi / 8 * ((np.arange(8)[:, None] * lanes[None, :]) % 8)
    phases = np.concatenate([np.cos(turn), np.sin(turn)], 0).astype(np.float32)
    q = np.arange(8)
    turn = 2.0 * math.pi / NS * (s[:, None] * q[None, :])
    twiddles = np.concatenate([np.cos(turn), np.sin(turn)], 1).astype(np.float32)
    return x_high, x_low, y_high, y_low, phases, twiddles


def split(value):
    high = value.astype(BF16)
    return high, (value - high.astype(F32)).astype(BF16)


def flip(index, bits):
    total = 0
    for unit in (1, 2, 4):
        bit = lax.rem(lax.div(index, unit), 2)
        total = total + unit * ((1 - bit) if bits & unit else bit)
    return total


def kernel(modes_in, scalar, obstacle, x_high_in, x_low_in, y_high_in, y_low_in, phases_in, twiddles_in, out,
           modes, row_zero, extra, arrived, twice, x_high, x_low, y_high, y_low, phases, twiddles, lhs, lone, lone_sent, lone_row, sent, sent_twice, spectra, rhs, waves, twist, fields, velocity,
           padded, edges_out, edges_in, planes, base, slopes,
           table_sem, mode_sem, extra_sem, lone_sem, spectra_sem, velocity_sem, halo_sem, plane_sem, send_sem, ready_sem, above_sem):
    sec, row, col = lax.axis_index("sec"), lax.axis_index("row"), lax.axis_index("col")

    barrier = pltpu.get_barrier_semaphore()

    def at_row(i):
        return (sec, lax.rem(row + i, ROWS), col)

    def at_col(i):
        return (sec, row, lax.rem(col + i, COLS))

    greeted = [(sec, 7 - row, lax.rem(col + i, COLS)) for i in FAR_FIRST + (0,)]
    greeted += [(sec, flip(row, i), c) for c in (7 - col, col) for i in range(6, 0, -1)]
    greeted += [at_col(i) for i in FAR_FIRST]
    for device in greeted:
        pl.semaphore_signal(barrier, inc=1, device_id=device, device_id_type=MESH)
    @pl.when((col == 0) & (row < 4))
    def _():
        for i in range(8):
            pl.semaphore_signal(barrier, inc=1, device_id=(sec, jnp.where(row > 0, 8 - row, 4), i), device_id_type=MESH)

    @pl.when(row == 0)
    def _():
        source = jnp.where(col < 4, jnp.where(col > 0, 8 - col, 4), jnp.where(col < 7, col + 1, 4))
        for i in range(8):
            pl.semaphore_signal(barrier, inc=1, device_id=(sec, i, source), device_id_type=MESH)

    has_above, has_below = sec < SECS - 1, sec > 0

    @pl.when(has_above)
    def _():
        pl.semaphore_signal(barrier, inc=1, device_id=(lax.rem(sec + 1, SECS), row, col), device_id_type=MESH)

    pairs = ((modes_in, modes), (scalar.at[0], padded.at[pl.ds(8, 256)]), (twiddles_in, twiddles), (phases_in, phases),
             (x_high_in, x_high), (x_low_in, x_low), (y_high_in, y_high), (y_low_in, y_low))
    loads = [pltpu.make_async_copy(here, there, table_sem.at[i]) for i, (here, there) in enumerate(pairs)]
    for load in loads:
        load.start()

    lead = (col, col, row)
    follow = (row, row, col)
    upper = [lax.div(f, 4) for f in follow]
    group = [f + u * (7 - 2 * f) for f, u in zip(follow, upper)]

    def device_at(p, f, l):
        return (sec, f, l) if p < 2 else (sec, l, f)

    loads[0].wait()
    for part in range(2):
        modes[2, part, 0] = modes[2, part, 0].T
    ahead = lax.broadcasted_iota(jnp.int32, (128, 128), 0) + lax.broadcasted_iota(jnp.int32, (128, 128), 1)
    mirror = jnp.where(ahead == 128, 1.0, 0.0).astype(F32)

    def turn_round(p):
        def go():
            for part in range(2):
                block = modes[p, part, 0]
                row_zero[p, part:part + 1] = block[0:1]
                modes[p, part, 0] = jnp.dot(mirror, block, precision=lax.Precision.HIGHEST, preferred_element_type=F32)
        return go

    for p in ORDER:
        pl.when(follow[p] >= 4)(turn_round(p))
    pl.semaphore_wait(barrier, 27 + lax.div(sec + 3, 4) + lax.div(row, 4) + 2 * lax.div(col, 4))

    @pl.when(has_below)
    def _():
        pl.semaphore_signal(above_sem, inc=1, device_id=(lax.rem(sec + SECS - 1, SECS), row, col), device_id_type=MESH)

    for i in (1, 2, 3):
        pl.semaphore_signal(ready_sem, inc=1, device_id=(sec, flip(row, i), col), device_id_type=MESH)

    def send_zero(p, copy=0):
        target = lax.rem(8 - follow[p], 4)
        return pltpu.make_async_remote_copy(
            row_zero.at[p], extra.at[p, lead[p]], send_sem.at[11 + p if copy == 0 else 23], extra_sem.at[p],
            device_id=device_at(p, target if copy == 0 else 7 - target, 0), device_id_type=MESH)

    zero_copies = ((0, 0), (1, 0), (2, 0), (2, 1))
    for p, copy in zero_copies:
        pl.when(follow[p] >= 4)(send_zero(p, copy).start)

    for p in ORDER:
        slot = 8 * upper[p] + lead[p]
        for i in FAR_FIRST + (0,):
            other = lax.rem(lead[p] + i, 8)
            for f in ((follow[p], 7 - follow[p]) if i else (7 - follow[p],)):
                pltpu.make_async_remote_copy(
                    modes.at[p, :, 0, pl.ds(pl.multiple_of(8 * (2 * other + lax.div(f, 4)), 8), 8), :] if p < 2
                    else modes.at[p, :, 0, pl.ds(pl.multiple_of(16 * other, 16), 16), :],
                    arrived.at[p, slot] if p < 2 else twice.at[slot],
                    send_sem.at[0], mode_sem.at[p], device_id=device_at(p, f, other), device_id_type=MESH).start()

    def plane_copies(piece):
        rows = pl.ds(sum(PIECES[:piece]), PIECES[piece])
        return [pltpu.make_async_remote_copy(
            scalar.at[0, rows], planes.at[i, rows], send_sem.at[15 + 2 * piece + i], plane_sem.at[2 * piece + i],
            device_id=(lax.rem(sec + step, SECS), row, col), device_id_type=MESH) for i, step in enumerate((1, 3))]

    def send_planes(piece):
        if PIECES[piece]:
            up, down = plane_copies(piece)
            pl.when(has_above)(up.start)
            pl.when(has_below)(down.start)

    loads[1].wait()
    edges_out[0] = padded[pl.ds(8, 256), pl.ds(128, 128)].T[120:128]
    edges_out[1] = padded[pl.ds(8, 256), pl.ds(0, 128)].T[0:8]
    halo_copies = (
        pltpu.make_async_remote_copy(scalar.at[0, pl.ds(248, 8)], padded.at[pl.ds(0, 8)], send_sem.at[3], halo_sem.at[0],
                                     device_id=at_row(1), device_id_type=MESH),
        pltpu.make_async_remote_copy(scalar.at[0, pl.ds(0, 8)], padded.at[pl.ds(264, 8)], send_sem.at[4], halo_sem.at[1],
                                     device_id=at_row(7), device_id_type=MESH),
        pltpu.make_async_remote_copy(edges_out.at[0], edges_in.at[0], send_sem.at[5], halo_sem.at[2],
                                     device_id=at_col(1), device_id_type=MESH),
        pltpu.make_async_remote_copy(edges_out.at[1], edges_in.at[1], send_sem.at[6], halo_sem.at[3],
                                     device_id=at_col(7), device_id_type=MESH),
    )
    for copy in halo_copies:
        copy.start()

    loads[2].wait()
    for q in range(1, 8):
        twist[0, q - 1] = jnp.broadcast_to(twiddles[:, q:q + 1], (256, 128))
        twist[1, q - 1] = jnp.broadcast_to(twiddles[:, 8 + q:9 + q], (256, 128))
    twice[8 * upper[2] + lead[2]] = modes[2, :, 0, pl.ds(pl.multiple_of(16 * lead[2], 16), 16), :]
    for p in range(2):
        own = 2 * lead[p] + upper[p]
        arrived[p, 8 * upper[p] + lead[p]] = modes[p, :, 0, pl.ds(pl.multiple_of(8 * own, 8), 8), :]
    for load in loads[3:]:
        load.wait()
    pl.semaphore_wait(ready_sem, 3)

    @pl.when(sec == 0)
    def _():
        planes[0] = jnp.zeros((256, 256), F32)

    @pl.when(sec == SECS - 1)
    def _():
        planes[1] = jnp.zeros((256, 256), F32)

    first = (row == 0) & (col == 0)

    def owners_of(p, block, half):
        if p < 2:
            return [(sec, 2 * (2 * p + half) + lax.rem(lax.div(block, 2), 2), block)]
        return [(sec, block, 4 * half + 2 * (1 - lax.rem(block, 2)) + side) for side in (lax.rem(col, 2),)]

    plain_owner = lax.rem(row + lax.div(col, 2), 2) == 0
    chunk = lax.div(row, 2)
    own_half = jnp.where(plain_owner, lax.rem(chunk, 2), lax.div(col, 4))
    own_part = jnp.where(plain_owner, lax.div(chunk, 2), 2)

    @pl.when(has_above)
    def _():
        pl.semaphore_wait(above_sem, 1)

    for p in ORDER:
        size = 8 if p < 2 else 16
        gathered = arrived.at[p] if p < 2 else twice
        some = gathered.at[pl.ds(0, 15)]
        pltpu.make_async_copy(some, some, mode_sem.at[p]).wait()
        if p == ORDER[0]:
            send_planes(0)

        @pl.when((lead[p] == 0) & (follow[p] < (4 if p < 2 else 8)))
        def _():
            pltpu.make_async_copy(extra.at[p], extra.at[p], extra_sem.at[p]).wait()
            for a in range(8):
                for part in range(2):
                    gathered[8 + a, part, 0:1] = jnp.where(group[p] > 0, extra[p, a, part:part + 1], 0.0)

        alone = jnp.where((lead[p] == 0) & (group[p] == 0) & (follow[p] < (4 if p < 2 else 8)), 1, 0)
        special = lax.broadcasted_iota(jnp.int32, (size, 128), 0) < alone
        for a in range(8):
            plus, minus = gathered[a], gathered[8 + a]
            sum_real, sum_imag = plus[0] + minus[0], plus[1] + minus[1]
            gap_real = jnp.where(special, extra[p, a, 1:2], plus[0] - minus[0])
            gap_imag = jnp.where(special, -extra[p, a, 0:1], plus[1] - minus[1])
            for block in range(8):
                cosine, sine = phases[block:block + 1, :], phases[8 + block:9 + block, :]
                if block == 0:
                    a_real, a_imag, b_real, b_imag = sum_real, sum_imag, gap_real, gap_imag
                else:
                    a_real, a_imag = sum_real * cosine - sum_imag * sine, sum_real * sine + sum_imag * cosine
                    b_real, b_imag = gap_real * cosine - gap_imag * sine, gap_real * sine + gap_imag * cosine
                for part, tile in enumerate(((a_real, -b_imag), (-a_imag, -b_real))):
                    high, low = split(jnp.concatenate(tile, 0))
                    lhs[pl.ds(2 * size * block, 2 * size), pl.ds(1024 * part + 128 * a, 128)] = high
                    lhs[pl.ds(2 * size * (8 + block), 2 * size), pl.ds(1024 * part + 128 * a, 128)] = low
        main = jnp.dot(lhs[pl.ds(0, 32 * size), :], x_high[...], preferred_element_type=F32)
        rest = jnp.dot(lhs[pl.ds(0, 16 * size), :], x_low[...], preferred_element_type=F32)
        total = main[:16 * size] + main[16 * size:] + rest
        results = sent.at[p] if p < 2 else sent_twice
        for block in range(8):
            for half in range(2):
                tile = total[2 * size * block:2 * size * (block + 1), 128 * half:128 * half + 128]
                results[block, half, 0] = tile[:size]
                results[block, half, 1] = tile[size:]

        place = 128 * group[p] + (8 * (2 * lead[p] + upper[p]) if p < 2 else 16 * lead[p])
        rows = pl.ds(pl.multiple_of(place, size), size)
        for i in FAR_FIRST + (0,):
            block = lax.rem(lead[p] + i, 8)
            for half in range(2):
                for target in owners_of(p, block, half):
                    mine = target[1 if p < 2 else 2] == follow[p]

                    def away():
                        pltpu.make_async_remote_copy(
                            results.at[block, half], spectra.at[:, rows, :], send_sem.at[1], spectra_sem,
                            device_id=target, device_id_type=MESH).start()

                    if i > 0:
                        away()
                    else:
                        pl.when(jnp.logical_not(mine))(away)

                        @pl.when(mine)
                        def _():
                            spectra[:, rows, :] = results[block, half]

        if p == ORDER[0]:
            send_planes(1)
    send_planes(2)

    @pl.when(first)
    def _():
        lone[...] = jnp.zeros_like(lone)
        for p in range(3):
            for a in range(8):
                real, imag = extra[p, a, 0:1], extra[p, a, 1:2]
                cosine, sine = phases[0:8, :], phases[8:16, :]
                lone[8 * p:8 * p + 8, pl.ds(128 * a, 128)] = real * sine + imag * cosine
                lone[8 * p:8 * p + 8, pl.ds(1024 + 128 * a, 128)] = real * cosine - imag * sine
        high, low = split(lone[...])
        total = (jnp.dot(high, x_high[...], preferred_element_type=F32) + jnp.dot(low, x_high[...], preferred_element_type=F32)
                 + jnp.dot(high, x_low[...], preferred_element_type=F32))
        def lone_tile(parts, block):
            strip = [total[8 * p + block:8 * p + block + 1, 128 * half:128 * half + 128] for p in parts for half in range(2)]
            blank = jnp.zeros((1, 128), F32)
            strip = strip + [blank] * 4 if len(parts) == 2 else [blank] * 4 + strip + [blank] * 2
            return jnp.concatenate(strip, 0)

        by_col = [lone_tile((0, 1), c) for c in range(8)]
        for r in range(8):
            by_row = lone_tile((2,), r)
            for c in range(8):
                if r == c == 0:
                    lone_row[...] = by_col[c] + by_row
                    continue
                lone_sent[8 * r + c] = by_col[c] + by_row
                pltpu.make_async_remote_copy(
                    lone_sent.at[8 * r + c], lone_row, send_sem.at[14], lone_sem,
                    device_id=(sec, r, c), device_id_type=MESH).start()

    for copy in halo_copies:
        copy.wait()
    left_edge = edges_in[0].T[:, 7:8]
    right_edge = edges_in[1].T[:, 0:1]
    lane = lax.broadcasted_iota(jnp.int32, (128, 256), 1)
    for block in range(2):
        at = 8 + 128 * block
        here = padded[pl.ds(at, 128), :]
        left = jnp.where(lane == 0, left_edge[128 * block:128 * block + 128], pltpu.roll(here, 1, 1))
        right = jnp.where(lane == 255, right_edge[128 * block:128 * block + 128], pltpu.roll(here, 255, 1))
        back = padded[pl.ds(at - 1, 128), :]
        front = padded[pl.ds(at + 1, 128), :]
        flag = jnp.where(lane < 128, obstacle[0, block, 0].astype(F32), obstacle[0, block, 1].astype(F32))
        rows = pl.ds(128 * block, 128)
        slopes[0, rows, :] = right - left
        slopes[1, rows, :] = front - back
        base[rows, :] = here + 0.04 * (left + right + back + front - 6.0 * here) - 0.25 * flag * (here - 1.0)

    def spectra_through(semaphore):
        for count, here in ((504, plain_owner), (496, jnp.logical_not(plain_owner))):
            some = spectra.at[:, pl.ds(0, count), :]
            pl.when(here)(pltpu.make_async_copy(some, some, semaphore).wait)

    spectra_through(spectra_sem)
    send_planes(3)
    for q in range(8):
        for part in range(2):
            high, low = split(spectra[part, pl.ds(q, 64, stride=8), :])
            rhs[pl.ds(64 * part, 64), pl.ds(128 * q, 128)] = high
            rhs[pl.ds(128 + 64 * part, 64), pl.ds(128 * q, 128)] = low
    quarter = lax.rem(lax.broadcasted_iota(jnp.int32, (16, 128), 0), 4)
    lone_real = jnp.where(quarter == 0, 1.0, jnp.where(quarter == 2, -1.0, 0.0)) * spectra[1, 0:1, :]

    def combine(i, number):
        at = 16 * i
        rows = pl.ds(128 * number + at, 16)
        real, imag = [], []
        for q in range(8):
            re = waves[pl.ds(256 * number + at, 16), pl.ds(128 * q, 128)]
            if q == 0:
                real.append(re + lone_real)
                imag.append(None)
                continue
            im = waves[pl.ds(256 * number + 128 + at, 16), pl.ds(128 * q, 128)]
            cosine, sine = twist[0, q - 1, rows, :], twist[1, q - 1, rows, :]
            real.append(re * cosine - im * sine)
            imag.append(None if q == 4 else re * sine + im * cosine)
        a1, b1 = real[1] + real[7], imag[1] - imag[7]
        a2, b2 = real[2] + real[6], imag[2] - imag[6]
        a3, b3 = real[3] + real[5], imag[3] - imag[5]
        even, odd = real[0] + real[4], real[0] - real[4]
        e0, e2, e1, e3 = even + a2, even - a2, odd - b2, odd + b2
        d0, d2 = a1 + a3, b3 - b1
        amid, bmid = HALF_ROOT * (a1 - a3), HALF_ROOT * (b1 + b3)
        d1, d3 = amid - bmid, -amid - bmid
        for r, (e, d) in enumerate(((e0, d0), (e1, d1), (e2, d2), (e3, d3))):
            fields[r, rows, :] = e + d
            fields[r + 4, rows, :] = e - d
        return number

    def send_fields(number, peers, steps, rows):
        def go():
            for i in steps:
                peer = lax.rem(number + i, 8)
                pltpu.make_async_remote_copy(
                    fields.at[peer, rows], velocity.at[own_part, own_half, rows], send_sem.at[2], velocity_sem.at[own_part],
                    device_id=peers(i), device_id_type=MESH).start()
            velocity[own_part, own_half, rows] = fields[number, rows]
        return go

    for number in range(2):
        rows = pl.ds(256 * number, 256)
        waves[rows, :] = (jnp.dot(y_high[rows, :], rhs[...], preferred_element_type=F32)
                          + jnp.dot(y_low[rows, :], rhs[pl.ds(0, 128), :], preferred_element_type=F32))
        for i in range(8):
            combine(i, number)
        rows = pl.ds(128 * number, 128)
        pl.when(plain_owner)(send_fields(row, at_row, FAR_FIRST, rows))
        pl.when(jnp.logical_not(plain_owner))(send_fields(col, at_col, (4, 2, 6), rows))

    pieces = [piece for piece in range(4) if PIECES[piece]]
    for piece in pieces:
        up, down = plane_copies(piece)
        pl.when(has_below)(up.wait_recv)
        pl.when(has_above)(down.wait_recv)
    slopes[2] = planes[1] - planes[0]
    base[...] = base[...] + 0.04 * (planes[1] + planes[0])

    for p in range(3):
        one = pltpu.make_async_copy(velocity.at[p, 0], velocity.at[p, 0], velocity_sem.at[p])
        two = pltpu.make_async_copy(velocity.at[p], velocity.at[p], velocity_sem.at[p])
        pl.when(own_part == p)(one.wait)
        pl.when(own_part != p)(two.wait)
    @pl.when(jnp.logical_not(first))
    def _():
        pltpu.make_async_copy(lone_row, lone_row, lone_sem).wait()

    quarter = lax.rem(lax.broadcasted_iota(jnp.int32, (256, 128), 0), 4)
    swing = jnp.where(quarter == 1, 1.0, jnp.where(quarter == 3, -1.0, 0.0))

    def field(p, half):
        return velocity[p, half] + swing * lone_row[2 * p + half:2 * p + half + 1, :]

    turned = [field(2, half).T for half in range(2)]
    for block in range(2):
        lanes = pl.ds(128 * block, 128)
        partial = field(0, block) * slopes[0, :, lanes] + field(1, block) * slopes[1, :, lanes]
        for half in range(2):
            rows = pl.ds(128 * half, 128)
            out[0, rows, lanes] = base[rows, lanes] - 0.125 * (
                partial[128 * half:128 * half + 128] + turned[half][:, 128 * block:128 * block + 128] * slopes[2, rows, lanes])

    sent_modes = spectra.at[:, pl.ds(0, 480), :]
    pltpu.make_async_copy(sent_modes, sent_modes, send_sem.at[0]).wait()

    spectra_through(send_sem.at[1])

    def fields_left(count):
        most = fields.at[pl.ds(0, count)]
        return pltpu.make_async_copy(most, most, send_sem.at[2]).wait

    pl.when(plain_owner)(fields_left(7))
    pl.when(jnp.logical_not(plain_owner))(fields_left(3))

    for p, copy in zero_copies:
        pl.when(follow[p] >= 4)(send_zero(p, copy).wait_send)

    @pl.when(first)
    def _():
        some = lone_sent.at[pl.ds(1, 63)]
        pltpu.make_async_copy(some, some, send_sem.at[14]).wait()

    for piece in pieces:
        up, down = plane_copies(piece)
        pl.when(has_above)(up.wait_send)
        pl.when(has_below)(down.wait_send)


def body(modes, scalar, obstacle):
    x_high, x_low, y_high, y_low, phases, twiddles = (jnp.asarray(t) for t in tables())
    anywhere = pl.BlockSpec(memory_space=pl.ANY)
    vmem = pl.BlockSpec(memory_space=pltpu.VMEM)
    smem = pl.BlockSpec(memory_space=pltpu.SMEM)
    dma = pltpu.SemaphoreType.DMA
    return pl.pallas_call(
        kernel,
        out_shape=pltpu.VMEM((1, 256, 256), F32),
        in_specs=[anywhere, anywhere, smem] + [anywhere] * 6,
        out_specs=vmem,
        scratch_shapes=[
            pltpu.VMEM((3, 2, 1, 128, 128), F32),
            pltpu.VMEM((3, 8, 128), F32),
            pltpu.VMEM((3, 8, 8, 128), F32),
            pltpu.VMEM((2, 16, 2, 8, 128), F32),
            pltpu.VMEM((16, 2, 16, 128), F32),
            pltpu.VMEM((2048, 256), BF16),
            pltpu.VMEM((2048, 256), BF16),
            pltpu.VMEM((512, 256), BF16),
            pltpu.VMEM((512, 128), BF16),
            pltpu.VMEM((16, 128), F32),
            pltpu.VMEM((256, 16), F32),
            pltpu.VMEM((512, 2048), BF16),
            pltpu.VMEM((32, 2048), F32),
            pltpu.VMEM((64, 8, 128), F32),
            pltpu.VMEM((8, 128), F32),
            pltpu.VMEM((2, 8, 2, 2, 8, 128), F32),
            pltpu.VMEM((8, 2, 2, 16, 128), F32),
            pltpu.VMEM((2, 512, 128), F32),
            pltpu.VMEM((256, 1024), BF16),
            pltpu.VMEM((512, 1024), F32),
            pltpu.VMEM((2, 7, 256, 128), F32),
            pltpu.VMEM((8, 256, 128), F32),
            pltpu.VMEM((3, 2, 256, 128), F32),
            pltpu.VMEM((272, 256), F32),
            pltpu.VMEM((2, 8, 256), F32),
            pltpu.VMEM((2, 8, 256), F32),
            pltpu.VMEM((2, 256, 256), F32),
            pltpu.VMEM((256, 256), F32),
            pltpu.VMEM((3, 256, 256), F32),
            dma((8,)), dma((3,)), dma((3,)), dma, dma, dma((3,)), dma((4,)), dma((8,)), dma((24,)), pltpu.SemaphoreType.REGULAR, pltpu.SemaphoreType.REGULAR,
        ],
        compiler_params=pltpu.CompilerParams(
            collective_id=0, has_side_effects=True, vmem_limit_bytes=56 * 1024 * 1024),
    )(modes, scalar, obstacle, x_high, x_low, y_high, y_low, phases, twiddles)


def solution(mesh):
    in_specs = (P(None, None, "sec", "row", "col"), P("sec", "row", "col"), P("sec", "row", "col"))
    out_specs = P("sec", "row", "col")
    return jax.shard_map(body, mesh=mesh, in_specs=in_specs, out_specs=out_specs, check_vma=False)
```
